32 devices in a mesh: row: 8 (over z, core), col: 4 (over y, x).
Axes of the slice: x: 2, y: 2, z: 4, core: 2. Of those that a mesh axis runs over, the one named last changes fastest.
Arguments:
- reflectivity: float32 [32, 256, 1024], P(('row', 'col')), may hold values from 0 to 40
- scan_hour: int32 [32], replicated, may hold values from 0 to 3, as said below
- basin_ids: int32 [256, 8], P('row', 'col'), may hold values from 0 to 255, as said below
Outputs:
- hourly_depth: float32 [4, 256, 1024], P(None, 'row', 'col')
- basin_depth: float32 [256, 4], P(('row', 'col'))
The draws below stay inside these ranges and needn't reach their ends.
Inputs may be any that keep to these rules, and one draw needn't show every extreme that they name: scan_hour starts at 0, never falls, rises by at most one from one scan to the next, and every hour has 1 to 12 scans. `basin_ids`: every basin is named by at least one segment, and all segments of a basin lie in one aligned block of 8 grid rows.
All inputs are finite; a program needn't handle non-finite values.
Results may differ from the reference program's by a relative error of at most 0.00021.
Values sent between devices are 32-bit elements; how exact they have to be, the bound alone decides.
A program may use at most 64 MiB of HBM per device.

```python
import math
import jax
import jax.numpy as jnp
from jax import lax

SEG = 128
BASIN_ROWS = 8
SCANS = 32
HOURS = 4
NY = 256
NX = 1024
BASINS = 256


def draw_scan_hour(key, part):
    spare = 11
    extra = SCANS - HOURS
    slots = jax.random.permutation(jax.random.fold_in(key, 5), HOURS * spare).astype(jnp.int32)
    chosen = slots[:extra] // spare
    hour_range = jnp.arange(HOURS, dtype=jnp.int32)
    counts = 1 + jnp.sum((chosen[:, None] == hour_range[None, :]).astype(jnp.int32), axis=0)
    ends = jnp.cumsum(counts).astype(jnp.int32)
    positions = jnp.arange(SCANS, dtype=jnp.int32)
    hours = jnp.sum((ends[None, :HOURS - 1] <= positions[:, None]).astype(jnp.int32), axis=1)
    return hours.astype(jnp.int32)


def block_order(block_key):
    return jax.random.permutation(block_key, BASIN_ROWS * (NX // SEG)).astype(jnp.int32)


def draw_basin_ids(key, part):
    seg_count = NX // SEG
    block_count = NY // BASIN_ROWS
    block_cells = BASIN_ROWS * seg_count
    block_keys = jax.random.split(jax.random.fold_in(key, 3), block_count)
    ranks = jax.vmap(block_order)(block_keys).astype(jnp.int32)
    spread = jax.random.randint(jax.random.fold_in(key, 4), (block_count, block_cells), 0, seg_count).astype(jnp.int32)
    local = jnp.where(ranks < seg_count, ranks, spread).astype(jnp.int32)
    base = jnp.arange(block_count, dtype=jnp.int32)[:, None] * seg_count + local
    labels = jax.random.permutation(jax.random.fold_in(key, 7), BASINS).astype(jnp.int32)
    return labels[base].reshape(NY, seg_count).astype(jnp.int32)


def shard_levels(own_key, dims, cuts, least, top_value):
    def one(axis_at, blocks):
        heights = jax.random.uniform(jax.random.fold_in(jax.random.fold_in(own_key, 6), axis_at), (blocks,), jnp.float32, least / len(cuts), top_value / len(cuts))
        return jnp.repeat(jnp.exp(heights), dims[axis_at] // blocks).reshape((-1,) + (1,) * (len(dims) - axis_at - 1))

    loudness = one(*cuts[0])
    for cut in cuts[1:]:
        loudness = loudness * one(*cut)
    return loudness


def setup_inputs(seed: int = 0) -> dict:
    key_list = jax.random.split(jax.random.key(seed), 4)
    return {
        "reflectivity": jnp.clip(40.0 * jax.random.uniform(key_list[0], (SCANS, NY, NX), jnp.float32) ** shard_levels(key_list[0], (SCANS, NY, NX), ((0, 32),), -0.2, 0.2), 0.0, 40.0),
        "scan_hour": draw_scan_hour(jax.random.fold_in(key_list[3], 71), 0),
        "basin_ids": draw_basin_ids(jax.random.fold_in(key_list[3], 71), 0),
    }


slope_db = math.log(10.0) / 16.0
offset_zr = math.log(200.0) / 1.6


def rain_depth(reflect):
    return jnp.exp(reflect * slope_db - offset_zr) / 12.0


def reference(reflectivity, scan_hour, basin_ids):
    def accumulate(running, scan_item):
        radar_frame, hour_slot = scan_item
        return running.at[hour_slot].add(rain_depth(radar_frame)), None

    initial = jnp.zeros((HOURS, NY, NX), jnp.float32)
    hourly, unused = lax.scan(accumulate, initial, (reflectivity, scan_hour))
    segment = hourly.reshape(HOURS, NY, NX // SEG, SEG).sum(axis=3).reshape(HOURS, -1)
    flat_ids = basin_ids.reshape(-1).astype(jnp.int32)
    totals = jax.ops.segment_sum(segment.T, flat_ids, num_segments=BASINS)
    pixels = jax.ops.segment_sum(jnp.full(flat_ids.shape, float(SEG), jnp.float32), flat_ids, num_segments=BASINS)
    return hourly, totals / pixels[:, None]
```

```python
import functools
import math

import jax
import jax.numpy as jnp
from jax import lax
from jax.experimental import pallas as pl
from jax.experimental.pallas import tpu as pltpu
from jax.sharding import PartitionSpec as P

SEG = 128
BASIN_ROWS = 8
HOUR_SCANS = 12
CORES = 2
LANES = 128
HELD = 1
MESH = pl.DeviceIdType.MESH

slope_db = math.log(10.0) / 16.0
offset_zr = math.log(200.0) / 1.6 + math.log(12.0)


def kernel(
    dims,
    refl_ref,
    hour_ref,
    ids_ref,
    hourly_ref,
    basin_ref,
    frame,
    hours,
    ids,
    gather,
    part,
    zrecv,
    plane_ids,
    all_ids,
    psend,
    pcount,
    precv,
    wave_sem,
    local_sem,
    load_sem,
    own_sem,
    in_send,
    in_recv,
    z_send,
    z_recv,
    id_send,
    id_recv,
    idz_send,
    idz_recv,
    b_send,
    b_recv,
):
    row_devices, col_devices, hour_count, slots, tile_rows, tile_cols, owned = dims
    planes = row_devices // CORES
    members = CORES * col_devices
    devices = row_devices * col_devices
    scan_block = gather.shape[2]
    scan_count = hour_ref.shape[0]
    plane_scans = members * scan_block
    segs = tile_cols // SEG
    basins = devices * owned
    width = precv.shape[2]

    row = lax.axis_index("row")
    col = lax.axis_index("col")
    plane = row // CORES
    core = row % CORES
    mine = core * col_devices + col
    me = row * col_devices + col

    def first_hour(p):
        return (p * plane_scans) // HOUR_SCANS

    def hour_span(p):
        rest = scan_count - plane_scans - p * plane_scans
        return hour_count - rest // HOUR_SCANS - first_hour(p)

    def by_plane(table):
        value = table[0]
        for p in range(1, planes):
            value = jnp.where(plane == p, table[p], value)
        return value

    def chunk_order(p):
        others = sorted((d for d in range(planes) if d != p), key=lambda d: -abs(d - p))
        if 0 in others:
            others.remove(0)
            others.insert(0, 0)
        return others + [p]

    def near_order(p):
        return sorted(range(planes), key=lambda d: abs(d - p))

    orders = [chunk_order(p) for p in range(planes)]
    order = [by_plane([o[t] for o in orders]) for t in range(planes)]
    nears = [near_order(p) for p in range(planes)]
    near = [by_plane([o[t] for o in nears]) for t in range(planes)]

    def member_at(k):
        dc = k // col_devices
        dq = k % col_devices
        half = col_devices // 2
        qq = ((col // 2 + dq // 2) % half) * 2 + (col + dq) % 2
        other = ((core + dc) % CORES) * col_devices + qq
        return other, plane * CORES + other // col_devices, other % col_devices

    def several(ref, send_sem, recv_sem):
        return pltpu.make_async_remote_copy(
            src_ref=ref,
            dst_ref=ref,
            send_sem=send_sem,
            recv_sem=recv_sem,
            device_id=((row + 1) % row_devices, col),
            device_id_type=MESH,
        )

    def along_z(step):
        return ((plane + step) * CORES + core, col)

    barrier = pltpu.get_barrier_semaphore()
    for k in range(1, members):
        _, r, q = member_at(k)
        pl.semaphore_signal(barrier, inc=1, device_id=(r, q), device_id_type=MESH)

    @pl.when(plane > 0)
    def _():
        pl.semaphore_signal(barrier, inc=1, device_id=along_z(-1), device_id_type=MESH)

    @pl.when(plane < planes - 1)
    def _():
        pl.semaphore_signal(barrier, inc=1, device_id=along_z(1), device_id_type=MESH)

    def block_of(source, d, c, q):
        rows = pl.ds(pl.multiple_of((d * CORES + c) * tile_rows, 8), tile_rows)
        cols = pl.ds(pl.multiple_of(q * tile_cols, 128), tile_cols)
        return source.at[:, rows, cols]

    def plane_rows(d):
        rows = CORES * tile_rows
        return pl.ds(pl.multiple_of(d * rows, 8), rows)

    load_ids = pltpu.make_async_copy(ids_ref, ids, local_sem.at[0])
    load_ids.start()
    loads = []
    for t, d in enumerate(order):
        load = pltpu.make_async_copy(
            refl_ref.at[:, plane_rows(d), :],
            frame.at[:, plane_rows(d), :],
            load_sem.at[t],
        )
        load.start()
        loads.append(load)
    load_own_ids = pltpu.make_async_copy(
        ids_ref, plane_ids.at[mine], local_sem.at[1]
    )
    load_own_ids.start()
    load_hours = pltpu.make_async_copy(hour_ref, hours, local_sem.at[2])
    load_hours.start()
    for d in range(planes):
        own = pltpu.make_async_copy(
            block_of(refl_ref, d, core, col), gather.at[d, mine], own_sem
        )
        own.start()

    for k in range(slots):
        zrecv[plane, k] = jnp.zeros((tile_rows, tile_cols), jnp.float32)

    load_ids.wait()
    beside = jnp.where(plane > 0, 1, 0) + jnp.where(plane < planes - 1, 1, 0)
    pl.semaphore_wait(barrier, members - 1 + beside)

    def id_copy(k):
        other, r, q = member_at(k)
        return pltpu.make_async_remote_copy(
            src_ref=ids,
            dst_ref=plane_ids.at[mine],
            send_sem=id_send,
            recv_sem=id_recv,
            device_id=(r, q),
            device_id_type=MESH,
        )

    for k in range(1, members):
        id_copy(k).start()

    @pl.when((plane == 1) & (plane < planes - 1))
    def _():
        pl.semaphore_signal(
            wave_sem.at[0], inc=1, device_id=along_z(1), device_id_type=MESH
        )

    @pl.when((plane == planes - 2) & (plane > 0))
    def _():
        pl.semaphore_signal(
            wave_sem.at[1], inc=1, device_id=along_z(-1), device_id_type=MESH
        )

    def in_copy(d, k):
        other, r, q = member_at(k)
        return pltpu.make_async_remote_copy(
            src_ref=block_of(frame, d, other // col_devices, q),
            dst_ref=gather.at[d, mine],
            send_sem=in_send,
            recv_sem=in_recv.at[d],
            device_id=(r, q),
            device_id_type=MESH,
        )

    def in_arrival(d):
        return several(gather.at[d, pl.ds(0, members - 1)], in_send, in_recv.at[d])

    def send_chunk(t):
        for k in range(1, members):
            in_copy(order[t], k).start()

    early = max(1, planes - HELD)
    for t in range(early):
        loads[t].wait()
        send_chunk(t)
    for t in range(early, planes):
        loads[t].wait()


    @pl.when(plane >= 2)
    def _():
        pl.semaphore_wait(wave_sem.at[0], 1)

        @pl.when(plane < planes - 1)
        def _():
            pl.semaphore_signal(
                wave_sem.at[0], inc=1, device_id=along_z(1), device_id_type=MESH
            )

    @pl.when(plane < planes - 2)
    def _():
        pl.semaphore_wait(wave_sem.at[1], 1)

        @pl.when(plane > 0)
        def _():
            pl.semaphore_signal(
                wave_sem.at[1], inc=1, device_id=along_z(-1), device_id_type=MESH
            )

    several(plane_ids.at[pl.ds(0, members - 1)], id_send, id_recv).wait_recv()
    load_own_ids.wait()

    def idz_copy(k):
        other = (plane + k) % planes
        return pltpu.make_async_remote_copy(
            src_ref=plane_ids,
            dst_ref=all_ids.at[plane],
            send_sem=idz_send,
            recv_sem=idz_recv.at[plane],
            device_id=(other * CORES + core, col),
            device_id_type=MESH,
        )

    def idz_arrival(p):
        return several(all_ids.at[p], idz_send, idz_recv.at[p])

    for k in range(1, planes):
        idz_copy(k).start()
    all_ids[plane] = plane_ids[...]
    load_hours.wait()
    pltpu.make_async_copy(gather.at[:, 0], gather.at[:, 0], own_sem).wait()

    base_hour = first_hour(plane)
    span = hour_span(plane)

    def z_copy(d, k):
        return pltpu.make_async_remote_copy(
            src_ref=part.at[d, k],
            dst_ref=zrecv.at[plane, k],
            send_sem=z_send,
            recv_sem=z_recv.at[plane],
            device_id=(d * CORES + core, col),
            device_id_type=MESH,
        )

    def owner_lanes(o):
        return pl.ds(pl.multiple_of(((o * owned) // width) * width, width), width)

    def b_copy(k):
        other = (me + k) % devices
        return pltpu.make_async_remote_copy(
            src_ref=psend.at[:, owner_lanes(other)],
            dst_ref=precv.at[me],
            send_sem=b_send,
            recv_sem=b_recv,
            device_id=(other // col_devices, other % col_devices),
            device_id_type=MESH,
        )

    def depth_of(raw):
        return jnp.exp(raw * slope_db - offset_zr)

    def sum_rows(p, carry):
        lane = lax.broadcasted_iota(jnp.int32, (tile_rows, basins), 1)
        count, *totals = carry
        for c in range(CORES):
            depths = []
            for b in range(scan_block):
                rows = pl.ds(
                    pl.multiple_of((p * CORES + c) * tile_rows, 8), tile_rows
                )
                depths.append(depth_of(frame[b, rows, :]))
            tiles = [all_ids[p, c * col_devices + q] for q in range(col_devices)]
            columns = jnp.transpose(jnp.concatenate(tiles, axis=0).astype(jnp.float32))
            columns = columns.astype(jnp.int32)
            for g in range(segs * col_devices):
                hit = columns[:, g : g + 1] == lane
                count = count + jnp.where(hit, float(SEG), 0.0)
                for b in range(scan_block):
                    part_depth = depths[b][:, g * SEG : (g + 1) * SEG]
                    value = jnp.sum(part_depth, axis=1, keepdims=True)
                    totals[b] = totals[b] + jnp.where(hit, value, 0.0)
        return (count, *totals)

    def chunk_sums(d):
        sums = [jnp.zeros((tile_rows, tile_cols), jnp.float32)] * slots
        for i in range(members):
            for b in range(scan_block):
                hour = hours[plane * plane_scans + i * scan_block + b] - base_hour
                depth = depth_of(gather[d, i, b])
                for k in range(slots):
                    sums[k] = sums[k] + jnp.where(hour == k, depth, 0.0)
        return sums

    def push_chunk(t):
        d = order[t]
        in_arrival(d).wait_recv()
        sums = chunk_sums(d)
        for k in range(slots):
            part[d, k] = sums[k]
        for k in range(slots):

            @pl.when(k < span)
            def _():
                z_copy(d, k).start()

    def spread_basins():
        zero = jnp.zeros((tile_rows, basins), jnp.float32)
        carry = (zero,) * (scan_block + 1)
        for t, p in enumerate(near):
            if t > 0:
                idz_arrival(p).wait_recv()
            carry = sum_rows(p, carry)
        count, *totals = carry
        for b in range(scan_block):
            psend[b : b + 1, :] = jnp.sum(totals[b], axis=0, keepdims=True)
        pcount[...] = jnp.sum(count, axis=0, keepdims=True)

        def b_start(k, carry):
            b_copy(k).start()
            return carry

        lax.fori_loop(1, devices, b_start, 0, unroll=True)
        precv[me] = psend[:, owner_lanes(me)]

    for t in range(planes - 1):
        push_chunk(t)
        if t == 0:
            spread_basins()
            for late in range(early, planes):
                send_chunk(late)

    for p in range(planes):

        @pl.when(p != plane)
        def _():
            several(
                zrecv.at[p, pl.ds(0, hour_span(p))], z_send, z_recv.at[p]
            ).wait_recv()

    for h in range(hour_count):
        total = None
        for p in range(planes):
            if first_hour(p) <= h < first_hour(p) + hour_span(p):
                term = zrecv[p, h - first_hour(p)]
                total = term if total is None else total + term
        hourly_ref[h] = total

    in_arrival(plane).wait_recv()
    sums = chunk_sums(plane)
    for k in range(slots):

        @pl.when(k < span)
        def _():
            hourly_ref[base_hour + k] += sums[k]

    several(precv.at[pl.ds(0, devices - 1)], b_send, b_recv).wait_recv()
    hour_rows = lax.broadcasted_iota(jnp.int32, (hour_count, width), 0)
    total = jnp.zeros((hour_count, width), jnp.float32)
    for o in range(devices):
        for b in range(scan_block):
            hour = hours[o * scan_block + b]
            total = total + jnp.where(hour_rows == hour, precv[o, b : b + 1, :], 0.0)
    mean = total / pcount[:, owner_lanes(me)]
    mean = pltpu.roll(mean, (width - (me * owned) % width) % width, 1)
    basin_ref[...] = mean[:, :owned]

    several(plane_ids.at[pl.ds(0, members - 1)], id_send, id_recv).wait_send()
    several(all_ids.at[pl.ds(0, planes - 1)], idz_send, idz_recv.at[0]).wait_send()
    several(precv.at[pl.ds(0, devices - 1)], b_send, b_recv).wait_send()
    several(gather.at[:, pl.ds(0, members - 1)], in_send, in_recv.at[0]).wait_send()
    for n in sorted({hour_span(p) for p in range(planes)}):

        @pl.when(span == n)
        def _():
            several(
                part.at[pl.ds(0, planes - 1), pl.ds(0, n)], z_send, z_recv.at[0]
            ).wait_send()


def write_out(hourly_ref, basin_ref, hourly_out, basin_out, sem):
    pairs = ((hourly_ref, hourly_out), (basin_ref, basin_out))
    copies = [pltpu.make_async_copy(s, d, sem.at[n]) for n, (s, d) in enumerate(pairs)]
    for copy in copies:
        copy.start()
    for copy in copies:
        copy.wait()


def body(reflectivity, scan_hour, basin_ids):
    row_devices = lax.axis_size("row")
    col_devices = lax.axis_size("col")
    scan_block, grid_height, grid_width = reflectivity.shape
    tile_rows = grid_height // row_devices
    tile_cols = grid_width // col_devices
    scan_count = scan_hour.shape[0]
    hour_count = (scan_count + 10) // HOUR_SCANS + 1
    devices = row_devices * col_devices
    owned = grid_height * grid_width // (SEG * BASIN_ROWS) // devices
    planes = row_devices // CORES
    members = CORES * col_devices
    plane_scans = members * scan_block
    slots = max(
        hour_count
        - (scan_count - plane_scans * (p + 1)) // HOUR_SCANS
        - (p * plane_scans) // HOUR_SCANS
        for p in range(planes)
    )
    width = max(LANES, owned)
    dims = (row_devices, col_devices, hour_count, slots, tile_rows, tile_cols, owned)
    dma = pltpu.SemaphoreType.DMA
    f32 = jnp.float32
    anywhere = pl.BlockSpec(memory_space=pltpu.HBM)
    inside = pl.BlockSpec(memory_space=pltpu.VMEM)
    hourly, basin = pl.pallas_call(
        functools.partial(kernel, dims),
        out_shape=(
            jax.ShapeDtypeStruct((hour_count, tile_rows, tile_cols), f32),
            jax.ShapeDtypeStruct((hour_count, owned), f32),
        ),
        in_specs=[anywhere] * 3,
        out_specs=(inside, inside),
        scratch_shapes=[
            pltpu.VMEM(reflectivity.shape, f32),
            pltpu.SMEM(scan_hour.shape, jnp.int32),
            pltpu.VMEM(basin_ids.shape[::-1], jnp.int32),
            pltpu.VMEM((planes, members, scan_block, tile_rows, tile_cols), f32),
            pltpu.VMEM((planes, slots, tile_rows, tile_cols), f32),
            pltpu.VMEM((planes, slots, tile_rows, tile_cols), f32),
            pltpu.VMEM((members,) + basin_ids.shape[::-1], jnp.int32),
            pltpu.VMEM((planes, members) + basin_ids.shape[::-1], jnp.int32),
            pltpu.VMEM((scan_block, devices * owned), f32),
            pltpu.VMEM((1, devices * owned), f32),
            pltpu.VMEM((devices, scan_block, width), f32),
            pltpu.SemaphoreType.REGULAR((2,)),
            dma((3,)),
            dma((planes,)),
            dma,
            dma,
            dma((planes,)),
            dma,
            dma((planes,)),
            dma,
            dma,
            dma,
            dma((planes,)),
            dma,
            dma,
        ],
        compiler_params=pltpu.CompilerParams(
            collective_id=0, has_side_effects=True, vmem_limit_bytes=40 * 2**20
        ),
    )(*(pltpu.with_memory_space_constraint(v, pltpu.HBM) for v in (reflectivity, scan_hour, basin_ids.T)))
    hourly, basin = pl.pallas_call(
        write_out,
        out_shape=(
            jax.ShapeDtypeStruct(hourly.shape, f32),
            jax.ShapeDtypeStruct(basin.shape, f32),
        ),
        in_specs=[inside] * 2,
        out_specs=(anywhere, anywhere),
        scratch_shapes=[dma((2,))],
        compiler_params=pltpu.CompilerParams(vmem_limit_bytes=8 * 2**20),
    )(hourly, basin)
    return hourly, basin.T


def solution(mesh):
    placed = (P(("row", "col"), None, None), P(), P("row", "col"))
    return jax.shard_map(
        body,
        mesh=mesh,
        in_specs=placed,
        out_specs=(P(None, "row", "col"), P(("row", "col"), None)),
        check_vma=False,
    )
```

```python
import functools
import math

import jax
import jax.numpy as jnp
from jax import lax
from jax.experimental import pallas as pl
from jax.experimental.pallas import tpu as pltpu
from jax.sharding import PartitionSpec as P

SEG = 128
BASIN_ROWS = 8
HOUR_SCANS = 12
CORES = 2
LANES = 128
MESH = pl.DeviceIdType.MESH

slope_db = math.log(10.0) / 16.0
offset_zr = math.log(200.0) / 1.6 + math.log(12.0)


def kernel(
    dims,
    refl_ref,
    hour_ref,
    ids_ref,
    hourly_ref,
    basin_ref,
    frame,
    hours,
    ids,
    gather,
    part,
    zrecv,
    plane_ids,
    all_ids,
    seg_own,
    seg_in,
    seg_part,
    zseg,
    seg_hour,
    wave_sem,
    local_sem,
    load_sem,
    own_sem,
    in_send,
    in_recv,
    z_send,
    z_recv,
    id_send,
    id_recv,
    idz_send,
    idz_recv,
    seg_send,
    seg_recv,
    zseg_send,
    zseg_recv,
    pair_send,
    pair_recv,
):
    row_devices, col_devices, hour_count, slots, tile_rows, tile_cols, owned = dims
    planes = row_devices // CORES
    members = CORES * col_devices
    devices = row_devices * col_devices
    scan_block = gather.shape[2]
    scan_count = hour_ref.shape[0]
    plane_scans = members * scan_block
    segs = tile_cols // SEG
    all_segs, half_rows = seg_own.shape[2:]

    row = lax.axis_index("row")
    col = lax.axis_index("col")
    plane = row // CORES
    core = row % CORES
    mine = core * col_devices + col
    me = row * col_devices + col

    def first_hour(p):
        return (p * plane_scans) // HOUR_SCANS

    def hour_span(p):
        rest = scan_count - plane_scans - p * plane_scans
        return hour_count - rest // HOUR_SCANS - first_hour(p)

    def by_plane(table):
        value = table[0]
        for p in range(1, planes):
            value = jnp.where(plane == p, table[p], value)
        return value

    def chunk_order(p):
        others = sorted((d for d in range(planes) if d != p), key=lambda d: -abs(d - p))
        if 0 in others:
            others.remove(0)
            others.insert(0, 0)
        return others + [p]

    orders = [chunk_order(p) for p in range(planes)]
    order = [by_plane([o[t] for o in orders]) for t in range(planes)]

    def member_at(k):
        dc = k // col_devices
        dq = k % col_devices
        half = col_devices // 2
        qq = ((col // 2 + dq // 2) % half) * 2 + (col + dq) % 2
        other = ((core + dc) % CORES) * col_devices + qq
        return other, plane * CORES + other // col_devices, other % col_devices

    def several(ref, send_sem, recv_sem):
        return pltpu.make_async_remote_copy(
            src_ref=ref,
            dst_ref=ref,
            send_sem=send_sem,
            recv_sem=recv_sem,
            device_id=((row + 1) % row_devices, col),
            device_id_type=MESH,
        )

    def along_z(step):
        return ((plane + step) * CORES + core, col)

    barrier = pltpu.get_barrier_semaphore()
    for k in range(1, members):
        _, r, q = member_at(k)
        pl.semaphore_signal(barrier, inc=1, device_id=(r, q), device_id_type=MESH)

    @pl.when(plane > 0)
    def _():
        pl.semaphore_signal(barrier, inc=1, device_id=along_z(-1), device_id_type=MESH)

    @pl.when(plane < planes - 1)
    def _():
        pl.semaphore_signal(barrier, inc=1, device_id=along_z(1), device_id_type=MESH)

    def block_of(source, d, c, q):
        rows = pl.ds(pl.multiple_of((d * CORES + c) * tile_rows, 8), tile_rows)
        cols = pl.ds(pl.multiple_of(q * tile_cols, 128), tile_cols)
        return source.at[:, rows, cols]

    def plane_rows(d):
        rows = CORES * tile_rows
        return pl.ds(pl.multiple_of(d * rows, 8), rows)

    load_ids = pltpu.make_async_copy(ids_ref, ids, local_sem.at[0])
    load_ids.start()
    loads = []
    for t, d in enumerate(order):
        load = pltpu.make_async_copy(
            refl_ref.at[:, plane_rows(d), :],
            frame.at[:, plane_rows(d), :],
            load_sem.at[t],
        )
        load.start()
        loads.append(load)
    load_own_ids = pltpu.make_async_copy(
        ids_ref, plane_ids.at[mine], local_sem.at[1]
    )
    load_own_ids.start()
    load_hours = pltpu.make_async_copy(hour_ref, hours, local_sem.at[2])
    load_hours.start()
    for d in range(planes):
        own = pltpu.make_async_copy(
            block_of(refl_ref, d, core, col), gather.at[d, mine], own_sem
        )
        own.start()

    for k in range(slots):
        zrecv[plane, k] = jnp.zeros((tile_rows, tile_cols), jnp.float32)

    load_ids.wait()
    beside = jnp.where(plane > 0, 1, 0) + jnp.where(plane < planes - 1, 1, 0)
    pl.semaphore_wait(barrier, members - 1 + beside)

    def id_copy(k):
        other, r, q = member_at(k)
        return pltpu.make_async_remote_copy(
            src_ref=ids,
            dst_ref=plane_ids.at[mine],
            send_sem=id_send,
            recv_sem=id_recv,
            device_id=(r, q),
            device_id_type=MESH,
        )

    for k in range(1, members):
        id_copy(k).start()

    @pl.when((plane == 1) & (plane < planes - 1))
    def _():
        pl.semaphore_signal(
            wave_sem.at[0], inc=1, device_id=along_z(1), device_id_type=MESH
        )

    @pl.when((plane == planes - 2) & (plane > 0))
    def _():
        pl.semaphore_signal(
            wave_sem.at[1], inc=1, device_id=along_z(-1), device_id_type=MESH
        )

    def in_copy(d, k):
        other, r, q = member_at(k)
        return pltpu.make_async_remote_copy(
            src_ref=block_of(frame, d, other // col_devices, q),
            dst_ref=gather.at[d, mine],
            send_sem=in_send,
            recv_sem=in_recv.at[d],
            device_id=(r, q),
            device_id_type=MESH,
        )

    def in_arrival(d):
        return several(gather.at[d, pl.ds(0, members - 1)], in_send, in_recv.at[d])

    def send_chunk(t, cores=range(CORES)):
        for c in cores:
            for k in range(max(1, c * col_devices), (c + 1) * col_devices):
                in_copy(order[t], k).start()

    def seg_copy(k):
        other, r, q = member_at(k)
        return pltpu.make_async_remote_copy(
            src_ref=seg_own.at[other // col_devices],
            dst_ref=seg_in.at[mine],
            send_sem=seg_send,
            recv_sem=seg_recv,
            device_id=(r, q),
            device_id_type=MESH,
        )

    def depth_of(raw):
        return jnp.exp(raw * slope_db - offset_zr)

    def sum_segments():
        seg_row = lax.broadcasted_iota(jnp.int32, (all_segs, SEG), 0)
        for b in range(scan_block):
            for c in range(CORES):
                rows = pl.ds(c * half_rows, half_rows)
                total = jnp.zeros((all_segs, half_rows), jnp.float32)
                for g in range(all_segs):
                    depth = depth_of(frame[b, rows, g * SEG : (g + 1) * SEG])
                    total = total + lax.dot_general(
                        jnp.where(seg_row == g, 1.0, 0.0),
                        depth,
                        (((1,), (1,)), ((), ())),
                        precision=lax.Precision.HIGHEST,
                        preferred_element_type=jnp.float32,
                    )
                seg_own[c, b] = total

    loads[0].wait()
    send_chunk(0, [0])
    for load in loads[1:]:
        load.wait()
    sum_segments()
    for k in range(1, members):
        seg_copy(k).start()
    seg_in[mine] = seg_own[core]
    send_chunk(0, range(1, CORES))
    for t in range(1, planes):
        send_chunk(t)


    @pl.when(plane >= 2)
    def _():
        pl.semaphore_wait(wave_sem.at[0], 1)

        @pl.when(plane < planes - 1)
        def _():
            pl.semaphore_signal(
                wave_sem.at[0], inc=1, device_id=along_z(1), device_id_type=MESH
            )

    @pl.when(plane < planes - 2)
    def _():
        pl.semaphore_wait(wave_sem.at[1], 1)

        @pl.when(plane > 0)
        def _():
            pl.semaphore_signal(
                wave_sem.at[1], inc=1, device_id=along_z(-1), device_id_type=MESH
            )

    several(plane_ids.at[pl.ds(0, members - 1)], id_send, id_recv).wait_recv()
    load_own_ids.wait()

    def idz_copy(k):
        other = (plane + k) % planes
        return pltpu.make_async_remote_copy(
            src_ref=plane_ids,
            dst_ref=all_ids.at[plane],
            send_sem=idz_send,
            recv_sem=idz_recv,
            device_id=(other * CORES + core, col),
            device_id_type=MESH,
        )

    for k in range(1, planes):
        idz_copy(k).start()
    all_ids[plane] = plane_ids[...]
    load_hours.wait()
    pltpu.make_async_copy(gather.at[:, 0], gather.at[:, 0], own_sem).wait()

    base_hour = first_hour(plane)
    span = hour_span(plane)

    def z_copy(d, k):
        return pltpu.make_async_remote_copy(
            src_ref=part.at[d, k],
            dst_ref=zrecv.at[plane, k],
            send_sem=z_send,
            recv_sem=z_recv.at[plane],
            device_id=(d * CORES + core, col),
            device_id_type=MESH,
        )

    def zseg_copy(k):
        other = (plane + k) % planes
        return pltpu.make_async_remote_copy(
            src_ref=seg_part,
            dst_ref=zseg.at[plane],
            send_sem=zseg_send,
            recv_sem=zseg_recv,
            device_id=(other * CORES + core, col),
            device_id_type=MESH,
        )

    def pair_copy():
        return pltpu.make_async_remote_copy(
            src_ref=seg_hour.at[core],
            dst_ref=seg_hour.at[core],
            send_sem=pair_send,
            recv_sem=pair_recv,
            device_id=(plane * CORES + 1 - core, col),
            device_id_type=MESH,
        )

    def reduce_segments():
        several(seg_in.at[pl.ds(0, members - 1)], seg_send, seg_recv).wait_recv()
        sums = [jnp.zeros((all_segs, half_rows), jnp.float32)] * slots
        for i in range(members):
            for b in range(scan_block):
                hour = hours[plane * plane_scans + i * scan_block + b] - base_hour
                for k in range(slots):
                    sums[k] = sums[k] + jnp.where(hour == k, seg_in[i, b], 0.0)
        for k in range(slots):
            seg_part[k] = sums[k]
            zseg[plane, k] = sums[k]
        for k in range(1, planes):
            zseg_copy(k).start()

    def pair_segments():
        several(zseg.at[pl.ds(0, planes - 1)], zseg_send, zseg_recv).wait_recv()
        for h in range(hour_count):
            total = None
            for p in range(planes):
                if first_hour(p) <= h < first_hour(p) + hour_span(p):
                    term = zseg[p, h - first_hour(p)]
                    total = term if total is None else total + term
            seg_hour[core, h] = total
        pair_copy().start()

    def basin_means():
        several(all_ids.at[pl.ds(0, planes - 1)], idz_send, idz_recv).wait_recv()
        pair_copy().wait()
        blocks = row_devices // CORES
        halves = []
        for c in range(CORES):
            lanes = []
            for r in range(c * blocks, (c + 1) * blocks):
                first = (r % CORES) * col_devices
                tiles = [all_ids[r // CORES, first + q] for q in range(col_devices)]
                lanes.append(jnp.concatenate(tiles, axis=0))
            halves.append(jnp.concatenate(lanes, axis=1))
        place = lax.broadcasted_iota(jnp.int32, (owned, half_rows), 0)
        zero = jnp.zeros((owned, half_rows), jnp.float32)
        totals = [zero] * hour_count
        count = zero
        for n in range(owned):
            hits = [half == me * owned + n for half in halves]
            for h in range(hour_count):
                kept = [jnp.where(hits[c], seg_hour[c, h], 0.0) for c in range(CORES)]
                kept = jnp.sum(sum(kept), axis=0, keepdims=True)
                totals[h] = jnp.where(place == n, kept, totals[h])
            found = sum(jnp.where(hit, float(SEG), 0.0) for hit in hits)
            count = jnp.where(place == n, jnp.sum(found, axis=0, keepdims=True), count)
        pixels = jnp.sum(count, axis=1, keepdims=True)
        lane = lax.broadcasted_iota(jnp.int32, (owned, LANES), 1)
        means = jnp.zeros((owned, LANES), jnp.float32)
        for h in range(hour_count):
            mean = jnp.sum(totals[h], axis=1, keepdims=True) / pixels
            means = jnp.where(lane == h, mean, means)
        basin_ref[...] = jnp.transpose(means)[:hour_count, :]

    def chunk_sums(d):
        sums = [jnp.zeros((tile_rows, tile_cols), jnp.float32)] * slots
        for i in range(members):
            for b in range(scan_block):
                hour = hours[plane * plane_scans + i * scan_block + b] - base_hour
                depth = depth_of(gather[d, i, b])
                for k in range(slots):
                    sums[k] = sums[k] + jnp.where(hour == k, depth, 0.0)
        return sums

    def push_chunk(t):
        d = order[t]
        in_arrival(d).wait_recv()
        sums = chunk_sums(d)
        for k in range(slots):
            part[d, k] = sums[k]
        for k in range(slots):

            @pl.when(k < span)
            def _():
                z_copy(d, k).start()

    reduce_segments()
    for t in range(planes - 1):
        if t == planes - 2:
            pair_segments()
        push_chunk(t)
    basin_means()

    for p in range(planes):

        @pl.when(p != plane)
        def _():
            several(
                zrecv.at[p, pl.ds(0, hour_span(p))], z_send, z_recv.at[p]
            ).wait_recv()

    for h in range(hour_count):
        total = None
        for p in range(planes):
            if first_hour(p) <= h < first_hour(p) + hour_span(p):
                term = zrecv[p, h - first_hour(p)]
                total = term if total is None else total + term
        hourly_ref[h] = total

    in_arrival(plane).wait_recv()
    sums = chunk_sums(plane)
    for k in range(slots):

        @pl.when(k < span)
        def _():
            hourly_ref[base_hour + k] += sums[k]

    several(plane_ids.at[pl.ds(0, members - 1)], id_send, id_recv).wait_send()
    several(all_ids.at[pl.ds(0, planes - 1)], idz_send, idz_recv).wait_send()
    several(seg_in.at[pl.ds(0, members - 1)], seg_send, seg_recv).wait_send()
    several(zseg.at[pl.ds(0, planes - 1)], zseg_send, zseg_recv).wait_send()
    several(gather.at[:, pl.ds(0, members - 1)], in_send, in_recv.at[0]).wait_send()
    for n in sorted({hour_span(p) for p in range(planes)}):

        @pl.when(span == n)
        def _():
            several(
                part.at[pl.ds(0, planes - 1), pl.ds(0, n)], z_send, z_recv.at[0]
            ).wait_send()


def write_out(hourly_ref, basin_ref, hourly_out, basin_out, sem):
    pairs = ((hourly_ref, hourly_out), (basin_ref, basin_out))
    copies = [pltpu.make_async_copy(s, d, sem.at[n]) for n, (s, d) in enumerate(pairs)]
    for copy in copies:
        copy.start()
    for copy in copies:
        copy.wait()


def body(reflectivity, scan_hour, basin_ids):
    row_devices = lax.axis_size("row")
    col_devices = lax.axis_size("col")
    scan_block, grid_height, grid_width = reflectivity.shape
    tile_rows = grid_height // row_devices
    tile_cols = grid_width // col_devices
    scan_count = scan_hour.shape[0]
    hour_count = (scan_count + 10) // HOUR_SCANS + 1
    devices = row_devices * col_devices
    owned = grid_height * grid_width // (SEG * BASIN_ROWS) // devices
    planes = row_devices // CORES
    members = CORES * col_devices
    plane_scans = members * scan_block
    slots = max(
        hour_count
        - (scan_count - plane_scans * (p + 1)) // HOUR_SCANS
        - (p * plane_scans) // HOUR_SCANS
        for p in range(planes)
    )
    seg_shape = (grid_width // SEG, grid_height // CORES)
    dims = (row_devices, col_devices, hour_count, slots, tile_rows, tile_cols, owned)
    dma = pltpu.SemaphoreType.DMA
    f32 = jnp.float32
    anywhere = pl.BlockSpec(memory_space=pltpu.HBM)
    inside = pl.BlockSpec(memory_space=pltpu.VMEM)
    hourly, basin = pl.pallas_call(
        functools.partial(kernel, dims),
        out_shape=(
            jax.ShapeDtypeStruct((hour_count, tile_rows, tile_cols), f32),
            jax.ShapeDtypeStruct((hour_count, owned), f32),
        ),
        in_specs=[anywhere] * 3,
        out_specs=(inside, inside),
        scratch_shapes=[
            pltpu.VMEM(reflectivity.shape, f32),
            pltpu.SMEM(scan_hour.shape, jnp.int32),
            pltpu.VMEM(basin_ids.shape[::-1], jnp.int32),
            pltpu.VMEM((planes, members, scan_block, tile_rows, tile_cols), f32),
            pltpu.VMEM((planes, slots, tile_rows, tile_cols), f32),
            pltpu.VMEM((planes, slots, tile_rows, tile_cols), f32),
            pltpu.VMEM((members,) + basin_ids.shape[::-1], jnp.int32),
            pltpu.VMEM((planes, members) + basin_ids.shape[::-1], jnp.int32),
            pltpu.VMEM((CORES, scan_block) + seg_shape, f32),
            pltpu.VMEM((members, scan_block) + seg_shape, f32),
            pltpu.VMEM((slots,) + seg_shape, f32),
            pltpu.VMEM((planes, slots) + seg_shape, f32),
            pltpu.VMEM((CORES, hour_count) + seg_shape, f32),
            pltpu.SemaphoreType.REGULAR((2,)),
            dma((3,)),
            dma((planes,)),
            dma,
            dma,
            dma((planes,)),
            dma,
            dma((planes,)),
            dma,
            dma,
            dma,
            dma,
            dma,
            dma,
            dma,
            dma,
            dma,
            dma,
        ],
        compiler_params=pltpu.CompilerParams(
            collective_id=0, has_side_effects=True, vmem_limit_bytes=40 * 2**20
        ),
    )(*(pltpu.with_memory_space_constraint(v, pltpu.HBM) for v in (reflectivity, scan_hour, basin_ids.T)))
    hourly, basin = pl.pallas_call(
        write_out,
        out_shape=(
            jax.ShapeDtypeStruct(hourly.shape, f32),
            jax.ShapeDtypeStruct(basin.shape, f32),
        ),
        in_specs=[inside] * 2,
        out_specs=(anywhere, anywhere),
        scratch_shapes=[dma((2,))],
        compiler_params=pltpu.CompilerParams(vmem_limit_bytes=8 * 2**20),
    )(hourly, basin)
    return hourly, basin.T


def solution(mesh):
    placed = (P(("row", "col"), None, None), P(), P("row", "col"))
    return jax.shard_map(
        body,
        mesh=mesh,
        in_specs=placed,
        out_specs=(P(None, "row", "col"), P(("row", "col"), None)),
        check_vma=False,
    )
```

```python
import functools
import math

import jax
import jax.numpy as jnp
from jax import lax
from jax.experimental import pallas as pl
from jax.experimental.pallas import tpu as pltpu
from jax.sharding import PartitionSpec as P

SEG = 128
BASIN_ROWS = 8
HOUR_SCANS = 12
CORES = 2
LANES = 128
PIECES = 2
MESH = pl.DeviceIdType.MESH

slope_db = math.log(10.0) / 16.0
offset_zr = math.log(200.0) / 1.6 + math.log(12.0)


def kernel(
    dims,
    refl_ref,
    hour_ref,
    ids_ref,
    hourly_ref,
    basin_ref,
    frame,
    hours,
    ids,
    gather,
    part,
    zrecv,
    plane_ids,
    all_ids,
    seg_own,
    seg_in,
    seg_part,
    zseg,
    seg_hour,
    wave_sem,
    local_sem,
    load_sem,
    own_sem,
    in_send,
    in_recv,
    z_send,
    z_recv,
    id_send,
    id_recv,
    idz_send,
    idz_recv,
    seg_send,
    seg_recv,
    zseg_send,
    zseg_recv,
    pair_send,
    pair_recv,
):
    row_devices, col_devices, hour_count, slots, tile_rows, tile_cols, owned = dims
    planes = row_devices // CORES
    members = CORES * col_devices
    devices = row_devices * col_devices
    scan_block = gather.shape[2]
    scan_count = hour_ref.shape[0]
    plane_scans = members * scan_block
    piece_rows = tile_rows // PIECES
    all_segs, half_rows = seg_own.shape[2:]

    row = lax.axis_index("row")
    col = lax.axis_index("col")
    plane = row // CORES
    core = row % CORES
    mine = core * col_devices + col
    me = row * col_devices + col

    def first_hour(p):
        return (p * plane_scans) // HOUR_SCANS

    def hour_span(p):
        rest = scan_count - plane_scans - p * plane_scans
        return hour_count - rest // HOUR_SCANS - first_hour(p)

    def by_plane(table):
        value = table[0]
        for p in range(1, planes):
            value = jnp.where(plane == p, table[p], value)
        return value

    def chunk_order(p):
        others = sorted((d for d in range(planes) if d != p), key=lambda d: -abs(d - p))
        if 0 in others:
            others.remove(0)
            others.insert(0, 0)
        return others + [p]

    orders = [chunk_order(p) for p in range(planes)]
    order = [by_plane([o[t] for o in orders]) for t in range(planes)]

    def member_at(k):
        dc = k // col_devices
        dq = k % col_devices
        half = col_devices // 2
        qq = ((col // 2 + dq // 2) % half) * 2 + (col + dq) % 2
        other = ((core + dc) % CORES) * col_devices + qq
        return other, plane * CORES + other // col_devices, other % col_devices

    def several(ref, send_sem, recv_sem):
        return pltpu.make_async_remote_copy(
            src_ref=ref,
            dst_ref=ref,
            send_sem=send_sem,
            recv_sem=recv_sem,
            device_id=((row + 1) % row_devices, col),
            device_id_type=MESH,
        )

    def along_z(step):
        return ((plane + step) * CORES + core, col)

    barrier = pltpu.get_barrier_semaphore()
    for k in range(1, members):
        _, r, q = member_at(k)
        pl.semaphore_signal(barrier, inc=1, device_id=(r, q), device_id_type=MESH)

    @pl.when(plane > 0)
    def _():
        pl.semaphore_signal(barrier, inc=1, device_id=along_z(-1), device_id_type=MESH)

    @pl.when(plane < planes - 1)
    def _():
        pl.semaphore_signal(barrier, inc=1, device_id=along_z(1), device_id_type=MESH)

    def block_of(source, d, c, q):
        rows = pl.ds(pl.multiple_of((d * CORES + c) * tile_rows, 8), tile_rows)
        cols = pl.ds(pl.multiple_of(q * tile_cols, 128), tile_cols)
        return source.at[:, rows, cols]

    def plane_rows(d):
        rows = CORES * tile_rows
        return pl.ds(pl.multiple_of(d * rows, 8), rows)

    load_ids = pltpu.make_async_copy(ids_ref, ids, local_sem.at[0])
    load_ids.start()
    loads = []
    for t, d in enumerate(order):
        load = pltpu.make_async_copy(
            refl_ref.at[:, plane_rows(d), :],
            frame.at[:, plane_rows(d), :],
            load_sem.at[t],
        )
        load.start()
        loads.append(load)
    load_own_ids = pltpu.make_async_copy(
        ids_ref, plane_ids.at[mine], local_sem.at[1]
    )
    load_own_ids.start()
    load_hours = pltpu.make_async_copy(hour_ref, hours, local_sem.at[2])
    load_hours.start()
    for d in range(planes):
        own = pltpu.make_async_copy(
            block_of(refl_ref, d, core, col), gather.at[d, mine], own_sem
        )
        own.start()

    for k in range(slots):
        zrecv[plane, k] = jnp.zeros((tile_rows, tile_cols), jnp.float32)

    load_ids.wait()
    beside = jnp.where(plane > 0, 1, 0) + jnp.where(plane < planes - 1, 1, 0)
    pl.semaphore_wait(barrier, members - 1 + beside)

    def id_copy(k):
        other, r, q = member_at(k)
        return pltpu.make_async_remote_copy(
            src_ref=ids,
            dst_ref=plane_ids.at[mine],
            send_sem=id_send,
            recv_sem=id_recv,
            device_id=(r, q),
            device_id_type=MESH,
        )

    for k in range(1, members):
        id_copy(k).start()

    @pl.when((plane == 1) & (plane < planes - 1))
    def _():
        pl.semaphore_signal(
            wave_sem.at[0], inc=1, device_id=along_z(1), device_id_type=MESH
        )

    @pl.when((plane == planes - 2) & (plane > 0))
    def _():
        pl.semaphore_signal(
            wave_sem.at[1], inc=1, device_id=along_z(-1), device_id_type=MESH
        )

    def piece(g):
        return pl.ds(g * piece_rows, piece_rows)

    def in_copy(d, g, k):
        other, r, q = member_at(k)
        first = (d * CORES + other // col_devices) * tile_rows + g * piece_rows
        rows = pl.ds(pl.multiple_of(first, 8), piece_rows)
        cols = pl.ds(pl.multiple_of(q * tile_cols, 128), tile_cols)
        return pltpu.make_async_remote_copy(
            src_ref=frame.at[:, rows, cols],
            dst_ref=gather.at[d, mine, :, piece(g)],
            send_sem=in_send,
            recv_sem=in_recv.at[d, g],
            device_id=(r, q),
            device_id_type=MESH,
        )

    def in_arrival(d, g):
        ref = gather.at[d, pl.ds(0, members - 1), :, piece(g)]
        return several(ref, in_send, in_recv.at[d, g])

    far_first = sorted(range(1, members), key=lambda k: (-(k % col_devices), k))

    def send_piece(t, g):
        for k in far_first:
            in_copy(order[t], g, k).start()

    def seg_copy(k):
        other, r, q = member_at(k)
        return pltpu.make_async_remote_copy(
            src_ref=seg_own.at[other // col_devices],
            dst_ref=seg_in.at[mine],
            send_sem=seg_send,
            recv_sem=seg_recv,
            device_id=(r, q),
            device_id_type=MESH,
        )

    def depth_of(raw):
        return jnp.exp(raw * slope_db - offset_zr)

    def sum_segments():
        near_lane = lax.broadcasted_iota(jnp.int32, (SEG, LANES), 1)
        for b in range(scan_block):
            for c in range(CORES):
                rows = pl.ds(c * half_rows, half_rows)
                total = jnp.zeros((half_rows, LANES), jnp.float32)
                for g in range(all_segs):
                    rest = depth_of(frame[b, rows, g * SEG : (g + 1) * SEG])
                    ones = jnp.where(near_lane == g, 1.0, 0.0).astype(jnp.bfloat16)
                    for _ in range(3):
                        head = rest.astype(jnp.bfloat16)
                        rest = rest - head.astype(jnp.float32)
                        total = total + jnp.dot(
                            head, ones, preferred_element_type=jnp.float32
                        )
                seg_own[c, b] = jnp.transpose(total)[:all_segs]

    loads[0].wait()
    send_piece(0, 0)
    for load in loads[1:]:
        load.wait()
    sum_segments()
    for k in range(1, members):
        seg_copy(k).start()
    seg_in[mine] = seg_own[core]
    for t in range(planes):
        for g in range(PIECES):
            if t or g:
                send_piece(t, g)


    @pl.when(plane >= 2)
    def _():
        pl.semaphore_wait(wave_sem.at[0], 1)

        @pl.when(plane < planes - 1)
        def _():
            pl.semaphore_signal(
                wave_sem.at[0], inc=1, device_id=along_z(1), device_id_type=MESH
            )

    @pl.when(plane < planes - 2)
    def _():
        pl.semaphore_wait(wave_sem.at[1], 1)

        @pl.when(plane > 0)
        def _():
            pl.semaphore_signal(
                wave_sem.at[1], inc=1, device_id=along_z(-1), device_id_type=MESH
            )

    several(plane_ids.at[pl.ds(0, members - 1)], id_send, id_recv).wait_recv()
    load_own_ids.wait()

    def idz_copy(k):
        other = (plane + k) % planes
        return pltpu.make_async_remote_copy(
            src_ref=plane_ids,
            dst_ref=all_ids.at[plane],
            send_sem=idz_send,
            recv_sem=idz_recv,
            device_id=(other * CORES + core, col),
            device_id_type=MESH,
        )

    for k in range(1, planes):
        idz_copy(k).start()
    all_ids[plane] = plane_ids[...]
    load_hours.wait()
    pltpu.make_async_copy(gather.at[:, 0], gather.at[:, 0], own_sem).wait()

    base_hour = first_hour(plane)
    span = hour_span(plane)

    def z_copy(d, g, k):
        return pltpu.make_async_remote_copy(
            src_ref=part.at[d, k, piece(g)],
            dst_ref=zrecv.at[plane, k, piece(g)],
            send_sem=z_send,
            recv_sem=z_recv.at[plane],
            device_id=(d * CORES + core, col),
            device_id_type=MESH,
        )

    def zseg_copy(k):
        other = (plane + k) % planes
        return pltpu.make_async_remote_copy(
            src_ref=seg_part,
            dst_ref=zseg.at[plane],
            send_sem=zseg_send,
            recv_sem=zseg_recv,
            device_id=(other * CORES + core, col),
            device_id_type=MESH,
        )

    def pair_copy():
        return pltpu.make_async_remote_copy(
            src_ref=seg_hour.at[core],
            dst_ref=seg_hour.at[core],
            send_sem=pair_send,
            recv_sem=pair_recv,
            device_id=(plane * CORES + 1 - core, col),
            device_id_type=MESH,
        )

    def reduce_segments():
        several(seg_in.at[pl.ds(0, members - 1)], seg_send, seg_recv).wait_recv()
        sums = [jnp.zeros((all_segs, half_rows), jnp.float32)] * slots
        for i in range(members):
            for b in range(scan_block):
                hour = hours[plane * plane_scans + i * scan_block + b] - base_hour
                for k in range(slots):
                    sums[k] = sums[k] + jnp.where(hour == k, seg_in[i, b], 0.0)
        for k in range(slots):
            seg_part[k] = sums[k]
            zseg[plane, k] = sums[k]
        for k in range(1, planes):
            zseg_copy(k).start()

    def pair_segments():
        several(zseg.at[pl.ds(0, planes - 1)], zseg_send, zseg_recv).wait_recv()
        for h in range(hour_count):
            total = None
            for p in range(planes):
                if first_hour(p) <= h < first_hour(p) + hour_span(p):
                    term = zseg[p, h - first_hour(p)]
                    total = term if total is None else total + term
            seg_hour[core, h] = total
        pair_copy().start()

    def basin_means():
        several(all_ids.at[pl.ds(0, planes - 1)], idz_send, idz_recv).wait_recv()
        pair_copy().wait()
        blocks = row_devices // CORES
        halves = []
        for c in range(CORES):
            lanes = []
            for r in range(c * blocks, (c + 1) * blocks):
                first = (r % CORES) * col_devices
                tiles = [all_ids[r // CORES, first + q] for q in range(col_devices)]
                lanes.append(jnp.concatenate(tiles, axis=0))
            halves.append(jnp.concatenate(lanes, axis=1))
        place = lax.broadcasted_iota(jnp.int32, (owned, half_rows), 0)
        zero = jnp.zeros((owned, half_rows), jnp.float32)
        totals = [zero] * hour_count
        count = zero
        for n in range(owned):
            hits = [half == me * owned + n for half in halves]
            for h in range(hour_count):
                kept = [jnp.where(hits[c], seg_hour[c, h], 0.0) for c in range(CORES)]
                kept = jnp.sum(sum(kept), axis=0, keepdims=True)
                totals[h] = jnp.where(place == n, kept, totals[h])
            found = sum(jnp.where(hit, float(SEG), 0.0) for hit in hits)
            count = jnp.where(place == n, jnp.sum(found, axis=0, keepdims=True), count)
        pixels = jnp.sum(count, axis=1, keepdims=True)
        lane = lax.broadcasted_iota(jnp.int32, (owned, LANES), 1)
        means = jnp.zeros((owned, LANES), jnp.float32)
        for h in range(hour_count):
            mean = jnp.sum(totals[h], axis=1, keepdims=True) / pixels
            means = jnp.where(lane == h, mean, means)
        basin_ref[...] = jnp.transpose(means)[:hour_count, :]

    def piece_sums(d, g):
        sums = [jnp.zeros((piece_rows, tile_cols), jnp.float32)] * slots
        for i in range(members):
            for b in range(scan_block):
                hour = hours[plane * plane_scans + i * scan_block + b] - base_hour
                depth = depth_of(gather[d, i, b, piece(g)])
                for k in range(slots):
                    sums[k] = sums[k] + jnp.where(hour == k, depth, 0.0)
        return sums

    def push_piece(t, g):
        d = order[t]
        in_arrival(d, g).wait_recv()
        sums = piece_sums(d, g)
        for k in range(slots):
            part[d, k, piece(g)] = sums[k]
        for k in range(slots):

            @pl.when(k < span)
            def _():
                z_copy(d, g, k).start()

    for t in range(planes - 1):
        for g in range(PIECES):
            push_piece(t, g)
            if t == 0 and g == 0:
                reduce_segments()
            if t == planes - 2 and g == 0:
                pair_segments()
    basin_means()

    for p in range(planes):

        @pl.when(p != plane)
        def _():
            several(
                zrecv.at[p, pl.ds(0, hour_span(p))], z_send, z_recv.at[p]
            ).wait_recv()

    for h in range(hour_count):
        total = None
        for p in range(planes):
            if first_hour(p) <= h < first_hour(p) + hour_span(p):
                term = zrecv[p, h - first_hour(p)]
                total = term if total is None else total + term
        hourly_ref[h] = total

    for g in range(PIECES):
        in_arrival(plane, g).wait_recv()
        sums = piece_sums(plane, g)
        for k in range(slots):

            @pl.when(k < span)
            def _():
                hourly_ref[base_hour + k, piece(g)] += sums[k]

    several(plane_ids.at[pl.ds(0, members - 1)], id_send, id_recv).wait_send()
    several(all_ids.at[pl.ds(0, planes - 1)], idz_send, idz_recv).wait_send()
    several(seg_in.at[pl.ds(0, members - 1)], seg_send, seg_recv).wait_send()
    several(zseg.at[pl.ds(0, planes - 1)], zseg_send, zseg_recv).wait_send()
    several(gather.at[:, pl.ds(0, members - 1)], in_send, in_recv.at[0, 0]).wait_send()
    for n in sorted({hour_span(p) for p in range(planes)}):

        @pl.when(span == n)
        def _():
            several(
                part.at[pl.ds(0, planes - 1), pl.ds(0, n)], z_send, z_recv.at[0]
            ).wait_send()


def write_out(hourly_ref, basin_ref, hourly_out, basin_out, sem):
    pairs = ((hourly_ref, hourly_out), (basin_ref, basin_out))
    copies = [pltpu.make_async_copy(s, d, sem.at[n]) for n, (s, d) in enumerate(pairs)]
    for copy in copies:
        copy.start()
    for copy in copies:
        copy.wait()


def body(reflectivity, scan_hour, basin_ids):
    row_devices = lax.axis_size("row")
    col_devices = lax.axis_size("col")
    scan_block, grid_height, grid_width = reflectivity.shape
    tile_rows = grid_height // row_devices
    tile_cols = grid_width // col_devices
    scan_count = scan_hour.shape[0]
    hour_count = (scan_count + 10) // HOUR_SCANS + 1
    devices = row_devices * col_devices
    owned = grid_height * grid_width // (SEG * BASIN_ROWS) // devices
    planes = row_devices // CORES
    members = CORES * col_devices
    plane_scans = members * scan_block
    slots = max(
        hour_count
        - (scan_count - plane_scans * (p + 1)) // HOUR_SCANS
        - (p * plane_scans) // HOUR_SCANS
        for p in range(planes)
    )
    seg_shape = (grid_width // SEG, grid_height // CORES)
    dims = (row_devices, col_devices, hour_count, slots, tile_rows, tile_cols, owned)
    dma = pltpu.SemaphoreType.DMA
    f32 = jnp.float32
    anywhere = pl.BlockSpec(memory_space=pltpu.HBM)
    inside = pl.BlockSpec(memory_space=pltpu.VMEM)
    hourly, basin = pl.pallas_call(
        functools.partial(kernel, dims),
        out_shape=(
            jax.ShapeDtypeStruct((hour_count, tile_rows, tile_cols), f32),
            jax.ShapeDtypeStruct((hour_count, owned), f32),
        ),
        in_specs=[anywhere] * 3,
        out_specs=(inside, inside),
        scratch_shapes=[
            pltpu.VMEM(reflectivity.shape, f32),
            pltpu.SMEM(scan_hour.shape, jnp.int32),
            pltpu.VMEM(basin_ids.shape[::-1], jnp.int32),
            pltpu.VMEM((planes, members, scan_block, tile_rows, tile_cols), f32),
            pltpu.VMEM((planes, slots, tile_rows, tile_cols), f32),
            pltpu.VMEM((planes, slots, tile_rows, tile_cols), f32),
            pltpu.VMEM((members,) + basin_ids.shape[::-1], jnp.int32),
            pltpu.VMEM((planes, members) + basin_ids.shape[::-1], jnp.int32),
            pltpu.VMEM((CORES, scan_block) + seg_shape, f32),
            pltpu.VMEM((members, scan_block) + seg_shape, f32),
            pltpu.VMEM((slots,) + seg_shape, f32),
            pltpu.VMEM((planes, slots) + seg_shape, f32),
            pltpu.VMEM((CORES, hour_count) + seg_shape, f32),
            pltpu.SemaphoreType.REGULAR((2,)),
            dma((3,)),
            dma((planes,)),
            dma,
            dma,
            dma((planes, PIECES)),
            dma,
            dma((planes,)),
            dma,
            dma,
            dma,
            dma,
            dma,
            dma,
            dma,
            dma,
            dma,
            dma,
        ],
        compiler_params=pltpu.CompilerParams(
            collective_id=0, has_side_effects=True, vmem_limit_bytes=40 * 2**20
        ),
    )(*(pltpu.with_memory_space_constraint(v, pltpu.HBM) for v in (reflectivity, scan_hour, basin_ids.T)))
    hourly, basin = pl.pallas_call(
        write_out,
        out_shape=(
            jax.ShapeDtypeStruct(hourly.shape, f32),
            jax.ShapeDtypeStruct(basin.shape, f32),
        ),
        in_specs=[inside] * 2,
        out_specs=(anywhere, anywhere),
        scratch_shapes=[dma((2,))],
        compiler_params=pltpu.CompilerParams(vmem_limit_bytes=8 * 2**20),
    )(hourly, basin)
    return hourly, basin.T


def solution(mesh):
    placed = (P(("row", "col"), None, None), P(), P("row", "col"))
    return jax.shard_map(
        body,
        mesh=mesh,
        in_specs=placed,
        out_specs=(P(None, "row", "col"), P(("row", "col"), None)),
        check_vma=False,
    )
```

```python
import functools
import math

import jax
import jax.numpy as jnp
from jax import lax
from jax.experimental import pallas as pl
from jax.experimental.pallas import tpu as pltpu
from jax.sharding import PartitionSpec as P

SEG = 128
BASIN_ROWS = 8
HOUR_SCANS = 12
CORES = 2
LANES = 128
PIECES = 2
MESH = pl.DeviceIdType.MESH

slope_db = math.log(10.0) / 16.0
offset_zr = math.log(200.0) / 1.6 + math.log(12.0)


def kernel(
    dims,
    refl_ref,
    hour_ref,
    ids_ref,
    hourly_ref,
    basin_ref,
    frame,
    hours,
    ids,
    gather,
    part,
    zrecv,
    plane_ids,
    all_ids,
    seg_own,
    seg_in,
    seg_part,
    zseg,
    seg_hour,
    wave_sem,
    local_sem,
    load_sem,
    own_sem,
    in_send,
    in_recv,
    z_send,
    z_recv,
    id_send,
    id_recv,
    idz_send,
    idz_recv,
    seg_send,
    seg_recv,
    zseg_send,
    zseg_recv,
    pair_send,
    pair_recv,
):
    row_devices, col_devices, hour_count, slots, tile_rows, tile_cols, owned = dims
    planes = row_devices // CORES
    members = CORES * col_devices
    devices = row_devices * col_devices
    scan_block = gather.shape[2]
    scan_count = hour_ref.shape[0]
    plane_scans = members * scan_block
    piece_rows = tile_rows // PIECES
    all_segs, half_rows = seg_own.shape[2:]

    row = lax.axis_index("row")
    col = lax.axis_index("col")
    plane = row // CORES
    core = row % CORES
    mine = core * col_devices + col
    me = row * col_devices + col

    def first_hour(p):
        return (p * plane_scans) // HOUR_SCANS

    def hour_span(p):
        rest = scan_count - plane_scans - p * plane_scans
        return hour_count - rest // HOUR_SCANS - first_hour(p)

    def by_plane(table):
        value = table[0]
        for p in range(1, planes):
            value = jnp.where(plane == p, table[p], value)
        return value

    def chunk_order(p):
        others = sorted((d for d in range(planes) if d != p), key=lambda d: -abs(d - p))
        if 0 in others:
            others.remove(0)
            others.insert(0, 0)
        return others + [p]

    orders = [chunk_order(p) for p in range(planes)]
    order = [by_plane([o[t] for o in orders]) for t in range(planes)]

    def member_at(k):
        dc = k // col_devices
        dq = k % col_devices
        half = col_devices // 2
        qq = ((col // 2 + dq // 2) % half) * 2 + (col + dq) % 2
        other = ((core + dc) % CORES) * col_devices + qq
        return other, plane * CORES + other // col_devices, other % col_devices

    def several(ref, send_sem, recv_sem):
        return pltpu.make_async_remote_copy(
            src_ref=ref,
            dst_ref=ref,
            send_sem=send_sem,
            recv_sem=recv_sem,
            device_id=((row + 1) % row_devices, col),
            device_id_type=MESH,
        )

    def along_z(step):
        return ((plane + step) * CORES + core, col)

    barrier = pltpu.get_barrier_semaphore()
    for k in range(1, members):
        _, r, q = member_at(k)
        pl.semaphore_signal(barrier, inc=1, device_id=(r, q), device_id_type=MESH)

    greeter = core == CORES - 1
    below = greeter & (plane > 0)
    above = greeter & (plane < planes - 1)

    @pl.when(below)
    def _():
        pl.semaphore_signal(barrier, inc=1, device_id=along_z(-1), device_id_type=MESH)

    @pl.when(above)
    def _():
        pl.semaphore_signal(barrier, inc=1, device_id=along_z(1), device_id_type=MESH)

    def block_of(source, d, c, q):
        rows = pl.ds(pl.multiple_of((d * CORES + c) * tile_rows, 8), tile_rows)
        cols = pl.ds(pl.multiple_of(q * tile_cols, 128), tile_cols)
        return source.at[:, rows, cols]

    def plane_rows(d):
        rows = CORES * tile_rows
        return pl.ds(pl.multiple_of(d * rows, 8), rows)

    load_ids = pltpu.make_async_copy(ids_ref, ids, local_sem.at[0])
    load_ids.start()
    loads = []
    for t, d in enumerate(order):
        load = pltpu.make_async_copy(
            refl_ref.at[:, plane_rows(d), :],
            frame.at[:, plane_rows(d), :],
            load_sem.at[t],
        )
        load.start()
        loads.append(load)
    load_own_ids = pltpu.make_async_copy(
        ids_ref, plane_ids.at[mine], local_sem.at[1]
    )
    load_own_ids.start()
    load_hours = pltpu.make_async_copy(hour_ref, hours, local_sem.at[2])
    load_hours.start()
    for d in range(planes):
        own = pltpu.make_async_copy(
            block_of(refl_ref, d, core, col), gather.at[d, mine], own_sem
        )
        own.start()

    for k in range(slots):
        zrecv[plane, k] = jnp.zeros((tile_rows, tile_cols), jnp.float32)

    load_ids.wait()
    beside = jnp.where(below, 1, 0) + jnp.where(above, 1, 0)
    pl.semaphore_wait(barrier, members - 1 + beside)

    def id_copy(k):
        other, r, q = member_at(k)
        return pltpu.make_async_remote_copy(
            src_ref=ids,
            dst_ref=plane_ids.at[mine],
            send_sem=id_send,
            recv_sem=id_recv,
            device_id=(r, q),
            device_id_type=MESH,
        )

    for k in range(1, members):
        id_copy(k).start()

    @pl.when(greeter & (plane == 0))
    def _():
        pl.semaphore_signal(
            wave_sem.at[0], inc=1, device_id=along_z(1), device_id_type=MESH
        )

    @pl.when(greeter & (plane == planes - 1))
    def _():
        pl.semaphore_signal(
            wave_sem.at[1], inc=1, device_id=along_z(-1), device_id_type=MESH
        )

    def piece(g):
        return pl.ds(g * piece_rows, piece_rows)

    def in_copy(d, g, k):
        other, r, q = member_at(k)
        first = (d * CORES + other // col_devices) * tile_rows + g * piece_rows
        rows = pl.ds(pl.multiple_of(first, 8), piece_rows)
        cols = pl.ds(pl.multiple_of(q * tile_cols, 128), tile_cols)
        return pltpu.make_async_remote_copy(
            src_ref=frame.at[:, rows, cols],
            dst_ref=gather.at[d, mine, :, piece(g)],
            send_sem=in_send,
            recv_sem=in_recv.at[d, g],
            device_id=(r, q),
            device_id_type=MESH,
        )

    def in_arrival(d, g):
        ref = gather.at[d, pl.ds(0, members - 1), :, piece(g)]
        return several(ref, in_send, in_recv.at[d, g])

    far_first = sorted(range(1, members), key=lambda k: (-(k % col_devices), k))

    def send_piece(t, g):
        for k in far_first:
            in_copy(order[t], g, k).start()

    def seg_copy(k):
        other, r, q = member_at(k)
        return pltpu.make_async_remote_copy(
            src_ref=seg_own.at[other // col_devices],
            dst_ref=seg_in.at[mine],
            send_sem=seg_send,
            recv_sem=seg_recv,
            device_id=(r, q),
            device_id_type=MESH,
        )

    def depth_of(raw):
        return jnp.exp(raw * slope_db - offset_zr)

    def sum_segments():
        near_lane = lax.broadcasted_iota(jnp.int32, (SEG, LANES), 1)
        for b in range(scan_block):
            for c in range(CORES):
                rows = pl.ds(c * half_rows, half_rows)
                total = jnp.zeros((half_rows, LANES), jnp.float32)
                for g in range(all_segs):
                    rest = depth_of(frame[b, rows, g * SEG : (g + 1) * SEG])
                    ones = jnp.where(near_lane == g, 1.0, 0.0).astype(jnp.bfloat16)
                    for _ in range(3):
                        head = rest.astype(jnp.bfloat16)
                        rest = rest - head.astype(jnp.float32)
                        total = total + jnp.dot(
                            head, ones, preferred_element_type=jnp.float32
                        )
                seg_own[c, b] = jnp.transpose(total)[:all_segs]

    loads[0].wait()
    send_piece(0, 0)
    for load in loads[1:]:
        load.wait()
    sum_segments()
    for k in range(1, members):
        seg_copy(k).start()
    seg_in[mine] = seg_own[core]
    for t in range(planes):
        for g in range(PIECES):
            if t or g:
                send_piece(t, g)


    @pl.when(below)
    def _():
        pl.semaphore_wait(wave_sem.at[0], 1)

        @pl.when(above)
        def _():
            pl.semaphore_signal(
                wave_sem.at[0], inc=1, device_id=along_z(1), device_id_type=MESH
            )

    @pl.when(above)
    def _():
        pl.semaphore_wait(wave_sem.at[1], 1)

        @pl.when(below)
        def _():
            pl.semaphore_signal(
                wave_sem.at[1], inc=1, device_id=along_z(-1), device_id_type=MESH
            )

    @pl.when(greeter)
    def _():
        for c in range(CORES - 1):
            pl.semaphore_signal(
                wave_sem.at[2],
                inc=1,
                device_id=(plane * CORES + c, col),
                device_id_type=MESH,
            )

    @pl.when(jnp.logical_not(greeter))
    def _():
        pl.semaphore_wait(wave_sem.at[2], 1)

    several(plane_ids.at[pl.ds(0, members - 1)], id_send, id_recv).wait_recv()
    load_own_ids.wait()

    def idz_copy(k):
        other = (plane + k) % planes
        return pltpu.make_async_remote_copy(
            src_ref=plane_ids,
            dst_ref=all_ids.at[plane],
            send_sem=idz_send,
            recv_sem=idz_recv,
            device_id=(other * CORES + core, col),
            device_id_type=MESH,
        )

    for k in range(1, planes):
        idz_copy(k).start()
    all_ids[plane] = plane_ids[...]
    load_hours.wait()
    pltpu.make_async_copy(gather.at[:, 0], gather.at[:, 0], own_sem).wait()

    base_hour = first_hour(plane)
    span = hour_span(plane)

    def z_copy(d, g, k):
        return pltpu.make_async_remote_copy(
            src_ref=part.at[d, k, piece(g)],
            dst_ref=zrecv.at[plane, k, piece(g)],
            send_sem=z_send,
            recv_sem=z_recv.at[plane],
            device_id=(d * CORES + core, col),
            device_id_type=MESH,
        )

    def zseg_copy(k, n):
        other = (plane + k) % planes
        return pltpu.make_async_remote_copy(
            src_ref=seg_part.at[pl.ds(0, n)],
            dst_ref=zseg.at[pl.ds(plane * slots, n)],
            send_sem=zseg_send,
            recv_sem=zseg_recv,
            device_id=(other * CORES + core, col),
            device_id_type=MESH,
        )

    spans = sorted({hour_span(p) for p in range(planes)})

    def by_span(action):
        for n in spans:

            @pl.when(span == n)
            def _():
                action(n)

    def pair_copy():
        return pltpu.make_async_remote_copy(
            src_ref=seg_hour.at[core],
            dst_ref=seg_hour.at[core],
            send_sem=pair_send,
            recv_sem=pair_recv,
            device_id=(plane * CORES + 1 - core, col),
            device_id_type=MESH,
        )

    def reduce_segments():
        several(seg_in.at[pl.ds(0, members - 1)], seg_send, seg_recv).wait_recv()
        sums = [jnp.zeros((all_segs, half_rows), jnp.float32)] * slots
        for i in range(members):
            for b in range(scan_block):
                hour = hours[plane * plane_scans + i * scan_block + b] - base_hour
                for k in range(slots):
                    sums[k] = sums[k] + jnp.where(hour == k, seg_in[i, b], 0.0)
        for k in range(slots):
            seg_part[k] = sums[k]
            zseg[plane * slots + k] = sums[k]

        def send(n):
            for k in range(1, planes):
                zseg_copy(k, n).start()

        by_span(send)

    def pair_segments():
        for p in range(planes):
            n = sum(hour_span(o) for o in range(planes) if o != p)

            @pl.when(plane == p)
            def _():
                several(zseg.at[pl.ds(0, n)], zseg_send, zseg_recv).wait_recv()

        for h in range(hour_count):
            total = None
            for p in range(planes):
                if first_hour(p) <= h < first_hour(p) + hour_span(p):
                    term = zseg[p * slots + h - first_hour(p)]
                    total = term if total is None else total + term
            seg_hour[core, h] = total
        pair_copy().start()

    def basin_means():
        several(all_ids.at[pl.ds(0, planes - 1)], idz_send, idz_recv).wait_recv()
        pair_copy().wait()
        blocks = row_devices // CORES
        halves = []
        for c in range(CORES):
            lanes = []
            for r in range(c * blocks, (c + 1) * blocks):
                first = (r % CORES) * col_devices
                tiles = [all_ids[r // CORES, first + q] for q in range(col_devices)]
                lanes.append(jnp.concatenate(tiles, axis=0))
            halves.append(jnp.concatenate(lanes, axis=1))
        place = lax.broadcasted_iota(jnp.int32, (owned, half_rows), 0)
        zero = jnp.zeros((owned, half_rows), jnp.float32)
        totals = [zero] * hour_count
        count = zero
        for n in range(owned):
            hits = [half == me * owned + n for half in halves]
            for h in range(hour_count):
                kept = [jnp.where(hits[c], seg_hour[c, h], 0.0) for c in range(CORES)]
                kept = jnp.sum(sum(kept), axis=0, keepdims=True)
                totals[h] = jnp.where(place == n, kept, totals[h])
            found = sum(jnp.where(hit, float(SEG), 0.0) for hit in hits)
            count = jnp.where(place == n, jnp.sum(found, axis=0, keepdims=True), count)
        pixels = jnp.sum(count, axis=1, keepdims=True)
        lane = lax.broadcasted_iota(jnp.int32, (owned, LANES), 1)
        means = jnp.zeros((owned, LANES), jnp.float32)
        for h in range(hour_count):
            mean = jnp.sum(totals[h], axis=1, keepdims=True) / pixels
            means = jnp.where(lane == h, mean, means)
        basin_ref[...] = jnp.transpose(means)[:hour_count, :]

    def piece_sums(d, g):
        sums = [jnp.zeros((piece_rows, tile_cols), jnp.float32)] * slots
        for i in range(members):
            for b in range(scan_block):
                hour = hours[plane * plane_scans + i * scan_block + b] - base_hour
                depth = depth_of(gather[d, i, b, piece(g)])
                for k in range(slots):
                    sums[k] = sums[k] + jnp.where(hour == k, depth, 0.0)
        return sums

    def push_piece(t, g):
        d = order[t]
        in_arrival(d, g).wait_recv()
        sums = piece_sums(d, g)
        for k in range(slots):
            part[d, k, piece(g)] = sums[k]
        for k in range(slots):

            @pl.when(k < span)
            def _():
                z_copy(d, g, k).start()

    for t in range(planes - 1):
        for g in range(PIECES):
            push_piece(t, g)
            if t == 0 and g == 0:
                reduce_segments()
    pair_segments()
    basin_means()

    for p in range(planes):

        @pl.when(p != plane)
        def _():
            several(
                zrecv.at[p, pl.ds(0, hour_span(p))], z_send, z_recv.at[p]
            ).wait_recv()

    for h in range(hour_count):
        total = None
        for p in range(planes):
            if first_hour(p) <= h < first_hour(p) + hour_span(p):
                term = zrecv[p, h - first_hour(p)]
                total = term if total is None else total + term
        hourly_ref[h] = total

    for g in range(PIECES):
        in_arrival(plane, g).wait_recv()
        sums = piece_sums(plane, g)
        for k in range(slots):

            @pl.when(k < span)
            def _():
                hourly_ref[base_hour + k, piece(g)] += sums[k]

    several(plane_ids.at[pl.ds(0, members - 1)], id_send, id_recv).wait_send()
    several(all_ids.at[pl.ds(0, planes - 1)], idz_send, idz_recv).wait_send()
    several(seg_in.at[pl.ds(0, members - 1)], seg_send, seg_recv).wait_send()
    several(gather.at[:, pl.ds(0, members - 1)], in_send, in_recv.at[0, 0]).wait_send()

    def sums_sent(n):
        several(
            zseg.at[pl.ds(0, (planes - 1) * n)], zseg_send, zseg_recv
        ).wait_send()
        several(
            part.at[pl.ds(0, planes - 1), pl.ds(0, n)], z_send, z_recv.at[0]
        ).wait_send()

    by_span(sums_sent)


def write_out(hourly_ref, basin_ref, hourly_out, basin_out, sem):
    pairs = ((hourly_ref, hourly_out), (basin_ref, basin_out))
    copies = [pltpu.make_async_copy(s, d, sem.at[n]) for n, (s, d) in enumerate(pairs)]
    for copy in copies:
        copy.start()
    for copy in copies:
        copy.wait()


def body(reflectivity, scan_hour, basin_ids):
    row_devices = lax.axis_size("row")
    col_devices = lax.axis_size("col")
    scan_block, grid_height, grid_width = reflectivity.shape
    tile_rows = grid_height // row_devices
    tile_cols = grid_width // col_devices
    scan_count = scan_hour.shape[0]
    hour_count = (scan_count + 10) // HOUR_SCANS + 1
    devices = row_devices * col_devices
    owned = grid_height * grid_width // (SEG * BASIN_ROWS) // devices
    planes = row_devices // CORES
    members = CORES * col_devices
    plane_scans = members * scan_block
    slots = max(
        hour_count
        - (scan_count - plane_scans * (p + 1)) // HOUR_SCANS
        - (p * plane_scans) // HOUR_SCANS
        for p in range(planes)
    )
    seg_shape = (grid_width // SEG, grid_height // CORES)
    dims = (row_devices, col_devices, hour_count, slots, tile_rows, tile_cols, owned)
    dma = pltpu.SemaphoreType.DMA
    f32 = jnp.float32
    anywhere = pl.BlockSpec(memory_space=pltpu.HBM)
    inside = pl.BlockSpec(memory_space=pltpu.VMEM)
    hourly, basin = pl.pallas_call(
        functools.partial(kernel, dims),
        out_shape=(
            jax.ShapeDtypeStruct((hour_count, tile_rows, tile_cols), f32),
            jax.ShapeDtypeStruct((hour_count, owned), f32),
        ),
        in_specs=[anywhere] * 3,
        out_specs=(inside, inside),
        scratch_shapes=[
            pltpu.VMEM(reflectivity.shape, f32),
            pltpu.SMEM(scan_hour.shape, jnp.int32),
            pltpu.VMEM(basin_ids.shape[::-1], jnp.int32),
            pltpu.VMEM((planes, members, scan_block, tile_rows, tile_cols), f32),
            pltpu.VMEM((planes, slots, tile_rows, tile_cols), f32),
            pltpu.VMEM((planes, slots, tile_rows, tile_cols), f32),
            pltpu.VMEM((members,) + basin_ids.shape[::-1], jnp.int32),
            pltpu.VMEM((planes, members) + basin_ids.shape[::-1], jnp.int32),
            pltpu.VMEM((CORES, scan_block) + seg_shape, f32),
            pltpu.VMEM((members, scan_block) + seg_shape, f32),
            pltpu.VMEM((slots,) + seg_shape, f32),
            pltpu.VMEM((planes * slots,) + seg_shape, f32),
            pltpu.VMEM((CORES, hour_count) + seg_shape, f32),
            pltpu.SemaphoreType.REGULAR((3,)),
            dma((3,)),
            dma((planes,)),
            dma,
            dma,
            dma((planes, PIECES)),
            dma,
            dma((planes,)),
            dma,
            dma,
            dma,
            dma,
            dma,
            dma,
            dma,
            dma,
            dma,
            dma,
        ],
        compiler_params=pltpu.CompilerParams(
            collective_id=0, has_side_effects=True, vmem_limit_bytes=40 * 2**20
        ),
    )(*(pltpu.with_memory_space_constraint(v, pltpu.HBM) for v in (reflectivity, scan_hour, basin_ids.T)))
    hourly, basin = pl.pallas_call(
        write_out,
        out_shape=(
            jax.ShapeDtypeStruct(hourly.shape, f32),
            jax.ShapeDtypeStruct(basin.shape, f32),
        ),
        in_specs=[inside] * 2,
        out_specs=(anywhere, anywhere),
        scratch_shapes=[dma((2,))],
        compiler_params=pltpu.CompilerParams(vmem_limit_bytes=8 * 2**20),
    )(hourly, basin)
    return hourly, basin.T


def solution(mesh):
    placed = (P(("row", "col"), None, None), P(), P("row", "col"))
    return jax.shard_map(
        body,
        mesh=mesh,
        in_specs=placed,
        out_specs=(P(None, "row", "col"), P(("row", "col"), None)),
        check_vma=False,
    )
```

```python
import functools
import math

import jax
import jax.numpy as jnp
from jax import lax
from jax.experimental import pallas as pl
from jax.experimental.pallas import tpu as pltpu
from jax.sharding import PartitionSpec as P

SEG = 128
BASIN_ROWS = 8
HOUR_SCANS = 12
CORES = 2
LANES = 128
SWAP_ROWS = 8
SHARE_AT = (1, 2)
MESH = pl.DeviceIdType.MESH

slope_db = math.log(10.0) / 16.0
offset_zr = math.log(200.0) / 1.6 + math.log(12.0)


def kernel(
    dims,
    refl_ref,
    hour_ref,
    ids_ref,
    hourly_ref,
    basin_ref,
    frame,
    hours,
    ids,
    gather,
    part,
    zrecv,
    plane_ids,
    all_ids,
    seg_own,
    seg_in,
    seg_part,
    zseg,
    seg_hour,
    swap_in,
    gsum,
    grecv,
    gpart,
    zgrecv,
    wave_sem,
    local_sem,
    load_sem,
    own_sem,
    in_send,
    in_recv,
    z_send,
    z_recv,
    id_send,
    id_recv,
    idz_recv,
    seg_send,
    seg_recv,
    zseg_send,
    zseg_recv,
    pair_send,
    pair_recv,
    swap_send,
    swap_recv,
    g_send,
    g_recv,
    zg_send,
    zg_recv,
):
    row_devices, col_devices, hour_count, slots, tile_rows, tile_cols, owned = dims
    planes = row_devices // CORES
    pairs = planes // 2
    members = CORES * col_devices
    devices = row_devices * col_devices
    scan_block = gather.shape[2]
    scan_count = hour_ref.shape[0]
    plane_scans = members * scan_block
    direct = tile_rows - SWAP_ROWS
    pieces = ((0, 8), (8, direct - 8))
    all_segs, half_rows = seg_own.shape[2:]
    pair_slots = gsum.shape[1]

    row = lax.axis_index("row")
    col = lax.axis_index("col")
    plane = row // CORES
    core = row % CORES
    mine = core * col_devices + col
    me = row * col_devices + col
    pair = plane // 2
    parity = plane % 2
    twin = plane + 1 - 2 * parity

    def first_hour(p):
        return (p * plane_scans) // HOUR_SCANS

    def hour_span(p):
        rest = scan_count - plane_scans - p * plane_scans
        return hour_count - rest // HOUR_SCANS - first_hour(p)

    def pair_hours(j):
        return first_hour(2 * j + 1) + hour_span(2 * j + 1) - first_hour(2 * j)

    def by_plane(table):
        value = table[0]
        for p in range(1, planes):
            value = jnp.where(plane == p, table[p], value)
        return value

    def chunk_order(p):
        others = sorted((d for d in range(planes) if d != p), key=lambda d: -abs(d - p))
        if 0 in others:
            others.remove(0)
            others.insert(0, 0)
        return others + [p]

    orders = [chunk_order(p) for p in range(planes)]
    order = [by_plane([o[t] for o in orders]) for t in range(planes)]
    swaps = [(pair + 1 + n) % pairs for n in range(pairs)]

    def member_at(k):
        dc = k // col_devices
        dq = k % col_devices
        half = col_devices // 2
        qq = ((col // 2 + dq // 2) % half) * 2 + (col + dq) % 2
        other = ((core + dc) % CORES) * col_devices + qq
        return other, plane * CORES + other // col_devices, other % col_devices

    def several(ref, send_sem, recv_sem):
        return pltpu.make_async_remote_copy(
            src_ref=ref,
            dst_ref=ref,
            send_sem=send_sem,
            recv_sem=recv_sem,
            device_id=((row + 1) % row_devices, col),
            device_id_type=MESH,
        )

    def signal(sem, r, q):
        pl.semaphore_signal(sem, inc=1, device_id=(r, q), device_id_type=MESH)

    def row_at(p):
        return p * CORES + core

    barrier = pltpu.get_barrier_semaphore()
    for k in range(1, members):
        _, r, q = member_at(k)
        signal(barrier, r, q)

    greeter = core == CORES - 1
    below = greeter & (plane > 0)
    above = greeter & (plane < planes - 1)

    @pl.when(below)
    def _():
        signal(barrier, row_at(plane - 1), col)

    @pl.when(above)
    def _():
        signal(barrier, row_at(plane + 1), col)

    def tile_at(d, c):
        return pl.multiple_of((d * CORES + c) * tile_rows, 8)

    def lanes_of(q):
        return pl.ds(pl.multiple_of(q * tile_cols, 128), tile_cols)

    def plane_rows(d, count=1):
        rows = CORES * tile_rows
        return pl.ds(pl.multiple_of(d * rows, 8), rows * count)

    load_ids = pltpu.make_async_copy(ids_ref, ids, local_sem.at[0])
    load_ids.start()
    for t, d in enumerate(order):
        pltpu.make_async_copy(
            refl_ref.at[:, plane_rows(d), :],
            frame.at[:, plane_rows(d), :],
            load_sem.at[min(t, 1)],
        ).start()

    def frame_loaded(late):
        rows = frame.at[:, plane_rows(0, planes - 1 if late else 1), :]
        pltpu.make_async_copy(rows, rows, load_sem.at[late]).wait()

    load_hours = pltpu.make_async_copy(hour_ref, hours, local_sem.at[1])
    load_hours.start()
    for d in range(planes):
        rows = pl.ds(tile_at(d, core), direct)
        pltpu.make_async_copy(
            refl_ref.at[:, rows, lanes_of(col)], gather.at[d, mine], own_sem
        ).start()

    for k in range(slots):
        zrecv[plane * slots + k] = jnp.zeros((direct, tile_cols), jnp.float32)

    load_ids.wait()
    plane_ids[mine] = ids[...]
    beside = jnp.where(below, 1, 0) + jnp.where(above, 1, 0)
    pl.semaphore_wait(barrier, members - 1 + beside)

    def id_copy(k):
        other, r, q = member_at(k)
        return pltpu.make_async_remote_copy(
            src_ref=ids,
            dst_ref=plane_ids.at[mine],
            send_sem=id_send,
            recv_sem=id_recv,
            device_id=(r, q),
            device_id_type=MESH,
        )

    for k in range(1, members):
        id_copy(k).start()

    @pl.when(greeter)
    def _():
        signal(wave_sem.at[3], row_at(twin), col)

    @pl.when(greeter & (plane == 0))
    def _():
        signal(wave_sem.at[0], row_at(plane + 1), col)

    @pl.when(greeter & (plane == planes - 1))
    def _():
        signal(wave_sem.at[1], row_at(plane - 1), col)

    def piece(g):
        return pl.ds(*pieces[g])

    def in_copy(d, g, k):
        other, r, q = member_at(k)
        first, count = pieces[g]
        rows = pl.ds(pl.multiple_of(tile_at(d, other // col_devices) + first, 8), count)
        return pltpu.make_async_remote_copy(
            src_ref=frame.at[:, rows, lanes_of(q)],
            dst_ref=gather.at[d, mine, :, piece(g)],
            send_sem=in_send,
            recv_sem=in_recv.at[d, g],
            device_id=(r, q),
            device_id_type=MESH,
        )

    def in_arrival(d, g):
        ref = gather.at[d, pl.ds(0, members - 1), :, piece(g)]
        return several(ref, in_send, in_recv.at[d, g])

    far_first = sorted(range(1, members), key=lambda k: (-(k % col_devices), k))

    def send_piece(t, g):
        for k in far_first:
            in_copy(order[t], g, k).start()

    def seg_copy(k):
        other, r, q = member_at(k)
        return pltpu.make_async_remote_copy(
            src_ref=seg_own.at[other // col_devices],
            dst_ref=seg_in.at[mine],
            send_sem=seg_send,
            recv_sem=seg_recv,
            device_id=(r, q),
            device_id_type=MESH,
        )

    def depth_of(raw):
        return jnp.exp(raw * slope_db - offset_zr)

    def sum_segments():
        near_lane = lax.broadcasted_iota(jnp.int32, (SEG, LANES), 1)
        for b in range(scan_block):
            for c in range(CORES):
                rows = pl.ds(c * half_rows, half_rows)
                total = jnp.zeros((half_rows, LANES), jnp.float32)
                for g in range(all_segs):
                    rest = depth_of(frame[b, rows, g * SEG : (g + 1) * SEG])
                    ones = jnp.where(near_lane == g, 1.0, 0.0).astype(jnp.bfloat16)
                    for _ in range(3):
                        head = rest.astype(jnp.bfloat16)
                        rest = rest - head.astype(jnp.float32)
                        total = total + jnp.dot(
                            head, ones, preferred_element_type=jnp.float32
                        )
                seg_own[c, b] = jnp.transpose(total)[:all_segs]

    frame_loaded(0)
    send_piece(0, 0)
    frame_loaded(1)
    sum_segments()
    for k in range(1, members):
        seg_copy(k).start()
    seg_in[mine] = seg_own[core]
    send_piece(0, 1)
    for t in range(1, planes - 1):
        for g in range(len(pieces)):
            send_piece(t, g)
    send_piece(planes - 1, 0)

    def tell_core(sem):
        @pl.when(greeter)
        def _():
            for c in range(CORES - 1):
                signal(sem, plane * CORES + c, col)

        @pl.when(jnp.logical_not(greeter))
        def _():
            pl.semaphore_wait(sem, 1)


    @pl.when(greeter)
    def _():
        pl.semaphore_wait(wave_sem.at[3], 1)

    tell_core(wave_sem.at[4])

    def swap_rows(d, c):
        return pl.ds(pl.multiple_of(tile_at(d, c) + direct, 8), SWAP_ROWS)

    def swap_copy(j, d, c, p, slot):
        return pltpu.make_async_remote_copy(
            src_ref=frame.at[:, swap_rows(d, c), :],
            dst_ref=swap_in.at[j, slot],
            send_sem=swap_send,
            recv_sem=swap_recv.at[j],
            device_id=(p * CORES + c, col),
            device_id_type=MESH,
        )

    for j in swaps:
        for c in range(CORES):
            swap_copy(j, 2 * j + 1 - parity, c, twin, 1 + core).start()
    for j in swaps:
        swap_copy(j, 2 * j + parity, 1 - core, plane, 0).start()


    @pl.when(below)
    def _():
        pl.semaphore_wait(wave_sem.at[0], 1)

        @pl.when(above)
        def _():
            signal(wave_sem.at[0], row_at(plane + 1), col)

    @pl.when(above)
    def _():
        pl.semaphore_wait(wave_sem.at[1], 1)

        @pl.when(below)
        def _():
            signal(wave_sem.at[1], row_at(plane - 1), col)

    tell_core(wave_sem.at[2])

    several(plane_ids.at[pl.ds(0, members - 1)], id_send, id_recv).wait_recv()

    plane_block = pl.ds(plane * members, members)
    for k in range(1, planes):
        pltpu.make_async_remote_copy(
            src_ref=plane_ids,
            dst_ref=all_ids.at[plane_block],
            send_sem=id_send,
            recv_sem=idz_recv,
            device_id=(row_at((plane + k) % planes), col),
            device_id_type=MESH,
        ).start()
    all_ids[plane_block] = plane_ids[...]
    load_hours.wait()
    pltpu.make_async_copy(gather.at[:, 0], gather.at[:, 0], own_sem).wait()

    base_hour = first_hour(plane)
    span = hour_span(plane)
    pair_base = first_hour(2 * pair)
    spans = sorted({hour_span(p) for p in range(planes)})

    def by_span(action):
        for n in spans:

            @pl.when(span == n)
            def _():
                action(n)

    def z_copy(d, g, k):
        return pltpu.make_async_remote_copy(
            src_ref=part.at[d, k, piece(g)],
            dst_ref=zrecv.at[plane * slots + k, piece(g)],
            send_sem=z_send,
            recv_sem=z_recv,
            device_id=(row_at(d), col),
            device_id_type=MESH,
        )

    def zseg_copy(k, n):
        return pltpu.make_async_remote_copy(
            src_ref=seg_part.at[pl.ds(0, n)],
            dst_ref=zseg.at[pl.ds(plane * slots, n)],
            send_sem=zseg_send,
            recv_sem=zseg_recv,
            device_id=(row_at((plane + k) % planes), col),
            device_id_type=MESH,
        )

    def pair_copy():
        return pltpu.make_async_remote_copy(
            src_ref=seg_hour.at[core],
            dst_ref=seg_hour.at[core],
            send_sem=pair_send,
            recv_sem=pair_recv,
            device_id=(plane * CORES + 1 - core, col),
            device_id_type=MESH,
        )

    def wait_slots(ref, send_sem, recv_sem):
        for p in range(planes):
            n = sum(hour_span(o) for o in range(planes) if o != p)

            @pl.when(plane == p)
            def _():
                several(ref.at[pl.ds(0, n)], send_sem, recv_sem).wait_recv()

    def sum_planes(ref, h):
        total = None
        for p in range(planes):
            if first_hour(p) <= h < first_hour(p) + hour_span(p):
                term = ref[p * slots + h - first_hour(p)]
                total = term if total is None else total + term
        return total

    def add_by_hour(sums, raw, p, member, b, base):
        hour = hours[p * plane_scans + member * scan_block + b] - base
        return [
            total + jnp.where(hour == k, raw, 0.0) for k, total in enumerate(sums)
        ]

    def reduce_segments():
        several(seg_in.at[pl.ds(0, members - 1)], seg_send, seg_recv).wait_recv()
        sums = [jnp.zeros((all_segs, half_rows), jnp.float32)] * slots
        for i in range(members):
            for b in range(scan_block):
                sums = add_by_hour(sums, seg_in[i, b], plane, i, b, base_hour)
        for k in range(slots):
            seg_part[k] = sums[k]
            zseg[plane * slots + k] = sums[k]

        def send(n):
            for k in range(1, planes):
                zseg_copy(k, n).start()

        by_span(send)

    def pair_segments():
        wait_slots(zseg, zseg_send, zseg_recv)
        for h in range(hour_count):
            seg_hour[core, h] = sum_planes(zseg, h)
        pair_copy().start()

    def basin_means():
        several(
            all_ids.at[pl.ds(0, (planes - 1) * members)], id_send, idz_recv
        ).wait_recv()
        pair_copy().wait()
        blocks = row_devices // CORES
        halves = []
        for c in range(CORES):
            lanes = []
            for r in range(c * blocks, (c + 1) * blocks):
                first = r * col_devices
                tiles = [all_ids[first + q] for q in range(col_devices)]
                lanes.append(jnp.concatenate(tiles, axis=0))
            halves.append(jnp.concatenate(lanes, axis=1))
        place = lax.broadcasted_iota(jnp.int32, (owned, half_rows), 0)
        zero = jnp.zeros((owned, half_rows), jnp.float32)
        totals = [zero] * hour_count
        count = zero
        for n in range(owned):
            hits = [half == me * owned + n for half in halves]
            for h in range(hour_count):
                kept = [jnp.where(hits[c], seg_hour[c, h], 0.0) for c in range(CORES)]
                kept = jnp.sum(sum(kept), axis=0, keepdims=True)
                totals[h] = jnp.where(place == n, kept, totals[h])
            found = sum(jnp.where(hit, float(SEG), 0.0) for hit in hits)
            count = jnp.where(place == n, jnp.sum(found, axis=0, keepdims=True), count)
        pixels = jnp.sum(count, axis=1, keepdims=True)
        lane = lax.broadcasted_iota(jnp.int32, (owned, LANES), 1)
        means = jnp.zeros((owned, LANES), jnp.float32)
        for h in range(hour_count):
            mean = jnp.sum(totals[h], axis=1, keepdims=True) / pixels
            means = jnp.where(lane == h, mean, means)
        basin_ref[...] = jnp.transpose(means)[:hour_count, :]

    def piece_sums(d, g):
        sums = [jnp.zeros((pieces[g][1], tile_cols), jnp.float32)] * slots
        for i in range(members):
            for b in range(scan_block):
                depth = depth_of(gather[d, i, b, piece(g)])
                sums = add_by_hour(sums, depth, plane, i, b, base_hour)
        return sums

    def push_piece(t, g):
        d = order[t]
        in_arrival(d, g).wait_recv()
        sums = piece_sums(d, g)
        for k in range(slots):
            part[d, k, piece(g)] = sums[k]
        for k in range(slots):

            @pl.when(k < span)
            def _():
                z_copy(d, g, k).start()

    def share_swap(n):
        j = swaps[n]
        several(swap_in.at[j], swap_send, swap_recv.at[j]).wait_recv()
        sums = [jnp.zeros((SWAP_ROWS, frame.shape[2]), jnp.float32)] * pair_slots
        for b in range(scan_block):
            own = frame[b, swap_rows(2 * j + parity, core), :]
            sources = (
                (own, plane, core),
                (swap_in[j, 0, b], plane, 1 - core),
                (swap_in[j, 1, b], twin, 0),
                (swap_in[j, 2, b], twin, 1),
            )
            for raw, p, c in sources:
                member = c * col_devices + col
                sums = add_by_hour(sums, depth_of(raw), p, member, b, pair_base)
        for k in range(pair_slots):
            gsum[j, k] = sums[k]
        for k in range(col_devices - 1, 0, -1):
            _, r, q = member_at(k)
            pltpu.make_async_remote_copy(
                src_ref=gsum.at[j, :, :, lanes_of(q)],
                dst_ref=grecv.at[j, col],
                send_sem=g_send,
                recv_sem=g_recv.at[j],
                device_id=(r, q),
                device_id_type=MESH,
            ).start()

    def join_swap(n):
        j = swaps[n]
        several(
            grecv.at[j, pl.ds(0, col_devices - 1)], g_send, g_recv.at[j]
        ).wait_recv()
        totals = []
        for k in range(pair_slots):
            total = gsum[j, k, :, lanes_of(col)]
            for m in range(1, col_devices):
                _, _, q = member_at(m)
                total = total + grecv[j, q, k]
            totals.append(total)
        if n < pairs - 1:
            for k in range(pair_slots):
                gpart[j, k] = totals[k]
            pltpu.make_async_remote_copy(
                src_ref=gpart.at[j],
                dst_ref=zgrecv.at[pair],
                send_sem=zg_send,
                recv_sem=zg_recv,
                device_id=(row_at(2 * j + parity), col),
                device_id_type=MESH,
            ).start()
        else:
            for k in range(pair_slots):
                zgrecv[pair, k] = totals[k]

    pushes = [(t, g) for t in range(planes - 1) for g in range(len(pieces))]
    for n, (t, g) in enumerate(pushes):
        push_piece(t, g)
        if n == 0:
            reduce_segments()
        if n in SHARE_AT:
            share_swap(SHARE_AT.index(n))
        if n == SHARE_AT[-1]:
            for m in range(len(SHARE_AT), pairs):
                share_swap(m)
            send_piece(planes - 1, 1)
    for n in range(pairs - 1):
        join_swap(n)
    pair_segments()
    basin_means()
    join_swap(pairs - 1)

    wait_slots(zrecv, z_send, z_recv)
    several(zgrecv.at[pl.ds(0, pairs - 1)], zg_send, zg_recv).wait_recv()
    for h in range(hour_count):
        hourly_ref[h, :direct] = sum_planes(zrecv, h)
        total = None
        for j in range(pairs):
            if first_hour(2 * j) <= h < first_hour(2 * j) + pair_hours(j):
                term = zgrecv[j, h - first_hour(2 * j)]
                total = term if total is None else total + term
        hourly_ref[h, direct:] = total

    for g in range(len(pieces)):
        in_arrival(plane, g).wait_recv()
        sums = piece_sums(plane, g)
        for k in range(slots):

            @pl.when(k < span)
            def _():
                hourly_ref[base_hour + k, piece(g)] += sums[k]

    several(
        all_ids.at[pl.ds(0, planes * members - 1)], id_send, id_recv
    ).wait_send()
    several(seg_in.at[pl.ds(0, members - 1)], seg_send, seg_recv).wait_send()
    several(
        gather.at[:, pl.ds(0, members - 1)], in_send, in_recv.at[0, 0]
    ).wait_send()
    several(swap_in, swap_send, swap_recv.at[0]).wait_send()
    several(
        grecv.at[:, pl.ds(0, col_devices - 1)], g_send, g_recv.at[0]
    ).wait_send()
    several(gpart.at[pl.ds(0, pairs - 1)], zg_send, zg_recv).wait_send()

    def sums_sent(n):
        several(
            zseg.at[pl.ds(0, (planes - 1) * n)], zseg_send, zseg_recv
        ).wait_send()
        several(
            part.at[pl.ds(0, planes - 1), pl.ds(0, n)], z_send, z_recv
        ).wait_send()

    by_span(sums_sent)


def write_out(hourly_ref, basin_ref, hourly_out, basin_out, sem):
    pairs = ((hourly_ref, hourly_out), (basin_ref, basin_out))
    copies = [pltpu.make_async_copy(s, d, sem.at[n]) for n, (s, d) in enumerate(pairs)]
    for copy in copies:
        copy.start()
    for copy in copies:
        copy.wait()


def body(reflectivity, scan_hour, basin_ids):
    row_devices = lax.axis_size("row")
    col_devices = lax.axis_size("col")
    scan_block, grid_height, grid_width = reflectivity.shape
    tile_rows = grid_height // row_devices
    tile_cols = grid_width // col_devices
    scan_count = scan_hour.shape[0]
    hour_count = (scan_count + 10) // HOUR_SCANS + 1
    devices = row_devices * col_devices
    owned = grid_height * grid_width // (SEG * BASIN_ROWS) // devices
    planes = row_devices // CORES
    pairs = planes // 2
    members = CORES * col_devices
    plane_scans = members * scan_block

    def span_of(first, last):
        rest = scan_count - plane_scans * (last + 1)
        return hour_count - rest // HOUR_SCANS - (first * plane_scans) // HOUR_SCANS

    slots = max(span_of(p, p) for p in range(planes))
    pair_slots = max(span_of(2 * j, 2 * j + 1) for j in range(pairs))
    seg_shape = (grid_width // SEG, grid_height // CORES)
    dims = (row_devices, col_devices, hour_count, slots, tile_rows, tile_cols, owned)
    direct = tile_rows - SWAP_ROWS
    dma = pltpu.SemaphoreType.DMA
    f32 = jnp.float32
    id_shape = basin_ids.shape[::-1]
    anywhere = pl.BlockSpec(memory_space=pltpu.HBM)
    inside = pl.BlockSpec(memory_space=pltpu.VMEM)
    hourly, basin = pl.pallas_call(
        functools.partial(kernel, dims),
        out_shape=(
            jax.ShapeDtypeStruct((hour_count, tile_rows, tile_cols), f32),
            jax.ShapeDtypeStruct((hour_count, owned), f32),
        ),
        in_specs=[anywhere] * 3,
        out_specs=(inside, inside),
        scratch_shapes=[
            pltpu.VMEM(reflectivity.shape, f32),
            pltpu.SMEM(scan_hour.shape, jnp.int32),
            pltpu.VMEM(id_shape, jnp.int32),
            pltpu.VMEM((planes, members, scan_block, direct, tile_cols), f32),
            pltpu.VMEM((planes, slots, direct, tile_cols), f32),
            pltpu.VMEM((planes * slots, direct, tile_cols), f32),
            pltpu.VMEM((members,) + id_shape, jnp.int32),
            pltpu.VMEM((planes * members,) + id_shape, jnp.int32),
            pltpu.VMEM((CORES, scan_block) + seg_shape, f32),
            pltpu.VMEM((members, scan_block) + seg_shape, f32),
            pltpu.VMEM((slots,) + seg_shape, f32),
            pltpu.VMEM((planes * slots,) + seg_shape, f32),
            pltpu.VMEM((CORES, hour_count) + seg_shape, f32),
            pltpu.VMEM((pairs, CORES + 1, scan_block, SWAP_ROWS, grid_width), f32),
            pltpu.VMEM((pairs, pair_slots, SWAP_ROWS, grid_width), f32),
            pltpu.VMEM((pairs, col_devices, pair_slots, SWAP_ROWS, tile_cols), f32),
            pltpu.VMEM((pairs, pair_slots, SWAP_ROWS, tile_cols), f32),
            pltpu.VMEM((pairs, pair_slots, SWAP_ROWS, tile_cols), f32),
            pltpu.SemaphoreType.REGULAR((5,)),
            dma((2,)),
            dma((2,)),
            dma,
            dma,
            dma((planes, 2)),
            dma,
            dma,
            dma,
            dma,
            dma,
            dma,
            dma,
            dma,
            dma,
            dma,
            dma,
            dma,
            dma((pairs,)),
            dma,
            dma((pairs,)),
            dma,
            dma,
        ],
        compiler_params=pltpu.CompilerParams(
            collective_id=0, has_side_effects=True, vmem_limit_bytes=40 * 2**20
        ),
    )(*(pltpu.with_memory_space_constraint(v, pltpu.HBM) for v in (reflectivity, scan_hour, basin_ids.T)))
    hourly, basin = pl.pallas_call(
        write_out,
        out_shape=(
            jax.ShapeDtypeStruct(hourly.shape, f32),
            jax.ShapeDtypeStruct(basin.shape, f32),
        ),
        in_specs=[inside] * 2,
        out_specs=(anywhere, anywhere),
        scratch_shapes=[dma((2,))],
        compiler_params=pltpu.CompilerParams(vmem_limit_bytes=8 * 2**20),
    )(hourly, basin)
    return hourly, basin.T


def solution(mesh):
    placed = (P(("row", "col"), None, None), P(), P("row", "col"))
    return jax.shard_map(
        body,
        mesh=mesh,
        in_specs=placed,
        out_specs=(P(None, "row", "col"), P(("row", "col"), None)),
        check_vma=False,
    )
```

```python
import functools
import math

import jax
import jax.numpy as jnp
from jax import lax
from jax.experimental import pallas as pl
from jax.experimental.pallas import tpu as pltpu
from jax.sharding import PartitionSpec as P

SEG = 128
BASIN_ROWS = 8
HOUR_SCANS = 12
CORES = 2
LANES = 128
FIRST = (8, 16, 32)
LATER = (16, 32)
OWN = (16,)
SWAP_ROWS = 16
SHARE_AFTER = 1
MESH = pl.DeviceIdType.MESH

slope_db = math.log(10.0) / 16.0
offset_zr = math.log(200.0) / 1.6 + math.log(12.0)


def kernel(
    dims,
    refl_ref,
    hour_ref,
    ids_ref,
    hourly_ref,
    basin_ref,
    frame,
    hours,
    ids,
    gather,
    part,
    zrecv,
    plane_ids,
    all_ids,
    seg_own,
    seg_in,
    seg_part,
    zseg,
    seg_hour,
    swap_in,
    gsum,
    grecv,
    wave_sem,
    local_sem,
    load_sem,
    in_send,
    in_recv,
    z_send,
    z_recv,
    id_send,
    id_recv,
    idz_recv,
    seg_send,
    seg_recv,
    zseg_send,
    zseg_recv,
    pair_send,
    pair_recv,
    swap_send,
    swap_recv,
    g_send,
    g_recv,
):
    row_devices, col_devices, hour_count, slots, tile_rows, tile_cols, owned = dims
    planes = row_devices // CORES
    members = CORES * col_devices
    devices = row_devices * col_devices
    scan_block = gather.shape[2]
    scan_count = hour_ref.shape[0]
    plane_scans = members * scan_block
    cuts = [FIRST] + [LATER] * (planes - 2) + [OWN]
    pieces = [list(zip((0,) + ends[:-1], ends)) for ends in cuts]
    piece_sem = [sum(map(len, cuts[:t])) for t in range(planes)]
    all_segs, half_rows = seg_own.shape[2:]
    kept_rows = tile_rows - SWAP_ROWS
    pair_slots = gsum.shape[1]

    row = lax.axis_index("row")
    col = lax.axis_index("col")
    plane = row // CORES
    core = row % CORES
    mine = core * col_devices + col
    me = row * col_devices + col
    pair = plane // 2
    twin = plane + 1 - 2 * (plane % 2)

    def first_hour(p):
        return (p * plane_scans) // HOUR_SCANS

    def hour_span(p):
        rest = scan_count - plane_scans - p * plane_scans
        return hour_count - rest // HOUR_SCANS - first_hour(p)

    def pair_span(j):
        return first_hour(2 * j + 1) + hour_span(2 * j + 1) - first_hour(2 * j)

    def by_plane(table):
        value = table[0]
        for p in range(1, planes):
            value = jnp.where(plane == p, table[p], value)
        return value

    def chunk_order(p):
        others = sorted((d for d in range(planes) if d != p), key=lambda d: -abs(d - p))
        if 0 in others:
            others.remove(0)
            others.insert(0, 0)
        return others + [p]

    orders = [chunk_order(p) for p in range(planes)]
    order = [by_plane([o[t] for o in orders]) for t in range(planes)]
    whole = [order[t] != twin for t in range(planes)]

    def member_at(k):
        dc = k // col_devices
        dq = k % col_devices
        half = col_devices // 2
        qq = ((col // 2 + dq // 2) % half) * 2 + (col + dq) % 2
        other = ((core + dc) % CORES) * col_devices + qq
        return other, plane * CORES + other // col_devices, other % col_devices

    def several(ref, send_sem, recv_sem):
        return pltpu.make_async_remote_copy(
            src_ref=ref,
            dst_ref=ref,
            send_sem=send_sem,
            recv_sem=recv_sem,
            device_id=((row + 1) % row_devices, col),
            device_id_type=MESH,
        )

    def signal(sem, r, q):
        pl.semaphore_signal(sem, inc=1, device_id=(r, q), device_id_type=MESH)

    def row_at(p):
        return p * CORES + core

    barrier = pltpu.get_barrier_semaphore()
    far_first = sorted(range(1, members), key=lambda k: (-(k % col_devices), k))
    for k in far_first:
        _, r, q = member_at(k)
        signal(barrier, r, q)

    greeter = core == CORES - 1
    below = greeter & (plane > 0)
    above = greeter & (plane < planes - 1)

    @pl.when(below)
    def _():
        signal(barrier, row_at(plane - 1), col)

    @pl.when(above)
    def _():
        signal(barrier, row_at(plane + 1), col)

    def tile_at(d, c):
        return pl.multiple_of((d * CORES + c) * tile_rows, 8)

    def lanes_of(q):
        return pl.ds(pl.multiple_of(q * tile_cols, 128), tile_cols)

    def plane_rows(d):
        rows = CORES * tile_rows
        return pl.ds(pl.multiple_of(d * rows, 8), rows)

    load_ids = pltpu.make_async_copy(ids_ref, ids, local_sem.at[0])
    load_ids.start()
    for t, d in enumerate(order):
        pltpu.make_async_copy(
            refl_ref.at[:, plane_rows(d), :],
            frame.at[:, plane_rows(d), :],
            load_sem.at[min(t, 1)],
        ).start()

    def frame_loaded(late):
        count = (planes - 1 if late else 1) * CORES * tile_rows
        rows = frame.at[:, pl.ds(0, count), :]
        pltpu.make_async_copy(rows, rows, load_sem.at[late]).wait()

    load_hours = pltpu.make_async_copy(hour_ref, hours, local_sem.at[1])
    load_hours.start()
    for k in range(slots):
        zrecv[plane * slots + k] = jnp.zeros((tile_rows, tile_cols), jnp.float32)
        zrecv[twin * slots + k, kept_rows:] = jnp.zeros(
            (SWAP_ROWS, tile_cols), jnp.float32
        )

    load_ids.wait()
    plane_ids[mine] = ids[...]
    beside = jnp.where(below, 1, 0) + jnp.where(above, 1, 0)
    pl.semaphore_wait(barrier, members - 1 + beside)

    def id_copy(k):
        other, r, q = member_at(k)
        return pltpu.make_async_remote_copy(
            src_ref=ids,
            dst_ref=plane_ids.at[mine],
            send_sem=id_send,
            recv_sem=id_recv,
            device_id=(r, q),
            device_id_type=MESH,
        )

    for k in range(1, members):
        id_copy(k).start()

    @pl.when(greeter)
    def _():
        signal(wave_sem.at[3], row_at(twin), col)

    @pl.when(greeter & (plane == 0))
    def _():
        signal(wave_sem.at[0], row_at(plane + 1), col)

    @pl.when(greeter & (plane == planes - 1))
    def _():
        signal(wave_sem.at[1], row_at(plane - 1), col)

    def piece(t, g):
        first, end = pieces[t][g]
        return pl.ds(first, end - first)

    def in_copy(t, g, k):
        other, r, q = member_at(k)
        d = order[t]
        first, end = pieces[t][g]
        top = pl.multiple_of(tile_at(d, other // col_devices) + first, 8)
        return pltpu.make_async_remote_copy(
            src_ref=frame.at[:, pl.ds(top, end - first), lanes_of(q)],
            dst_ref=gather.at[d, mine, :, piece(t, g)],
            send_sem=in_send,
            recv_sem=in_recv.at[piece_sem[t] + g],
            device_id=(r, q),
            device_id_type=MESH,
        )

    def in_arrival(t, g):
        ref = gather.at[order[t], pl.ds(0, members - 1), :, piece(t, g)]
        return several(ref, in_send, in_recv.at[piece_sem[t] + g])

    def if_sent(t, g, action):
        if pieces[t][g][0] < kept_rows:
            action(t, g)
        else:

            @pl.when(whole[t])
            def _():
                action(t, g)

    def send_piece(t, g):
        for k in far_first:
            in_copy(t, g, k).start()

    def seg_copy(k):
        other, r, q = member_at(k)
        return pltpu.make_async_remote_copy(
            src_ref=seg_own.at[other // col_devices],
            dst_ref=seg_in.at[mine],
            send_sem=seg_send,
            recv_sem=seg_recv,
            device_id=(r, q),
            device_id_type=MESH,
        )

    def depth_of(raw):
        return jnp.exp(raw * slope_db - offset_zr)

    def sum_segments():
        near_lane = lax.broadcasted_iota(jnp.int32, (SEG, LANES), 1)
        for b in range(scan_block):
            for c in range(CORES):
                rows = pl.ds(c * half_rows, half_rows)
                total = jnp.zeros((half_rows, LANES), jnp.float32)
                for g in range(all_segs):
                    rest = depth_of(frame[b, rows, g * SEG : (g + 1) * SEG])
                    ones = jnp.where(near_lane == g, 1.0, 0.0).astype(jnp.bfloat16)
                    for _ in range(3):
                        head = rest.astype(jnp.bfloat16)
                        rest = rest - head.astype(jnp.float32)
                        total = total + jnp.dot(
                            head, ones, preferred_element_type=jnp.float32
                        )
                seg_own[c, b] = jnp.transpose(total)[:all_segs]

    frame_loaded(0)
    send_piece(0, 0)
    frame_loaded(1)
    sum_segments()
    for k in range(1, members):
        seg_copy(k).start()
    seg_in[mine] = seg_own[core]
    for t in range(planes):
        for g in range(len(pieces[t])):
            if t or g:
                if_sent(t, g, send_piece)

    for d in range(planes):
        rows = pl.ds(tile_at(d, core), tile_rows)
        gather[d, mine] = frame[:, rows, lanes_of(col)]

    def tell_core(sem):
        @pl.when(greeter)
        def _():
            for c in range(CORES - 1):
                signal(sem, plane * CORES + c, col)

        @pl.when(jnp.logical_not(greeter))
        def _():
            pl.semaphore_wait(sem, 1)


    @pl.when(greeter)
    def _():
        pl.semaphore_wait(wave_sem.at[3], 1)

    tell_core(wave_sem.at[4])

    def swap_rows(d, c):
        return pl.ds(pl.multiple_of(tile_at(d, c) + kept_rows, 8), SWAP_ROWS)

    def swap_copy(d, c, slot):
        return pltpu.make_async_remote_copy(
            src_ref=frame.at[:, swap_rows(d, c), :],
            dst_ref=swap_in.at[slot],
            send_sem=swap_send,
            recv_sem=swap_recv,
            device_id=(d * CORES + c, col),
            device_id_type=MESH,
        )

    for c in range(CORES):
        swap_copy(twin, c, 1 + core).start()
    swap_copy(plane, 1 - core, 0).start()


    @pl.when(below)
    def _():
        pl.semaphore_wait(wave_sem.at[0], 1)

        @pl.when(above)
        def _():
            signal(wave_sem.at[0], row_at(plane + 1), col)

    @pl.when(above)
    def _():
        pl.semaphore_wait(wave_sem.at[1], 1)

        @pl.when(below)
        def _():
            signal(wave_sem.at[1], row_at(plane - 1), col)

    tell_core(wave_sem.at[2])

    several(plane_ids.at[pl.ds(0, members - 1)], id_send, id_recv).wait_recv()

    plane_block = pl.ds(plane * members, members)
    for k in range(1, planes):
        pltpu.make_async_remote_copy(
            src_ref=plane_ids,
            dst_ref=all_ids.at[plane_block],
            send_sem=id_send,
            recv_sem=idz_recv,
            device_id=(row_at((plane + k) % planes), col),
            device_id_type=MESH,
        ).start()
    all_ids[plane_block] = plane_ids[...]
    load_hours.wait()

    base_hour = first_hour(plane)
    span = hour_span(plane)
    pair_base = first_hour(2 * pair)
    spans = sorted({hour_span(p) for p in range(planes)})

    def by_span(action):
        for n in spans:

            @pl.when(span == n)
            def _():
                action(n)

    def side(p):
        return jnp.where(p == twin, 1, 0)

    def z_copy(t, g, k):
        return pltpu.make_async_remote_copy(
            src_ref=part.at[order[t], k, piece(t, g)],
            dst_ref=zrecv.at[plane * slots + k, piece(t, g)],
            send_sem=z_send.at[side(order[t])],
            recv_sem=z_recv.at[side(order[t])],
            device_id=(row_at(order[t]), col),
            device_id_type=MESH,
        )

    def zseg_copy(k, n):
        return pltpu.make_async_remote_copy(
            src_ref=seg_part.at[pl.ds(0, n)],
            dst_ref=zseg.at[pl.ds(plane * slots, n)],
            send_sem=zseg_send,
            recv_sem=zseg_recv,
            device_id=(row_at((plane + k) % planes), col),
            device_id_type=MESH,
        )

    def pair_copy():
        return pltpu.make_async_remote_copy(
            src_ref=seg_hour.at[core],
            dst_ref=seg_hour.at[core],
            send_sem=pair_send,
            recv_sem=pair_recv,
            device_id=(plane * CORES + 1 - core, col),
            device_id_type=MESH,
        )

    def wait_slots(ref, send_sem, recv_sem):
        for p in range(planes):
            n = sum(hour_span(o) for o in range(planes) if o != p)

            @pl.when(plane == p)
            def _():
                several(ref.at[pl.ds(0, n)], send_sem, recv_sem).wait_recv()

    def sum_planes(ref, h):
        total = None
        for p in range(planes):
            if first_hour(p) <= h < first_hour(p) + hour_span(p):
                term = ref[p * slots + h - first_hour(p)]
                total = term if total is None else total + term
        return total

    def add_by_hour(sums, raw, p, member, b, base):
        hour = hours[p * plane_scans + member * scan_block + b] - base
        return [
            total + jnp.where(hour == k, raw, 0.0) for k, total in enumerate(sums)
        ]

    def reduce_segments():
        several(seg_in.at[pl.ds(0, members - 1)], seg_send, seg_recv).wait_recv()
        sums = [jnp.zeros((all_segs, half_rows), jnp.float32)] * slots
        for i in range(members):
            for b in range(scan_block):
                sums = add_by_hour(sums, seg_in[i, b], plane, i, b, base_hour)
        for k in range(slots):
            seg_part[k] = sums[k]
            zseg[plane * slots + k] = sums[k]

        def send(n):
            for k in range(1, planes):
                zseg_copy(k, n).start()

        by_span(send)

    def pair_segments():
        wait_slots(zseg, zseg_send, zseg_recv)
        for h in range(hour_count):
            seg_hour[core, h] = sum_planes(zseg, h)
        pair_copy().start()

    def basin_means():
        several(
            all_ids.at[pl.ds(0, (planes - 1) * members)], id_send, idz_recv
        ).wait_recv()
        pair_copy().wait()
        blocks = row_devices // CORES
        halves = []
        for c in range(CORES):
            lanes = []
            for r in range(c * blocks, (c + 1) * blocks):
                first = r * col_devices
                tiles = [all_ids[first + q] for q in range(col_devices)]
                lanes.append(jnp.concatenate(tiles, axis=0))
            halves.append(jnp.concatenate(lanes, axis=1))
        place = lax.broadcasted_iota(jnp.int32, (owned, half_rows), 0)
        zero = jnp.zeros((owned, half_rows), jnp.float32)
        totals = [zero] * hour_count
        count = zero
        for n in range(owned):
            hits = [half == me * owned + n for half in halves]
            for h in range(hour_count):
                kept = [jnp.where(hits[c], seg_hour[c, h], 0.0) for c in range(CORES)]
                kept = jnp.sum(sum(kept), axis=0, keepdims=True)
                totals[h] = jnp.where(place == n, kept, totals[h])
            found = sum(jnp.where(hit, float(SEG), 0.0) for hit in hits)
            count = jnp.where(place == n, jnp.sum(found, axis=0, keepdims=True), count)
        pixels = jnp.sum(count, axis=1, keepdims=True)
        lane = lax.broadcasted_iota(jnp.int32, (owned, LANES), 1)
        means = jnp.zeros((owned, LANES), jnp.float32)
        for h in range(hour_count):
            mean = jnp.sum(totals[h], axis=1, keepdims=True) / pixels
            means = jnp.where(lane == h, mean, means)
        basin_ref[...] = jnp.transpose(means)[:hour_count, :]

    def piece_sums(t, g):
        first, end = pieces[t][g]
        sums = [jnp.zeros((end - first, tile_cols), jnp.float32)] * slots
        for i in range(members):
            for b in range(scan_block):
                depth = depth_of(gather[order[t], i, b, piece(t, g)])
                sums = add_by_hour(sums, depth, plane, i, b, base_hour)
        return sums

    def push_piece(t, g):
        in_arrival(t, g).wait_recv()
        sums = piece_sums(t, g)
        for k in range(slots):
            part[order[t], k, piece(t, g)] = sums[k]
        for k in range(slots):

            @pl.when(k < span)
            def _():
                z_copy(t, g, k).start()

    def share_swap():
        several(swap_in, swap_send, swap_recv).wait_recv()
        for k in range(col_devices - 1, -1, -1):
            _, r, q = member_at(k)
            lanes = lanes_of(q)
            sums = [jnp.zeros((SWAP_ROWS, tile_cols), jnp.float32)] * pair_slots
            for b in range(scan_block):
                sources = (
                    (frame[b, swap_rows(plane, core), lanes], plane, core),
                    (swap_in[0, b, :, lanes], plane, 1 - core),
                    (swap_in[1, b, :, lanes], twin, 0),
                    (swap_in[2, b, :, lanes], twin, 1),
                )
                for raw, p, c in sources:
                    member = c * col_devices + col
                    sums = add_by_hour(sums, depth_of(raw), p, member, b, pair_base)
            for n in range(pair_slots):
                gsum[k, n] = sums[n]
            if k > 0:
                pltpu.make_async_remote_copy(
                    src_ref=gsum.at[k],
                    dst_ref=grecv.at[col],
                    send_sem=g_send,
                    recv_sem=g_recv,
                    device_id=(r, q),
                    device_id_type=MESH,
                ).start()

    def join_swap():
        several(grecv.at[pl.ds(0, col_devices - 1)], g_send, g_recv).wait_recv()
        for n in range(pair_slots):
            total = gsum[0, n]
            for k in range(1, col_devices):
                _, _, q = member_at(k)
                total = total + grecv[q, n]

            @pl.when(n < pair_span(pair))
            def _():
                hourly_ref[pair_base + n, kept_rows:] += total

    for t in range(planes - 1):
        for g in range(len(pieces[t])):
            if_sent(t, g, push_piece)
            if t == 0 and g == 0:
                reduce_segments()
        if t == SHARE_AFTER:
            share_swap()
    pair_segments()
    basin_means()

    for p in range(planes):
        other = p + 1 - 2 * (p % 2)
        n = sum(hour_span(o) for o in range(planes) if o not in (p, other))

        @pl.when(plane == p)
        def _():
            several(zrecv.at[pl.ds(0, n)], z_send.at[0], z_recv.at[0]).wait_recv()
            several(
                zrecv.at[pl.ds(0, hour_span(other)), pl.ds(0, kept_rows)],
                z_send.at[1],
                z_recv.at[1],
            ).wait_recv()

    for h in range(hour_count):
        hourly_ref[h] = sum_planes(zrecv, h)

    for g in range(len(pieces[-1])):
        in_arrival(planes - 1, g).wait_recv()
        sums = piece_sums(planes - 1, g)
        for k in range(slots):

            @pl.when(k < span)
            def _():
                hourly_ref[base_hour + k, piece(planes - 1, g)] += sums[k]

    join_swap()

    several(
        all_ids.at[pl.ds(0, planes * members - 1)], id_send, id_recv
    ).wait_send()
    several(seg_in.at[pl.ds(0, members - 1)], seg_send, seg_recv).wait_send()
    several(
        gather.at[pl.ds(0, planes - 1), pl.ds(0, members - 1)],
        in_send,
        in_recv.at[0],
    ).wait_send()
    several(swap_in, swap_send, swap_recv).wait_send()
    several(grecv.at[pl.ds(0, col_devices - 1)], g_send, g_recv).wait_send()

    def sums_sent(n):
        several(
            zseg.at[pl.ds(0, (planes - 1) * n)], zseg_send, zseg_recv
        ).wait_send()
        several(
            part.at[pl.ds(0, planes - 2), pl.ds(0, n)], z_send.at[0], z_recv.at[0]
        ).wait_send()
        several(
            part.at[0, pl.ds(0, n), pl.ds(0, kept_rows)],
            z_send.at[1],
            z_recv.at[1],
        ).wait_send()

    by_span(sums_sent)


def write_out(hourly_ref, basin_ref, hourly_out, basin_out, sem):
    pairs = ((hourly_ref, hourly_out), (basin_ref, basin_out))
    copies = [pltpu.make_async_copy(s, d, sem.at[n]) for n, (s, d) in enumerate(pairs)]
    for copy in copies:
        copy.start()
    for copy in copies:
        copy.wait()


def body(reflectivity, scan_hour, basin_ids):
    row_devices = lax.axis_size("row")
    col_devices = lax.axis_size("col")
    scan_block, grid_height, grid_width = reflectivity.shape
    tile_rows = grid_height // row_devices
    tile_cols = grid_width // col_devices
    scan_count = scan_hour.shape[0]
    hour_count = (scan_count + 10) // HOUR_SCANS + 1
    devices = row_devices * col_devices
    owned = grid_height * grid_width // (SEG * BASIN_ROWS) // devices
    planes = row_devices // CORES
    members = CORES * col_devices
    plane_scans = members * scan_block

    def span_of(first, last):
        rest = scan_count - plane_scans * (last + 1)
        return hour_count - rest // HOUR_SCANS - (first * plane_scans) // HOUR_SCANS

    slots = max(span_of(p, p) for p in range(planes))
    pair_slots = max(span_of(2 * j, 2 * j + 1) for j in range(planes // 2))
    seg_shape = (grid_width // SEG, grid_height // CORES)
    dims = (row_devices, col_devices, hour_count, slots, tile_rows, tile_cols, owned)
    piece_count = len(FIRST) + len(LATER) * (planes - 2) + len(OWN)
    dma = pltpu.SemaphoreType.DMA
    f32 = jnp.float32
    id_shape = basin_ids.shape[::-1]
    anywhere = pl.BlockSpec(memory_space=pltpu.HBM)
    inside = pl.BlockSpec(memory_space=pltpu.VMEM)
    hourly, basin = pl.pallas_call(
        functools.partial(kernel, dims),
        out_shape=(
            jax.ShapeDtypeStruct((hour_count, tile_rows, tile_cols), f32),
            jax.ShapeDtypeStruct((hour_count, owned), f32),
        ),
        in_specs=[anywhere] * 3,
        out_specs=(inside, inside),
        scratch_shapes=[
            pltpu.VMEM(reflectivity.shape, f32),
            pltpu.SMEM(scan_hour.shape, jnp.int32),
            pltpu.VMEM(id_shape, jnp.int32),
            pltpu.VMEM((planes, members, scan_block, tile_rows, tile_cols), f32),
            pltpu.VMEM((planes, slots, tile_rows, tile_cols), f32),
            pltpu.VMEM((planes * slots, tile_rows, tile_cols), f32),
            pltpu.VMEM((members,) + id_shape, jnp.int32),
            pltpu.VMEM((planes * members,) + id_shape, jnp.int32),
            pltpu.VMEM((CORES, scan_block) + seg_shape, f32),
            pltpu.VMEM((members, scan_block) + seg_shape, f32),
            pltpu.VMEM((slots,) + seg_shape, f32),
            pltpu.VMEM((planes * slots,) + seg_shape, f32),
            pltpu.VMEM((CORES, hour_count) + seg_shape, f32),
            pltpu.VMEM((CORES + 1, scan_block, SWAP_ROWS, grid_width), f32),
            pltpu.VMEM((col_devices, pair_slots, SWAP_ROWS, tile_cols), f32),
            pltpu.VMEM((col_devices, pair_slots, SWAP_ROWS, tile_cols), f32),
            pltpu.SemaphoreType.REGULAR((5,)),
            dma((2,)),
            dma((2,)),
            dma,
            dma((piece_count,)),
            dma((2,)),
            dma((2,)),
            dma,
            dma,
            dma,
            dma,
            dma,
            dma,
            dma,
            dma,
            dma,
            dma,
            dma,
            dma,
            dma,
        ],
        compiler_params=pltpu.CompilerParams(
            collective_id=0, has_side_effects=True, vmem_limit_bytes=40 * 2**20
        ),
    )(*(pltpu.with_memory_space_constraint(v, pltpu.HBM) for v in (reflectivity, scan_hour, basin_ids.T)))
    hourly, basin = pl.pallas_call(
        write_out,
        out_shape=(
            jax.ShapeDtypeStruct(hourly.shape, f32),
            jax.ShapeDtypeStruct(basin.shape, f32),
        ),
        in_specs=[inside] * 2,
        out_specs=(anywhere, anywhere),
        scratch_shapes=[dma((2,))],
        compiler_params=pltpu.CompilerParams(vmem_limit_bytes=8 * 2**20),
    )(hourly, basin)
    return hourly, basin.T


def solution(mesh):
    placed = (P(("row", "col"), None, None), P(), P("row", "col"))
    return jax.shard_map(
        body,
        mesh=mesh,
        in_specs=placed,
        out_specs=(P(None, "row", "col"), P(("row", "col"), None)),
        check_vma=False,
    )
```

```python
import functools
import math

import jax
import jax.numpy as jnp
from jax import lax
from jax.experimental import pallas as pl
from jax.experimental.pallas import tpu as pltpu
from jax.sharding import PartitionSpec as P

SEG = 128
BASIN_ROWS = 8
HOUR_SCANS = 12
CORES = 2
LANES = 128
FIRST = (8, 16, 32)
LATER = (16, 32)
OWN = (16,)
SWAP_ROWS = 16
SHARE_AFTER = 1
MESH = pl.DeviceIdType.MESH

slope_db = math.log(10.0) / 16.0
offset_zr = math.log(200.0) / 1.6 + math.log(12.0)


def sent_words(dims, scan_block, pair_slots, span):
    row_devices, col_devices, hour_count, slots, tile_rows, tile_cols, owned = dims
    planes = row_devices // CORES
    members = CORES * col_devices
    kept_rows = tile_rows - SWAP_ROWS
    seg_words = row_devices * tile_rows // CORES * col_devices * tile_cols // SEG
    chunk_rows = (planes - 2) * tile_rows + kept_rows
    pixels = (members - 1) * (chunk_rows + kept_rows) * tile_cols * scan_block
    segments = ((members - 1) * scan_block + hour_count) * seg_words
    swapped = (CORES + 1) * SWAP_ROWS * col_devices * tile_cols * scan_block
    shared = (col_devices - 1) * pair_slots * SWAP_ROWS * tile_cols
    sums = span * (chunk_rows * tile_cols + (planes - 1) * seg_words)
    return pixels + segments + swapped + shared + sums


def kernel(
    dims,
    refl_ref,
    hour_ref,
    ids_ref,
    hourly_ref,
    basin_ref,
    frame,
    hours,
    ids,
    gather,
    part,
    zrecv,
    plane_ids,
    all_ids,
    flat_ids,
    seg_own,
    seg_in,
    seg_part,
    zseg,
    seg_hour,
    swap_in,
    gsum,
    grecv,
    spare,
    wave_sem,
    local_sem,
    load_sem,
    sent_sem,
    in_recv,
    z_recv,
    id_send,
    id_recv,
    idz_recv,
    seg_recv,
    zseg_recv,
    pair_recv,
    swap_recv,
    g_recv,
):
    row_devices, col_devices, hour_count, slots, tile_rows, tile_cols, owned = dims
    planes = row_devices // CORES
    members = CORES * col_devices
    devices = row_devices * col_devices
    scan_block = gather.shape[2]
    scan_count = hour_ref.shape[0]
    plane_scans = members * scan_block
    cuts = [FIRST] + [LATER] * (planes - 2) + [OWN]
    pieces = [list(zip((0,) + ends[:-1], ends)) for ends in cuts]
    piece_sem = [sum(map(len, cuts[:t])) for t in range(planes)]
    all_segs, half_rows = seg_own.shape[2:]
    kept_rows = tile_rows - SWAP_ROWS
    pair_slots = gsum.shape[1]

    row = lax.axis_index("row")
    col = lax.axis_index("col")
    plane = row // CORES
    core = row % CORES
    mine = core * col_devices + col
    me = row * col_devices + col
    pair = plane // 2
    twin = plane + 1 - 2 * (plane % 2)

    def first_hour(p):
        return (p * plane_scans) // HOUR_SCANS

    def hour_span(p):
        rest = scan_count - plane_scans - p * plane_scans
        return hour_count - rest // HOUR_SCANS - first_hour(p)

    def pair_span(j):
        return first_hour(2 * j + 1) + hour_span(2 * j + 1) - first_hour(2 * j)

    def by_plane(table):
        value = table[0]
        for p in range(1, planes):
            value = jnp.where(plane == p, table[p], value)
        return value

    def chunk_order(p):
        others = sorted((d for d in range(planes) if d != p), key=lambda d: -abs(d - p))
        if 0 in others:
            others.remove(0)
            others.insert(0, 0)
        return others + [p]

    orders = [chunk_order(p) for p in range(planes)]
    order = [by_plane([o[t] for o in orders]) for t in range(planes)]
    whole = [order[t] != twin for t in range(planes)]

    def member_at(k):
        dc = k // col_devices
        dq = k % col_devices
        half = col_devices // 2
        qq = ((col // 2 + dq // 2) % half) * 2 + (col + dq) % 2
        other = ((core + dc) % CORES) * col_devices + qq
        return other, plane * CORES + other // col_devices, other % col_devices

    def several(ref, send_sem, recv_sem):
        return pltpu.make_async_remote_copy(
            src_ref=ref,
            dst_ref=ref,
            send_sem=send_sem,
            recv_sem=recv_sem,
            device_id=((row + 1) % row_devices, col),
            device_id_type=MESH,
        )

    def signal(sem, r, q):
        pl.semaphore_signal(sem, inc=1, device_id=(r, q), device_id_type=MESH)

    def row_at(p):
        return p * CORES + core

    barrier = pltpu.get_barrier_semaphore()
    far_first = sorted(range(1, members), key=lambda k: (-(k % col_devices), k))
    for k in far_first:
        _, r, q = member_at(k)
        signal(barrier, r, q)

    greeter = core == CORES - 1
    below = greeter & (plane > 0)
    above = greeter & (plane < planes - 1)

    @pl.when(below)
    def _():
        signal(barrier, row_at(plane - 1), col)

    @pl.when(above)
    def _():
        signal(barrier, row_at(plane + 1), col)

    def tile_at(d, c):
        return pl.multiple_of((d * CORES + c) * tile_rows, 8)

    def lanes_of(q):
        return pl.ds(pl.multiple_of(q * tile_cols, 128), tile_cols)

    def plane_rows(d):
        rows = CORES * tile_rows
        return pl.ds(pl.multiple_of(d * rows, 8), rows)

    load_ids = pltpu.make_async_copy(ids_ref, ids, local_sem.at[0])
    load_ids.start()
    for t, d in enumerate(order):
        pltpu.make_async_copy(
            refl_ref.at[:, plane_rows(d), :],
            frame.at[:, plane_rows(d), :],
            load_sem.at[min(t, 1)],
        ).start()

    def frame_loaded(late):
        count = (planes - 1 if late else 1) * CORES * tile_rows
        rows = frame.at[:, pl.ds(0, count), :]
        pltpu.make_async_copy(rows, rows, load_sem.at[late]).wait()

    load_hours = pltpu.make_async_copy(hour_ref, hours, local_sem.at[1])
    load_hours.start()
    for k in range(slots):
        zrecv[plane * slots + k] = jnp.zeros((tile_rows, tile_cols), jnp.float32)
        zrecv[twin * slots + k, kept_rows:] = jnp.zeros(
            (SWAP_ROWS, tile_cols), jnp.float32
        )

    load_ids.wait()
    plane_ids[mine] = ids[...]
    beside = jnp.where(below, 1, 0) + jnp.where(above, 1, 0)
    pl.semaphore_wait(barrier, members - 1 + beside)

    def id_copy(k):
        other, r, q = member_at(k)
        return pltpu.make_async_remote_copy(
            src_ref=ids,
            dst_ref=plane_ids.at[mine],
            send_sem=id_send,
            recv_sem=id_recv,
            device_id=(r, q),
            device_id_type=MESH,
        )

    for k in range(1, members):
        id_copy(k).start()

    @pl.when(greeter)
    def _():
        signal(wave_sem.at[2], row_at(twin), col)

    @pl.when(greeter & (plane == 0))
    def _():
        signal(wave_sem.at[0], row_at(plane + 1), col)

    @pl.when(greeter & (plane == planes - 1))
    def _():
        signal(wave_sem.at[1], row_at(plane - 1), col)

    def piece(t, g):
        first, end = pieces[t][g]
        return pl.ds(first, end - first)

    def in_copy(t, g, k):
        other, r, q = member_at(k)
        d = order[t]
        first, end = pieces[t][g]
        top = pl.multiple_of(tile_at(d, other // col_devices) + first, 8)
        return pltpu.make_async_remote_copy(
            src_ref=frame.at[:, pl.ds(top, end - first), lanes_of(q)],
            dst_ref=gather.at[d, mine, :, piece(t, g)],
            send_sem=sent_sem,
            recv_sem=in_recv.at[piece_sem[t] + g],
            device_id=(r, q),
            device_id_type=MESH,
        )

    def in_arrival(t, g):
        ref = gather.at[order[t], pl.ds(0, members - 1), :, piece(t, g)]
        return several(ref, sent_sem, in_recv.at[piece_sem[t] + g])

    def if_sent(t, g, action):
        if pieces[t][g][0] < kept_rows:
            action(t, g)
        else:

            @pl.when(whole[t])
            def _():
                action(t, g)

    def send_piece(t, g):
        for k in far_first:
            in_copy(t, g, k).start()

    def seg_copy(k):
        other, r, q = member_at(k)
        return pltpu.make_async_remote_copy(
            src_ref=seg_own.at[other // col_devices],
            dst_ref=seg_in.at[mine],
            send_sem=sent_sem,
            recv_sem=seg_recv,
            device_id=(r, q),
            device_id_type=MESH,
        )

    def depth_of(raw):
        return jnp.exp(raw * slope_db - offset_zr)

    def sum_segments():
        near_lane = lax.broadcasted_iota(jnp.int32, (SEG, LANES), 1)
        for b in range(scan_block):
            for c in range(CORES):
                rows = pl.ds(c * half_rows, half_rows)
                total = jnp.zeros((half_rows, LANES), jnp.float32)
                for g in range(all_segs):
                    rest = depth_of(frame[b, rows, g * SEG : (g + 1) * SEG])
                    ones = jnp.where(near_lane == g, 1.0, 0.0).astype(jnp.bfloat16)
                    for _ in range(3):
                        head = rest.astype(jnp.bfloat16)
                        rest = rest - head.astype(jnp.float32)
                        total = total + jnp.dot(
                            head, ones, preferred_element_type=jnp.float32
                        )
                seg_own[c, b] = jnp.transpose(total)[:all_segs]

    frame_loaded(0)
    send_piece(0, 0)
    frame_loaded(1)
    sum_segments()
    for k in range(1, members):
        seg_copy(k).start()
    seg_in[mine] = seg_own[core]
    for t in range(planes):
        for g in range(len(pieces[t])):
            if t or g:
                if_sent(t, g, send_piece)

    for d in range(planes):
        rows = pl.ds(tile_at(d, core), tile_rows)
        gather[d, mine] = frame[:, rows, lanes_of(col)]

    def tell_core(sem):
        @pl.when(greeter)
        def _():
            for c in range(CORES - 1):
                signal(sem, plane * CORES + c, col)

        @pl.when(jnp.logical_not(greeter))
        def _():
            pl.semaphore_wait(sem, 1)


    @pl.when(greeter)
    def _():
        pl.semaphore_wait(wave_sem.at[2], 1)

    tell_core(wave_sem.at[0])

    def swap_rows(d, c):
        return pl.ds(pl.multiple_of(tile_at(d, c) + kept_rows, 8), SWAP_ROWS)

    def swap_copy(d, c, slot):
        return pltpu.make_async_remote_copy(
            src_ref=frame.at[:, swap_rows(d, c), :],
            dst_ref=swap_in.at[slot],
            send_sem=sent_sem,
            recv_sem=swap_recv,
            device_id=(d * CORES + c, col),
            device_id_type=MESH,
        )

    for c in range(CORES):
        swap_copy(twin, c, 1 + core).start()
    swap_copy(plane, 1 - core, 0).start()


    @pl.when(below)
    def _():
        pl.semaphore_wait(wave_sem.at[0], 1)

        @pl.when(above)
        def _():
            signal(wave_sem.at[0], row_at(plane + 1), col)

    @pl.when(above)
    def _():
        pl.semaphore_wait(wave_sem.at[1], 1)

        @pl.when(below)
        def _():
            signal(wave_sem.at[1], row_at(plane - 1), col)

    tell_core(wave_sem.at[1])

    several(plane_ids.at[pl.ds(0, members - 1)], id_send, id_recv).wait_recv()

    plane_block = pl.ds(plane * members, members)
    for k in range(1, planes):
        pltpu.make_async_remote_copy(
            src_ref=plane_ids,
            dst_ref=all_ids.at[plane_block],
            send_sem=id_send,
            recv_sem=idz_recv,
            device_id=(row_at((plane + k) % planes), col),
            device_id_type=MESH,
        ).start()
    all_ids[plane_block] = plane_ids[...]
    load_hours.wait()

    base_hour = first_hour(plane)
    span = hour_span(plane)
    pair_base = first_hour(2 * pair)
    spans = sorted({hour_span(p) for p in range(planes)})

    def by_span(action):
        for n in spans:

            @pl.when(span == n)
            def _():
                action(n)

    def side(p):
        return jnp.where(p == twin, 1, 0)

    def z_copy(t, g, k):
        return pltpu.make_async_remote_copy(
            src_ref=part.at[order[t], k, piece(t, g)],
            dst_ref=zrecv.at[plane * slots + k, piece(t, g)],
            send_sem=sent_sem,
            recv_sem=z_recv.at[side(order[t])],
            device_id=(row_at(order[t]), col),
            device_id_type=MESH,
        )

    def zseg_copy(k, n):
        return pltpu.make_async_remote_copy(
            src_ref=seg_part.at[pl.ds(0, n)],
            dst_ref=zseg.at[pl.ds(plane * slots, n)],
            send_sem=sent_sem,
            recv_sem=zseg_recv,
            device_id=(row_at((plane + k) % planes), col),
            device_id_type=MESH,
        )

    def pair_copy():
        return pltpu.make_async_remote_copy(
            src_ref=seg_hour.at[core],
            dst_ref=seg_hour.at[core],
            send_sem=sent_sem,
            recv_sem=pair_recv,
            device_id=(plane * CORES + 1 - core, col),
            device_id_type=MESH,
        )

    def wait_slots(ref, send_sem, recv_sem):
        for p in range(planes):
            n = sum(hour_span(o) for o in range(planes) if o != p)

            @pl.when(plane == p)
            def _():
                several(ref.at[pl.ds(0, n)], send_sem, recv_sem).wait_recv()

    def sum_planes(ref, h):
        total = None
        for p in range(planes):
            if first_hour(p) <= h < first_hour(p) + hour_span(p):
                term = ref[p * slots + h - first_hour(p)]
                total = term if total is None else total + term
        return total

    def add_by_hour(sums, raw, p, member, b, base):
        hour = hours[p * plane_scans + member * scan_block + b] - base
        return [
            total + jnp.where(hour == k, raw, 0.0) for k, total in enumerate(sums)
        ]

    def reduce_segments():
        several(seg_in.at[pl.ds(0, members - 1)], sent_sem, seg_recv).wait_recv()
        sums = [jnp.zeros((all_segs, half_rows), jnp.float32)] * slots
        for i in range(members):
            for b in range(scan_block):
                sums = add_by_hour(sums, seg_in[i, b], plane, i, b, base_hour)
        for k in range(slots):
            seg_part[k] = sums[k]
            zseg[plane * slots + k] = sums[k]

        def send(n):
            for k in range(1, planes):
                zseg_copy(k, n).start()

        by_span(send)

    def pair_segments():
        wait_slots(zseg, sent_sem, zseg_recv)
        for h in range(hour_count):
            seg_hour[core, h] = sum_planes(zseg, h)
        pair_copy().start()

    def lay_ids():
        several(
            all_ids.at[pl.ds(0, (planes - 1) * members)], id_send, idz_recv
        ).wait_recv()
        blocks = row_devices // CORES
        for c in range(CORES):
            lanes = []
            for r in range(c * blocks, (c + 1) * blocks):
                first = r * col_devices
                tiles = [all_ids[first + q] for q in range(col_devices)]
                lanes.append(jnp.concatenate(tiles, axis=0))
            flat_ids[c] = jnp.concatenate(lanes, axis=1)

    def basin_means():
        pair_copy().wait_recv()
        halves = [flat_ids[c] for c in range(CORES)]
        place = lax.broadcasted_iota(jnp.int32, (owned, half_rows), 0)
        zero = jnp.zeros((owned, half_rows), jnp.float32)
        totals = [zero] * hour_count
        count = zero
        for n in range(owned):
            hits = [half == me * owned + n for half in halves]
            for h in range(hour_count):
                kept = [jnp.where(hits[c], seg_hour[c, h], 0.0) for c in range(CORES)]
                kept = jnp.sum(sum(kept), axis=0, keepdims=True)
                totals[h] = jnp.where(place == n, kept, totals[h])
            found = sum(jnp.where(hit, float(SEG), 0.0) for hit in hits)
            count = jnp.where(place == n, jnp.sum(found, axis=0, keepdims=True), count)
        pixels = jnp.sum(count, axis=1, keepdims=True)
        lane = lax.broadcasted_iota(jnp.int32, (owned, LANES), 1)
        means = jnp.zeros((owned, LANES), jnp.float32)
        for h in range(hour_count):
            mean = jnp.sum(totals[h], axis=1, keepdims=True) / pixels
            means = jnp.where(lane == h, mean, means)
        basin_ref[...] = jnp.transpose(means)[:hour_count, :]

    def piece_sums(t, g):
        first, end = pieces[t][g]
        sums = [jnp.zeros((end - first, tile_cols), jnp.float32)] * slots
        for i in range(members):
            for b in range(scan_block):
                depth = depth_of(gather[order[t], i, b, piece(t, g)])
                sums = add_by_hour(sums, depth, plane, i, b, base_hour)
        return sums

    def push_piece(t, g):
        in_arrival(t, g).wait_recv()
        sums = piece_sums(t, g)
        for k in range(slots):
            part[order[t], k, piece(t, g)] = sums[k]
        for k in range(slots):

            @pl.when(k < span)
            def _():
                z_copy(t, g, k).start()

    def share_swap():
        several(swap_in, sent_sem, swap_recv).wait_recv()
        for k in range(col_devices - 1, -1, -1):
            _, r, q = member_at(k)
            lanes = lanes_of(q)
            sums = [jnp.zeros((SWAP_ROWS, tile_cols), jnp.float32)] * pair_slots
            for b in range(scan_block):
                sources = (
                    (frame[b, swap_rows(plane, core), lanes], plane, core),
                    (swap_in[0, b, :, lanes], plane, 1 - core),
                    (swap_in[1, b, :, lanes], twin, 0),
                    (swap_in[2, b, :, lanes], twin, 1),
                )
                for raw, p, c in sources:
                    member = c * col_devices + col
                    sums = add_by_hour(sums, depth_of(raw), p, member, b, pair_base)
            for n in range(pair_slots):
                gsum[k, n] = sums[n]
            if k > 0:
                pltpu.make_async_remote_copy(
                    src_ref=gsum.at[k],
                    dst_ref=grecv.at[col],
                    send_sem=sent_sem,
                    recv_sem=g_recv,
                    device_id=(r, q),
                    device_id_type=MESH,
                ).start()

    def join_swap():
        several(grecv.at[pl.ds(0, col_devices - 1)], sent_sem, g_recv).wait_recv()
        for n in range(pair_slots):
            total = gsum[0, n]
            for k in range(1, col_devices):
                _, _, q = member_at(k)
                total = total + grecv[q, n]

            @pl.when(n < pair_span(pair))
            def _():
                hourly_ref[pair_base + n, kept_rows:] = total

    for t in range(planes - 1):
        for g in range(len(pieces[t])):
            if_sent(t, g, push_piece)
            if t == 0 and g == 0:
                reduce_segments()
        if t == SHARE_AFTER:
            share_swap()
    lay_ids()
    pair_segments()
    hourly_ref[...] = jnp.zeros_like(hourly_ref)
    for g in range(len(pieces[-1])):
        in_arrival(planes - 1, g).wait_recv()
        sums = piece_sums(planes - 1, g)
        for k in range(slots):

            @pl.when(k < span)
            def _():
                hourly_ref[base_hour + k, piece(planes - 1, g)] = sums[k]

    join_swap()
    basin_means()

    for p in range(planes):
        other = p + 1 - 2 * (p % 2)
        n = sum(hour_span(o) for o in range(planes) if o not in (p, other))

        @pl.when(plane == p)
        def _():
            several(zrecv.at[pl.ds(0, n)], sent_sem, z_recv.at[0]).wait_recv()
            several(
                zrecv.at[pl.ds(0, hour_span(other)), pl.ds(0, kept_rows)],
                sent_sem,
                z_recv.at[1],
            ).wait_recv()

    for h in range(hour_count):
        hourly_ref[h] += sum_planes(zrecv, h)

    several(
        all_ids.at[pl.ds(0, planes * members - 1)], id_send, id_recv
    ).wait_send()
    def all_sent(n):
        count = sent_words(dims, scan_block, pair_slots, n) // (8 * LANES)
        several(spare.at[pl.ds(0, count)], sent_sem, swap_recv).wait_send()

    by_span(all_sent)


def write_out(hourly_ref, basin_ref, hourly_out, basin_out, sem):
    pairs = ((hourly_ref, hourly_out), (basin_ref, basin_out))
    copies = [pltpu.make_async_copy(s, d, sem.at[n]) for n, (s, d) in enumerate(pairs)]
    for copy in copies:
        copy.start()
    for copy in copies:
        copy.wait()


def body(reflectivity, scan_hour, basin_ids):
    row_devices = lax.axis_size("row")
    col_devices = lax.axis_size("col")
    scan_block, grid_height, grid_width = reflectivity.shape
    tile_rows = grid_height // row_devices
    tile_cols = grid_width // col_devices
    scan_count = scan_hour.shape[0]
    hour_count = (scan_count + 10) // HOUR_SCANS + 1
    devices = row_devices * col_devices
    owned = grid_height * grid_width // (SEG * BASIN_ROWS) // devices
    planes = row_devices // CORES
    members = CORES * col_devices
    plane_scans = members * scan_block

    def span_of(first, last):
        rest = scan_count - plane_scans * (last + 1)
        return hour_count - rest // HOUR_SCANS - (first * plane_scans) // HOUR_SCANS

    slots = max(span_of(p, p) for p in range(planes))
    pair_slots = max(span_of(2 * j, 2 * j + 1) for j in range(planes // 2))
    seg_shape = (grid_width // SEG, grid_height // CORES)
    dims = (row_devices, col_devices, hour_count, slots, tile_rows, tile_cols, owned)
    piece_count = len(FIRST) + len(LATER) * (planes - 2) + len(OWN)
    spare_count = sent_words(dims, scan_block, pair_slots, slots) // (8 * LANES)
    dma = pltpu.SemaphoreType.DMA
    f32 = jnp.float32
    id_shape = basin_ids.shape[::-1]
    anywhere = pl.BlockSpec(memory_space=pltpu.HBM)
    inside = pl.BlockSpec(memory_space=pltpu.VMEM)
    hourly, basin = pl.pallas_call(
        functools.partial(kernel, dims),
        out_shape=(
            jax.ShapeDtypeStruct((hour_count, tile_rows, tile_cols), f32),
            jax.ShapeDtypeStruct((hour_count, owned), f32),
        ),
        in_specs=[anywhere] * 3,
        out_specs=(inside, inside),
        scratch_shapes=[
            pltpu.VMEM(reflectivity.shape, f32),
            pltpu.SMEM(scan_hour.shape, jnp.int32),
            pltpu.VMEM(id_shape, jnp.int32),
            pltpu.VMEM((planes, members, scan_block, tile_rows, tile_cols), f32),
            pltpu.VMEM((planes, slots, tile_rows, tile_cols), f32),
            pltpu.VMEM((planes * slots, tile_rows, tile_cols), f32),
            pltpu.VMEM((members,) + id_shape, jnp.int32),
            pltpu.VMEM((planes * members,) + id_shape, jnp.int32),
            pltpu.VMEM((CORES,) + seg_shape, jnp.int32),
            pltpu.VMEM((CORES, scan_block) + seg_shape, f32),
            pltpu.VMEM((members, scan_block) + seg_shape, f32),
            pltpu.VMEM((slots,) + seg_shape, f32),
            pltpu.VMEM((planes * slots,) + seg_shape, f32),
            pltpu.VMEM((CORES, hour_count) + seg_shape, f32),
            pltpu.VMEM((CORES + 1, scan_block, SWAP_ROWS, grid_width), f32),
            pltpu.VMEM((col_devices, pair_slots, SWAP_ROWS, tile_cols), f32),
            pltpu.VMEM((col_devices, pair_slots, SWAP_ROWS, tile_cols), f32),
            pltpu.VMEM((spare_count, 8, LANES), f32),
            pltpu.SemaphoreType.REGULAR((3,)),
            dma((2,)),
            dma((2,)),
            dma,
            dma((piece_count,)),
            dma((2,)),
            dma,
            dma,
            dma,
            dma,
            dma,
            dma,
            dma,
            dma,
        ],
        compiler_params=pltpu.CompilerParams(
            collective_id=0, has_side_effects=True, vmem_limit_bytes=40 * 2**20
        ),
    )(*(pltpu.with_memory_space_constraint(v, pltpu.HBM) for v in (reflectivity, scan_hour, basin_ids.T)))
    hourly, basin = pl.pallas_call(
        write_out,
        out_shape=(
            jax.ShapeDtypeStruct(hourly.shape, f32),
            jax.ShapeDtypeStruct(basin.shape, f32),
        ),
        in_specs=[inside] * 2,
        out_specs=(anywhere, anywhere),
        scratch_shapes=[dma((2,))],
        compiler_params=pltpu.CompilerParams(vmem_limit_bytes=8 * 2**20),
    )(hourly, basin)
    return hourly, basin.T


def solution(mesh):
    placed = (P(("row", "col"), None, None), P(), P("row", "col"))
    return jax.shard_map(
        body,
        mesh=mesh,
        in_specs=placed,
        out_specs=(P(None, "row", "col"), P(("row", "col"), None)),
        check_vma=False,
    )
```

```python
import functools
import math

import jax
import jax.numpy as jnp
from jax import lax
from jax.experimental import pallas as pl
from jax.experimental.pallas import tpu as pltpu
from jax.sharding import PartitionSpec as P

SEG = 128
BASIN_ROWS = 8
HOUR_SCANS = 12
CORES = 2
LANES = 128
FIRST = (8, 16, 32)
LATER = (16, 32)
OWN = (16,)
SWAP_ROWS = 16
SHARE_AFTER = 1
MESH = pl.DeviceIdType.MESH

slope_db = math.log(10.0) / 16.0
offset_zr = math.log(200.0) / 1.6 + math.log(12.0)


def sent_words(dims, scan_block, pair_slots, span):
    row_devices, col_devices, hour_count, slots, tile_rows, tile_cols, owned = dims
    planes = row_devices // CORES
    members = CORES * col_devices
    kept_rows = tile_rows - SWAP_ROWS
    seg_words = row_devices * tile_rows // CORES * col_devices * tile_cols // SEG
    chunk_rows = (planes - 2) * tile_rows + kept_rows
    pixels = (members - 1) * (chunk_rows + kept_rows) * tile_cols * scan_block
    segments = ((members - 1) * scan_block + hour_count) * seg_words
    swapped = (CORES + 1) * SWAP_ROWS * col_devices * tile_cols * scan_block
    shared = (col_devices - 1) * pair_slots * SWAP_ROWS * tile_cols
    sums = span * (chunk_rows * tile_cols + (planes - 1) * seg_words)
    return pixels + segments + swapped + shared + sums


def kernel(
    dims,
    refl_ref,
    hour_ref,
    ids_ref,
    hourly_ref,
    basin_ref,
    frame,
    hours,
    ids,
    gather,
    part,
    zrecv,
    plane_ids,
    all_ids,
    flat_ids,
    seg_own,
    seg_in,
    seg_part,
    zseg,
    seg_hour,
    swap_in,
    gsum,
    grecv,
    spare,
    wave_sem,
    local_sem,
    load_sem,
    sent_sem,
    in_recv,
    z_recv,
    id_send,
    id_recv,
    idz_recv,
    seg_recv,
    zseg_recv,
    pair_recv,
    swap_recv,
    g_recv,
):
    row_devices, col_devices, hour_count, slots, tile_rows, tile_cols, owned = dims
    planes = row_devices // CORES
    members = CORES * col_devices
    devices = row_devices * col_devices
    scan_block = gather.shape[2]
    scan_count = hour_ref.shape[0]
    plane_scans = members * scan_block
    cuts = [FIRST] + [LATER] * (planes - 2) + [OWN]
    pieces = [list(zip((0,) + ends[:-1], ends)) for ends in cuts]
    piece_sem = [sum(map(len, cuts[:t])) for t in range(planes)]
    all_segs, half_rows = seg_own.shape[2:]
    kept_rows = tile_rows - SWAP_ROWS
    pair_slots = gsum.shape[1]

    row = lax.axis_index("row")
    col = lax.axis_index("col")
    plane = row // CORES
    core = row % CORES
    mine = core * col_devices + col
    me = row * col_devices + col
    pair = plane // 2
    twin = plane + 1 - 2 * (plane % 2)

    def first_hour(p):
        return (p * plane_scans) // HOUR_SCANS

    def hour_span(p):
        rest = scan_count - plane_scans - p * plane_scans
        return hour_count - rest // HOUR_SCANS - first_hour(p)

    def pair_span(j):
        return first_hour(2 * j + 1) + hour_span(2 * j + 1) - first_hour(2 * j)

    def by_plane(table):
        value = table[0]
        for p in range(1, planes):
            value = jnp.where(plane == p, table[p], value)
        return value

    def chunk_order(p):
        others = sorted((d for d in range(planes) if d != p), key=lambda d: -abs(d - p))
        if 0 in others:
            others.remove(0)
            others.insert(0, 0)
        return others + [p]

    orders = [chunk_order(p) for p in range(planes)]
    order = [by_plane([o[t] for o in orders]) for t in range(planes)]
    whole = [order[t] != twin for t in range(planes)]

    def member_at(k):
        dc = k // col_devices
        dq = k % col_devices
        half = col_devices // 2
        qq = ((col // 2 + dq // 2) % half) * 2 + (col + dq) % 2
        other = ((core + dc) % CORES) * col_devices + qq
        return other, plane * CORES + other // col_devices, other % col_devices

    def several(ref, send_sem, recv_sem):
        return pltpu.make_async_remote_copy(
            src_ref=ref,
            dst_ref=ref,
            send_sem=send_sem,
            recv_sem=recv_sem,
            device_id=((row + 1) % row_devices, col),
            device_id_type=MESH,
        )

    def signal(sem, r, q):
        pl.semaphore_signal(sem, inc=1, device_id=(r, q), device_id_type=MESH)

    def row_at(p):
        return p * CORES + core

    barrier = pltpu.get_barrier_semaphore()
    far_first = sorted(range(1, members), key=lambda k: (-(k % col_devices), k))
    for k in far_first:
        _, r, q = member_at(k)
        signal(barrier, r, q)

    greeter = core == CORES - 1
    below = greeter & (plane > 0)
    above = greeter & (plane < planes - 1)

    @pl.when(below)
    def _():
        signal(barrier, row_at(plane - 1), col)

    @pl.when(above)
    def _():
        signal(barrier, row_at(plane + 1), col)

    def tile_at(d, c):
        return pl.multiple_of((d * CORES + c) * tile_rows, 8)

    def lanes_of(q):
        return pl.ds(pl.multiple_of(q * tile_cols, 128), tile_cols)

    def plane_rows(d):
        rows = CORES * tile_rows
        return pl.ds(pl.multiple_of(d * rows, 8), rows)

    load_ids = pltpu.make_async_copy(ids_ref, ids, local_sem.at[0])
    load_ids.start()
    for t, d in enumerate(order):
        pltpu.make_async_copy(
            refl_ref.at[:, plane_rows(d), :],
            frame.at[:, plane_rows(d), :],
            load_sem.at[min(t, 1)],
        ).start()

    def frame_loaded(late):
        count = (planes - 1 if late else 1) * CORES * tile_rows
        rows = frame.at[:, pl.ds(0, count), :]
        pltpu.make_async_copy(rows, rows, load_sem.at[late]).wait()

    load_hours = pltpu.make_async_copy(hour_ref, hours, local_sem.at[1])
    load_hours.start()
    for k in range(slots):
        zrecv[plane * slots + k] = jnp.zeros((tile_rows, tile_cols), jnp.float32)
        zrecv[twin * slots + k, kept_rows:] = jnp.zeros(
            (SWAP_ROWS, tile_cols), jnp.float32
        )

    load_ids.wait()
    plane_ids[mine] = ids[...]
    beside = jnp.where(below, 1, 0) + jnp.where(above, 1, 0)
    pl.semaphore_wait(barrier, members - 1 + beside)

    def id_copy(k):
        other, r, q = member_at(k)
        return pltpu.make_async_remote_copy(
            src_ref=ids,
            dst_ref=plane_ids.at[mine],
            send_sem=id_send,
            recv_sem=id_recv,
            device_id=(r, q),
            device_id_type=MESH,
        )

    for k in range(1, members):
        id_copy(k).start()

    @pl.when(greeter)
    def _():
        signal(wave_sem.at[2], row_at(twin), col)

    @pl.when(greeter & (plane == 0))
    def _():
        signal(wave_sem.at[0], row_at(plane + 1), col)

    @pl.when(greeter & (plane == planes - 1))
    def _():
        signal(wave_sem.at[1], row_at(plane - 1), col)

    def piece(t, g):
        first, end = pieces[t][g]
        return pl.ds(first, end - first)

    def in_copy(t, g, k):
        other, r, q = member_at(k)
        d = order[t]
        first, end = pieces[t][g]
        top = pl.multiple_of(tile_at(d, other // col_devices) + first, 8)
        return pltpu.make_async_remote_copy(
            src_ref=frame.at[:, pl.ds(top, end - first), lanes_of(q)],
            dst_ref=gather.at[d, mine, :, piece(t, g)],
            send_sem=sent_sem,
            recv_sem=in_recv.at[piece_sem[t] + g],
            device_id=(r, q),
            device_id_type=MESH,
        )

    def in_arrival(t, g):
        ref = gather.at[order[t], pl.ds(0, members - 1), :, piece(t, g)]
        return several(ref, sent_sem, in_recv.at[piece_sem[t] + g])

    def if_sent(t, g, action):
        if pieces[t][g][0] < kept_rows:
            action(t, g)
        else:

            @pl.when(whole[t])
            def _():
                action(t, g)

    def send_piece(t, g):
        for k in far_first:
            in_copy(t, g, k).start()

    def seg_copy(k):
        other, r, q = member_at(k)
        return pltpu.make_async_remote_copy(
            src_ref=seg_own.at[other // col_devices],
            dst_ref=seg_in.at[mine],
            send_sem=sent_sem,
            recv_sem=seg_recv,
            device_id=(r, q),
            device_id_type=MESH,
        )

    def depth_of(raw):
        return jnp.exp(raw * slope_db - offset_zr)

    def sum_segments():
        near_lane = lax.broadcasted_iota(jnp.int32, (SEG, LANES), 1)
        for b in range(scan_block):
            for c in range(CORES):
                rows = pl.ds(c * half_rows, half_rows)
                total = jnp.zeros((half_rows, LANES), jnp.float32)
                for g in range(all_segs):
                    rest = depth_of(frame[b, rows, g * SEG : (g + 1) * SEG])
                    ones = jnp.where(near_lane == g, 1.0, 0.0).astype(jnp.bfloat16)
                    for _ in range(3):
                        head = rest.astype(jnp.bfloat16)
                        rest = rest - head.astype(jnp.float32)
                        total = total + jnp.dot(
                            head, ones, preferred_element_type=jnp.float32
                        )
                seg_own[c, b] = jnp.transpose(total)[:all_segs]

    frame_loaded(0)
    send_piece(0, 0)
    frame_loaded(1)
    sum_segments()
    for k in range(1, members):
        seg_copy(k).start()
    seg_in[mine] = seg_own[core]
    for t in range(planes):
        for g in range(len(pieces[t])):
            if t or g:
                if_sent(t, g, send_piece)

    for d in range(planes):
        rows = pl.ds(tile_at(d, core), tile_rows)
        gather[d, mine] = frame[:, rows, lanes_of(col)]

    def tell_core(sem):
        @pl.when(greeter)
        def _():
            for c in range(CORES - 1):
                signal(sem, plane * CORES + c, col)

        @pl.when(jnp.logical_not(greeter))
        def _():
            pl.semaphore_wait(sem, 1)


    @pl.when(greeter)
    def _():
        pl.semaphore_wait(wave_sem.at[2], 1)

    tell_core(wave_sem.at[0])

    def swap_rows(d, c):
        return pl.ds(pl.multiple_of(tile_at(d, c) + kept_rows, 8), SWAP_ROWS)

    def swap_copy(d, c, slot):
        return pltpu.make_async_remote_copy(
            src_ref=frame.at[:, swap_rows(d, c), :],
            dst_ref=swap_in.at[slot],
            send_sem=sent_sem,
            recv_sem=swap_recv,
            device_id=(d * CORES + c, col),
            device_id_type=MESH,
        )

    for c in range(CORES):
        swap_copy(twin, c, 1 + core).start()
    swap_copy(plane, 1 - core, 0).start()


    @pl.when(below)
    def _():
        pl.semaphore_wait(wave_sem.at[0], 1)

        @pl.when(above)
        def _():
            signal(wave_sem.at[0], row_at(plane + 1), col)

    @pl.when(above)
    def _():
        pl.semaphore_wait(wave_sem.at[1], 1)

        @pl.when(below)
        def _():
            signal(wave_sem.at[1], row_at(plane - 1), col)

    tell_core(wave_sem.at[1])

    several(plane_ids.at[pl.ds(0, members - 1)], id_send, id_recv).wait_recv()

    plane_block = pl.ds(plane * members, members)
    for k in range(1, planes):
        pltpu.make_async_remote_copy(
            src_ref=plane_ids,
            dst_ref=all_ids.at[plane_block],
            send_sem=id_send,
            recv_sem=idz_recv,
            device_id=(row_at((plane + k) % planes), col),
            device_id_type=MESH,
        ).start()
    all_ids[plane_block] = plane_ids[...]
    load_hours.wait()

    base_hour = first_hour(plane)
    span = hour_span(plane)
    pair_base = first_hour(2 * pair)
    spans = sorted({hour_span(p) for p in range(planes)})

    def by_span(action):
        for n in spans:

            @pl.when(span == n)
            def _():
                action(n)

    def side(p):
        return jnp.where(p == twin, 1, 0)

    def z_copy(t, g, k):
        return pltpu.make_async_remote_copy(
            src_ref=part.at[order[t], k, piece(t, g)],
            dst_ref=zrecv.at[plane * slots + k, piece(t, g)],
            send_sem=sent_sem,
            recv_sem=z_recv.at[side(order[t])],
            device_id=(row_at(order[t]), col),
            device_id_type=MESH,
        )

    def zseg_copy(k, n):
        return pltpu.make_async_remote_copy(
            src_ref=seg_part.at[pl.ds(0, n)],
            dst_ref=zseg.at[pl.ds(plane * slots, n)],
            send_sem=sent_sem,
            recv_sem=zseg_recv,
            device_id=(row_at((plane + k) % planes), col),
            device_id_type=MESH,
        )

    def pair_copy():
        return pltpu.make_async_remote_copy(
            src_ref=seg_hour.at[core],
            dst_ref=seg_hour.at[core],
            send_sem=sent_sem,
            recv_sem=pair_recv,
            device_id=(plane * CORES + 1 - core, col),
            device_id_type=MESH,
        )

    def wait_slots(ref, send_sem, recv_sem):
        for p in range(planes):
            n = sum(hour_span(o) for o in range(planes) if o != p)

            @pl.when(plane == p)
            def _():
                several(ref.at[pl.ds(0, n)], send_sem, recv_sem).wait_recv()

    def sum_planes(ref, h):
        total = None
        for p in range(planes):
            if first_hour(p) <= h < first_hour(p) + hour_span(p):
                term = ref[p * slots + h - first_hour(p)]
                total = term if total is None else total + term
        return total

    def add_by_hour(sums, raw, p, member, b, base):
        hour = hours[p * plane_scans + member * scan_block + b] - base
        return [
            total + jnp.where(hour == k, raw, 0.0) for k, total in enumerate(sums)
        ]

    def reduce_segments():
        several(seg_in.at[pl.ds(0, members - 1)], sent_sem, seg_recv).wait_recv()
        sums = [jnp.zeros((all_segs, half_rows), jnp.float32)] * slots
        for i in range(members):
            for b in range(scan_block):
                sums = add_by_hour(sums, seg_in[i, b], plane, i, b, base_hour)
        for k in range(slots):
            seg_part[k] = sums[k]
            zseg[plane * slots + k] = sums[k]

        def send(n):
            for k in range(1, planes):
                zseg_copy(k, n).start()

        by_span(send)

    def pair_segments():
        wait_slots(zseg, sent_sem, zseg_recv)
        for h in range(hour_count):
            seg_hour[core, h] = sum_planes(zseg, h)
        pair_copy().start()

    def lay_ids():
        several(
            all_ids.at[pl.ds(0, (planes - 1) * members)], id_send, idz_recv
        ).wait_recv()
        blocks = row_devices // CORES
        for c in range(CORES):
            lanes = []
            for r in range(c * blocks, (c + 1) * blocks):
                first = r * col_devices
                tiles = [all_ids[first + q] for q in range(col_devices)]
                lanes.append(jnp.concatenate(tiles, axis=0))
            flat_ids[c] = jnp.concatenate(lanes, axis=1)

    def basin_means():
        pair_copy().wait_recv()
        halves = [flat_ids[c] for c in range(CORES)]
        place = lax.broadcasted_iota(jnp.int32, (owned, half_rows), 0)
        zero = jnp.zeros((owned, half_rows), jnp.float32)
        totals = [zero] * hour_count
        count = zero
        for n in range(owned):
            hits = [half == me * owned + n for half in halves]
            for h in range(hour_count):
                kept = [jnp.where(hits[c], seg_hour[c, h], 0.0) for c in range(CORES)]
                kept = jnp.sum(sum(kept), axis=0, keepdims=True)
                totals[h] = jnp.where(place == n, kept, totals[h])
            found = sum(jnp.where(hit, float(SEG), 0.0) for hit in hits)
            count = jnp.where(place == n, jnp.sum(found, axis=0, keepdims=True), count)
        pixels = jnp.sum(count, axis=1, keepdims=True)
        lane = lax.broadcasted_iota(jnp.int32, (owned, LANES), 1)
        means = jnp.zeros((owned, LANES), jnp.float32)
        for h in range(hour_count):
            mean = jnp.sum(totals[h], axis=1, keepdims=True) / pixels
            means = jnp.where(lane == h, mean, means)
        basin_ref[...] = jnp.transpose(means)[:hour_count, :]

    def piece_sums(t, g):
        first, end = pieces[t][g]
        sums = [jnp.zeros((end - first, tile_cols), jnp.float32)] * slots
        for i in range(members):
            for b in range(scan_block):
                depth = depth_of(gather[order[t], i, b, piece(t, g)])
                sums = add_by_hour(sums, depth, plane, i, b, base_hour)
        return sums

    def push_piece(t, g):
        in_arrival(t, g).wait_recv()
        sums = piece_sums(t, g)
        for k in range(slots):
            part[order[t], k, piece(t, g)] = sums[k]
        for k in range(slots):

            @pl.when(k < span)
            def _():
                z_copy(t, g, k).start()

    def share_swap():
        several(swap_in, sent_sem, swap_recv).wait_recv()
        for k in range(col_devices - 1, -1, -1):
            _, r, q = member_at(k)
            lanes = lanes_of(q)
            sums = [jnp.zeros((SWAP_ROWS, tile_cols), jnp.float32)] * pair_slots
            for b in range(scan_block):
                sources = (
                    (frame[b, swap_rows(plane, core), lanes], plane, core),
                    (swap_in[0, b, :, lanes], plane, 1 - core),
                    (swap_in[1, b, :, lanes], twin, 0),
                    (swap_in[2, b, :, lanes], twin, 1),
                )
                for raw, p, c in sources:
                    member = c * col_devices + col
                    sums = add_by_hour(sums, depth_of(raw), p, member, b, pair_base)
            for n in range(pair_slots):
                gsum[k, n] = sums[n]
            if k > 0:
                pltpu.make_async_remote_copy(
                    src_ref=gsum.at[k],
                    dst_ref=grecv.at[col],
                    send_sem=sent_sem,
                    recv_sem=g_recv,
                    device_id=(r, q),
                    device_id_type=MESH,
                ).start()

    def join_swap():
        several(grecv.at[pl.ds(0, col_devices - 1)], sent_sem, g_recv).wait_recv()
        for n in range(pair_slots):
            total = gsum[0, n]
            for k in range(1, col_devices):
                _, _, q = member_at(k)
                total = total + grecv[q, n]

            @pl.when(n < pair_span(pair))
            def _():
                hourly_ref[pair_base + n, kept_rows:] = total

    for t in range(planes - 1):
        for g in range(len(pieces[t])):
            if_sent(t, g, push_piece)
            if t == 0 and g == 0:
                reduce_segments()
        if t == SHARE_AFTER:
            share_swap()
    lay_ids()
    pair_segments()
    hourly_ref[...] = jnp.zeros_like(hourly_ref)
    for g in range(len(pieces[-1])):
        in_arrival(planes - 1, g).wait_recv()
        sums = piece_sums(planes - 1, g)
        for k in range(slots):

            @pl.when(k < span)
            def _():
                hourly_ref[base_hour + k, piece(planes - 1, g)] = sums[k]

    basin_means()
    join_swap()

    for p in range(planes):
        other = p + 1 - 2 * (p % 2)
        n = sum(hour_span(o) for o in range(planes) if o not in (p, other))

        @pl.when(plane == p)
        def _():
            several(zrecv.at[pl.ds(0, n)], sent_sem, z_recv.at[0]).wait_recv()
            several(
                zrecv.at[pl.ds(0, hour_span(other)), pl.ds(0, kept_rows)],
                sent_sem,
                z_recv.at[1],
            ).wait_recv()

    for h in range(hour_count):
        hourly_ref[h] += sum_planes(zrecv, h)

    several(
        all_ids.at[pl.ds(0, planes * members - 1)], id_send, id_recv
    ).wait_send()
    def all_sent(n):
        count = sent_words(dims, scan_block, pair_slots, n) // (8 * LANES)
        several(spare.at[pl.ds(0, count)], sent_sem, swap_recv).wait_send()

    by_span(all_sent)


def write_out(hourly_ref, basin_ref, hourly_out, basin_out, sem):
    pairs = ((hourly_ref, hourly_out), (basin_ref, basin_out))
    copies = [pltpu.make_async_copy(s, d, sem.at[n]) for n, (s, d) in enumerate(pairs)]
    for copy in copies:
        copy.start()
    for copy in copies:
        copy.wait()


def body(reflectivity, scan_hour, basin_ids):
    row_devices = lax.axis_size("row")
    col_devices = lax.axis_size("col")
    scan_block, grid_height, grid_width = reflectivity.shape
    tile_rows = grid_height // row_devices
    tile_cols = grid_width // col_devices
    scan_count = scan_hour.shape[0]
    hour_count = (scan_count + 10) // HOUR_SCANS + 1
    devices = row_devices * col_devices
    owned = grid_height * grid_width // (SEG * BASIN_ROWS) // devices
    planes = row_devices // CORES
    members = CORES * col_devices
    plane_scans = members * scan_block

    def span_of(first, last):
        rest = scan_count - plane_scans * (last + 1)
        return hour_count - rest // HOUR_SCANS - (first * plane_scans) // HOUR_SCANS

    slots = max(span_of(p, p) for p in range(planes))
    pair_slots = max(span_of(2 * j, 2 * j + 1) for j in range(planes // 2))
    seg_shape = (grid_width // SEG, grid_height // CORES)
    dims = (row_devices, col_devices, hour_count, slots, tile_rows, tile_cols, owned)
    piece_count = len(FIRST) + len(LATER) * (planes - 2) + len(OWN)
    spare_count = sent_words(dims, scan_block, pair_slots, slots) // (8 * LANES)
    dma = pltpu.SemaphoreType.DMA
    f32 = jnp.float32
    id_shape = basin_ids.shape[::-1]
    anywhere = pl.BlockSpec(memory_space=pltpu.HBM)
    inside = pl.BlockSpec(memory_space=pltpu.VMEM)
    hourly, basin = pl.pallas_call(
        functools.partial(kernel, dims),
        out_shape=(
            jax.ShapeDtypeStruct((hour_count, tile_rows, tile_cols), f32),
            jax.ShapeDtypeStruct((hour_count, owned), f32),
        ),
        in_specs=[anywhere] * 3,
        out_specs=(inside, inside),
        scratch_shapes=[
            pltpu.VMEM(reflectivity.shape, f32),
            pltpu.SMEM(scan_hour.shape, jnp.int32),
            pltpu.VMEM(id_shape, jnp.int32),
            pltpu.VMEM((planes, members, scan_block, tile_rows, tile_cols), f32),
            pltpu.VMEM((planes, slots, tile_rows, tile_cols), f32),
            pltpu.VMEM((planes * slots, tile_rows, tile_cols), f32),
            pltpu.VMEM((members,) + id_shape, jnp.int32),
            pltpu.VMEM((planes * members,) + id_shape, jnp.int32),
            pltpu.VMEM((CORES,) + seg_shape, jnp.int32),
            pltpu.VMEM((CORES, scan_block) + seg_shape, f32),
            pltpu.VMEM((members, scan_block) + seg_shape, f32),
            pltpu.VMEM((slots,) + seg_shape, f32),
            pltpu.VMEM((planes * slots,) + seg_shape, f32),
            pltpu.VMEM((CORES, hour_count) + seg_shape, f32),
            pltpu.VMEM((CORES + 1, scan_block, SWAP_ROWS, grid_width), f32),
            pltpu.VMEM((col_devices, pair_slots, SWAP_ROWS, tile_cols), f32),
            pltpu.VMEM((col_devices, pair_slots, SWAP_ROWS, tile_cols), f32),
            pltpu.VMEM((spare_count, 8, LANES), f32),
            pltpu.SemaphoreType.REGULAR((3,)),
            dma((2,)),
            dma((2,)),
            dma,
            dma((piece_count,)),
            dma((2,)),
            dma,
            dma,
            dma,
            dma,
            dma,
            dma,
            dma,
            dma,
        ],
        compiler_params=pltpu.CompilerParams(
            collective_id=0, has_side_effects=True, vmem_limit_bytes=40 * 2**20
        ),
    )(*(pltpu.with_memory_space_constraint(v, pltpu.HBM) for v in (reflectivity, scan_hour, basin_ids.T)))
    hourly, basin = pl.pallas_call(
        write_out,
        out_shape=(
            jax.ShapeDtypeStruct(hourly.shape, f32),
            jax.ShapeDtypeStruct(basin.shape, f32),
        ),
        in_specs=[inside] * 2,
        out_specs=(anywhere, anywhere),
        scratch_shapes=[dma((2,))],
        compiler_params=pltpu.CompilerParams(vmem_limit_bytes=8 * 2**20),
    )(hourly, basin)
    return hourly, basin.T


def solution(mesh):
    placed = (P(("row", "col"), None, None), P(), P("row", "col"))
    return jax.shard_map(
        body,
        mesh=mesh,
        in_specs=placed,
        out_specs=(P(None, "row", "col"), P(("row", "col"), None)),
        check_vma=False,
    )
```

```python
import functools
import math

import jax
import jax.numpy as jnp
from jax import lax
from jax.experimental import pallas as pl
from jax.experimental.pallas import tpu as pltpu
from jax.sharding import PartitionSpec as P

SEG = 128
BASIN_ROWS = 8
HOUR_SCANS = 12
CORES = 2
LANES = 128
FIRST = (8, 16, 32)
LATER = (16, 32)
OWN = (16,)
SWAP_ROWS = 16
SHARE_AFTER = 1
MESH = pl.DeviceIdType.MESH

slope_db = math.log(10.0) / 16.0
offset_zr = math.log(200.0) / 1.6 + math.log(12.0)


def sent_words(dims, scan_block, pair_slots, span):
    row_devices, col_devices, hour_count, slots, tile_rows, tile_cols, owned = dims
    planes = row_devices // CORES
    members = CORES * col_devices
    kept_rows = tile_rows - SWAP_ROWS
    seg_words = row_devices * tile_rows // CORES * col_devices * tile_cols // SEG
    chunk_rows = (planes - 2) * tile_rows + kept_rows
    pixels = (members - 1) * (chunk_rows + kept_rows) * tile_cols * scan_block
    segments = ((members - 1) * scan_block + hour_count) * seg_words
    swapped = (CORES + 1) * SWAP_ROWS * col_devices * tile_cols * scan_block
    shared = (col_devices - 1) * pair_slots * SWAP_ROWS * tile_cols
    sums = span * (chunk_rows * tile_cols + (planes - 1) * seg_words)
    return pixels + segments + swapped + shared + sums


def kernel(
    dims,
    refl_ref,
    hour_ref,
    ids_ref,
    hourly_ref,
    basin_ref,
    frame,
    hours,
    ids,
    gather,
    part,
    zrecv,
    plane_ids,
    all_ids,
    flat_ids,
    seg_own,
    seg_in,
    seg_part,
    zseg,
    seg_hour,
    swap_in,
    gsum,
    grecv,
    spare,
    wave_sem,
    local_sem,
    load_sem,
    sent_sem,
    in_recv,
    z_recv,
    id_send,
    id_recv,
    idz_recv,
    seg_recv,
    zseg_recv,
    pair_recv,
    swap_recv,
    g_recv,
):
    row_devices, col_devices, hour_count, slots, tile_rows, tile_cols, owned = dims
    planes = row_devices // CORES
    members = CORES * col_devices
    devices = row_devices * col_devices
    scan_block = gather.shape[2]
    scan_count = hour_ref.shape[0]
    plane_scans = members * scan_block
    cuts = [FIRST] + [LATER] * (planes - 2) + [OWN]
    pieces = [list(zip((0,) + ends[:-1], ends)) for ends in cuts]
    piece_sem = [sum(map(len, cuts[:t])) for t in range(planes)]
    all_segs, half_rows = seg_own.shape[2:]
    kept_rows = tile_rows - SWAP_ROWS
    pair_slots = gsum.shape[1]

    row = lax.axis_index("row")
    col = lax.axis_index("col")
    plane = row // CORES
    core = row % CORES
    mine = core * col_devices + col
    me = row * col_devices + col
    pair = plane // 2
    twin = plane + 1 - 2 * (plane % 2)

    def first_hour(p):
        return (p * plane_scans) // HOUR_SCANS

    def hour_span(p):
        rest = scan_count - plane_scans - p * plane_scans
        return hour_count - rest // HOUR_SCANS - first_hour(p)

    def pair_span(j):
        return first_hour(2 * j + 1) + hour_span(2 * j + 1) - first_hour(2 * j)

    def by_plane(table):
        value = table[0]
        for p in range(1, planes):
            value = jnp.where(plane == p, table[p], value)
        return value

    def chunk_order(p):
        others = sorted((d for d in range(planes) if d != p), key=lambda d: -abs(d - p))
        if 0 in others:
            others.remove(0)
            others.insert(0, 0)
        return others + [p]

    orders = [chunk_order(p) for p in range(planes)]
    order = [by_plane([o[t] for o in orders]) for t in range(planes)]
    whole = [order[t] != twin for t in range(planes)]

    def member_at(k):
        dc = k // col_devices
        dq = k % col_devices
        half = col_devices // 2
        qq = ((col // 2 + dq // 2) % half) * 2 + (col + dq) % 2
        other = ((core + dc) % CORES) * col_devices + qq
        return other, plane * CORES + other // col_devices, other % col_devices

    def several(ref, send_sem, recv_sem):
        return pltpu.make_async_remote_copy(
            src_ref=ref,
            dst_ref=ref,
            send_sem=send_sem,
            recv_sem=recv_sem,
            device_id=((row + 1) % row_devices, col),
            device_id_type=MESH,
        )

    def signal(sem, r, q):
        pl.semaphore_signal(sem, inc=1, device_id=(r, q), device_id_type=MESH)

    def row_at(p):
        return p * CORES + core

    barrier = pltpu.get_barrier_semaphore()
    far_first = sorted(range(1, members), key=lambda k: (-(k % col_devices), k))
    for k in far_first:
        _, r, q = member_at(k)
        signal(barrier, r, q)

    greeter = core == CORES - 1
    below = greeter & (plane > 0)
    above = greeter & (plane < planes - 1)

    @pl.when(below)
    def _():
        signal(barrier, row_at(plane - 1), col)

    @pl.when(above)
    def _():
        signal(barrier, row_at(plane + 1), col)

    def tile_at(d, c):
        return pl.multiple_of((d * CORES + c) * tile_rows, 8)

    def lanes_of(q):
        return pl.ds(pl.multiple_of(q * tile_cols, 128), tile_cols)

    def plane_rows(d):
        rows = CORES * tile_rows
        return pl.ds(pl.multiple_of(d * rows, 8), rows)

    load_ids = pltpu.make_async_copy(ids_ref, ids, local_sem.at[0])
    load_ids.start()
    for t, d in enumerate(order):
        pltpu.make_async_copy(
            refl_ref.at[:, plane_rows(d), :],
            frame.at[:, plane_rows(d), :],
            load_sem.at[min(t, 1)],
        ).start()

    def frame_loaded(late):
        count = (planes - 1 if late else 1) * CORES * tile_rows
        rows = frame.at[:, pl.ds(0, count), :]
        pltpu.make_async_copy(rows, rows, load_sem.at[late]).wait()

    load_hours = pltpu.make_async_copy(hour_ref, hours, local_sem.at[1])
    load_hours.start()
    for k in range(slots):
        zrecv[plane * slots + k] = jnp.zeros((tile_rows, tile_cols), jnp.float32)
        zrecv[twin * slots + k, kept_rows:] = jnp.zeros(
            (SWAP_ROWS, tile_cols), jnp.float32
        )

    load_ids.wait()
    plane_ids[mine] = ids[...]
    beside = jnp.where(below, 1, 0) + jnp.where(above, 1, 0)
    pl.semaphore_wait(barrier, members - 1 + beside)

    def id_copy(k):
        other, r, q = member_at(k)
        return pltpu.make_async_remote_copy(
            src_ref=ids,
            dst_ref=plane_ids.at[mine],
            send_sem=id_send,
            recv_sem=id_recv,
            device_id=(r, q),
            device_id_type=MESH,
        )

    for k in range(1, members):
        id_copy(k).start()

    @pl.when(greeter)
    def _():
        signal(wave_sem.at[2], row_at(twin), col)

    @pl.when(greeter & (plane == 0))
    def _():
        signal(wave_sem.at[0], row_at(plane + 1), col)

    @pl.when(greeter & (plane == planes - 1))
    def _():
        signal(wave_sem.at[1], row_at(plane - 1), col)

    def piece(t, g):
        first, end = pieces[t][g]
        return pl.ds(first, end - first)

    def in_copy(t, g, k):
        other, r, q = member_at(k)
        d = order[t]
        first, end = pieces[t][g]
        top = pl.multiple_of(tile_at(d, other // col_devices) + first, 8)
        return pltpu.make_async_remote_copy(
            src_ref=frame.at[:, pl.ds(top, end - first), lanes_of(q)],
            dst_ref=gather.at[d, mine, :, piece(t, g)],
            send_sem=sent_sem,
            recv_sem=in_recv.at[piece_sem[t] + g],
            device_id=(r, q),
            device_id_type=MESH,
        )

    def in_arrival(t, g):
        ref = gather.at[order[t], pl.ds(0, members - 1), :, piece(t, g)]
        return several(ref, sent_sem, in_recv.at[piece_sem[t] + g])

    def if_sent(t, g, action):
        if pieces[t][g][0] < kept_rows:
            action(t, g)
        else:

            @pl.when(whole[t])
            def _():
                action(t, g)

    def send_piece(t, g):
        for k in sorted(range(1, members), key=lambda k: (-(k % col_devices), -k)):
            in_copy(t, g, k).start()

    def seg_copy(k):
        other, r, q = member_at(k)
        return pltpu.make_async_remote_copy(
            src_ref=seg_own.at[other // col_devices],
            dst_ref=seg_in.at[mine],
            send_sem=sent_sem,
            recv_sem=seg_recv,
            device_id=(r, q),
            device_id_type=MESH,
        )

    def depth_of(raw):
        return jnp.exp(raw * slope_db - offset_zr)

    def sum_segments():
        near_lane = lax.broadcasted_iota(jnp.int32, (SEG, LANES), 1)
        for b in range(scan_block):
            for c in range(CORES):
                rows = pl.ds(c * half_rows, half_rows)
                total = jnp.zeros((half_rows, LANES), jnp.float32)
                for g in range(all_segs):
                    rest = depth_of(frame[b, rows, g * SEG : (g + 1) * SEG])
                    ones = jnp.where(near_lane == g, 1.0, 0.0).astype(jnp.bfloat16)
                    for _ in range(3):
                        head = rest.astype(jnp.bfloat16)
                        rest = rest - head.astype(jnp.float32)
                        total = total + jnp.dot(
                            head, ones, preferred_element_type=jnp.float32
                        )
                seg_own[c, b] = jnp.transpose(total)[:all_segs]

    frame_loaded(0)
    send_piece(0, 0)
    frame_loaded(1)
    sum_segments()
    for k in range(1, members):
        seg_copy(k).start()
    seg_in[mine] = seg_own[core]
    for t in range(planes):
        for g in range(len(pieces[t])):
            if t or g:
                if_sent(t, g, send_piece)

    for d in range(planes):
        rows = pl.ds(tile_at(d, core), tile_rows)
        gather[d, mine] = frame[:, rows, lanes_of(col)]

    def tell_core(sem):
        @pl.when(greeter)
        def _():
            for c in range(CORES - 1):
                signal(sem, plane * CORES + c, col)

        @pl.when(jnp.logical_not(greeter))
        def _():
            pl.semaphore_wait(sem, 1)


    @pl.when(greeter)
    def _():
        pl.semaphore_wait(wave_sem.at[2], 1)

    tell_core(wave_sem.at[0])

    def swap_rows(d, c):
        return pl.ds(pl.multiple_of(tile_at(d, c) + kept_rows, 8), SWAP_ROWS)

    def swap_copy(d, c, slot):
        return pltpu.make_async_remote_copy(
            src_ref=frame.at[:, swap_rows(d, c), :],
            dst_ref=swap_in.at[slot],
            send_sem=sent_sem,
            recv_sem=swap_recv,
            device_id=(d * CORES + c, col),
            device_id_type=MESH,
        )

    for c in range(CORES):
        swap_copy(twin, c, 1 + core).start()
    swap_copy(plane, 1 - core, 0).start()


    @pl.when(below)
    def _():
        pl.semaphore_wait(wave_sem.at[0], 1)

        @pl.when(above)
        def _():
            signal(wave_sem.at[0], row_at(plane + 1), col)

    @pl.when(above)
    def _():
        pl.semaphore_wait(wave_sem.at[1], 1)

        @pl.when(below)
        def _():
            signal(wave_sem.at[1], row_at(plane - 1), col)

    tell_core(wave_sem.at[1])

    several(plane_ids.at[pl.ds(0, members - 1)], id_send, id_recv).wait_recv()

    plane_block = pl.ds(plane * members, members)
    for k in range(1, planes):
        pltpu.make_async_remote_copy(
            src_ref=plane_ids,
            dst_ref=all_ids.at[plane_block],
            send_sem=id_send,
            recv_sem=idz_recv,
            device_id=(row_at((plane + k) % planes), col),
            device_id_type=MESH,
        ).start()
    all_ids[plane_block] = plane_ids[...]
    load_hours.wait()

    base_hour = first_hour(plane)
    span = hour_span(plane)
    pair_base = first_hour(2 * pair)
    spans = sorted({hour_span(p) for p in range(planes)})

    def by_span(action):
        for n in spans:

            @pl.when(span == n)
            def _():
                action(n)

    def side(p):
        return jnp.where(p == twin, 1, 0)

    def z_copy(t, g, k):
        return pltpu.make_async_remote_copy(
            src_ref=part.at[order[t], k, piece(t, g)],
            dst_ref=zrecv.at[plane * slots + k, piece(t, g)],
            send_sem=sent_sem,
            recv_sem=z_recv.at[side(order[t])],
            device_id=(row_at(order[t]), col),
            device_id_type=MESH,
        )

    def zseg_copy(k, n):
        return pltpu.make_async_remote_copy(
            src_ref=seg_part.at[pl.ds(0, n)],
            dst_ref=zseg.at[pl.ds(plane * slots, n)],
            send_sem=sent_sem,
            recv_sem=zseg_recv,
            device_id=(row_at((plane + k) % planes), col),
            device_id_type=MESH,
        )

    def pair_copy():
        return pltpu.make_async_remote_copy(
            src_ref=seg_hour.at[core],
            dst_ref=seg_hour.at[core],
            send_sem=sent_sem,
            recv_sem=pair_recv,
            device_id=(plane * CORES + 1 - core, col),
            device_id_type=MESH,
        )

    def wait_slots(ref, send_sem, recv_sem):
        for p in range(planes):
            n = sum(hour_span(o) for o in range(planes) if o != p)

            @pl.when(plane == p)
            def _():
                several(ref.at[pl.ds(0, n)], send_sem, recv_sem).wait_recv()

    def sum_planes(ref, h):
        total = None
        for p in range(planes):
            if first_hour(p) <= h < first_hour(p) + hour_span(p):
                term = ref[p * slots + h - first_hour(p)]
                total = term if total is None else total + term
        return total

    def add_by_hour(sums, raw, p, member, b, base):
        hour = hours[p * plane_scans + member * scan_block + b] - base
        return [
            total + jnp.where(hour == k, raw, 0.0) for k, total in enumerate(sums)
        ]

    def reduce_segments():
        several(seg_in.at[pl.ds(0, members - 1)], sent_sem, seg_recv).wait_recv()
        sums = [jnp.zeros((all_segs, half_rows), jnp.float32)] * slots
        for i in range(members):
            for b in range(scan_block):
                sums = add_by_hour(sums, seg_in[i, b], plane, i, b, base_hour)
        for k in range(slots):
            seg_part[k] = sums[k]
            zseg[plane * slots + k] = sums[k]

        def send(n):
            for k in range(1, planes):
                zseg_copy(k, n).start()

        by_span(send)

    def pair_segments():
        wait_slots(zseg, sent_sem, zseg_recv)
        for h in range(hour_count):
            seg_hour[core, h] = sum_planes(zseg, h)
        pair_copy().start()

    def lay_ids():
        several(
            all_ids.at[pl.ds(0, (planes - 1) * members)], id_send, idz_recv
        ).wait_recv()
        blocks = row_devices // CORES
        for c in range(CORES):
            lanes = []
            for r in range(c * blocks, (c + 1) * blocks):
                first = r * col_devices
                tiles = [all_ids[first + q] for q in range(col_devices)]
                lanes.append(jnp.concatenate(tiles, axis=0))
            flat_ids[c] = jnp.concatenate(lanes, axis=1)

    def basin_means():
        pair_copy().wait_recv()
        halves = [flat_ids[c] for c in range(CORES)]
        place = lax.broadcasted_iota(jnp.int32, (owned, half_rows), 0)
        zero = jnp.zeros((owned, half_rows), jnp.float32)
        totals = [zero] * hour_count
        count = zero
        for n in range(owned):
            hits = [half == me * owned + n for half in halves]
            for h in range(hour_count):
                kept = [jnp.where(hits[c], seg_hour[c, h], 0.0) for c in range(CORES)]
                kept = jnp.sum(sum(kept), axis=0, keepdims=True)
                totals[h] = jnp.where(place == n, kept, totals[h])
            found = sum(jnp.where(hit, float(SEG), 0.0) for hit in hits)
            count = jnp.where(place == n, jnp.sum(found, axis=0, keepdims=True), count)
        pixels = jnp.sum(count, axis=1, keepdims=True)
        lane = lax.broadcasted_iota(jnp.int32, (owned, LANES), 1)
        means = jnp.zeros((owned, LANES), jnp.float32)
        for h in range(hour_count):
            mean = jnp.sum(totals[h], axis=1, keepdims=True) / pixels
            means = jnp.where(lane == h, mean, means)
        basin_ref[...] = jnp.transpose(means)[:hour_count, :]

    def piece_sums(t, g):
        first, end = pieces[t][g]
        sums = [jnp.zeros((end - first, tile_cols), jnp.float32)] * slots
        for i in range(members):
            for b in range(scan_block):
                depth = depth_of(gather[order[t], i, b, piece(t, g)])
                sums = add_by_hour(sums, depth, plane, i, b, base_hour)
        return sums

    def push_piece(t, g):
        in_arrival(t, g).wait_recv()
        sums = piece_sums(t, g)
        for k in range(slots):
            part[order[t], k, piece(t, g)] = sums[k]
        for k in range(slots):

            @pl.when(k < span)
            def _():
                z_copy(t, g, k).start()

    def share_swap():
        several(swap_in, sent_sem, swap_recv).wait_recv()
        for k in range(col_devices - 1, -1, -1):
            _, r, q = member_at(k)
            lanes = lanes_of(q)
            sums = [jnp.zeros((SWAP_ROWS, tile_cols), jnp.float32)] * pair_slots
            for b in range(scan_block):
                sources = (
                    (frame[b, swap_rows(plane, core), lanes], plane, core),
                    (swap_in[0, b, :, lanes], plane, 1 - core),
                    (swap_in[1, b, :, lanes], twin, 0),
                    (swap_in[2, b, :, lanes], twin, 1),
                )
                for raw, p, c in sources:
                    member = c * col_devices + col
                    sums = add_by_hour(sums, depth_of(raw), p, member, b, pair_base)
            for n in range(pair_slots):
                gsum[k, n] = sums[n]
            if k > 0:
                pltpu.make_async_remote_copy(
                    src_ref=gsum.at[k],
                    dst_ref=grecv.at[col],
                    send_sem=sent_sem,
                    recv_sem=g_recv,
                    device_id=(r, q),
                    device_id_type=MESH,
                ).start()

    def join_swap():
        several(grecv.at[pl.ds(0, col_devices - 1)], sent_sem, g_recv).wait_recv()
        for n in range(pair_slots):
            total = gsum[0, n]
            for k in range(1, col_devices):
                _, _, q = member_at(k)
                total = total + grecv[q, n]

            @pl.when(n < pair_span(pair))
            def _():
                hourly_ref[pair_base + n, kept_rows:] = total

    for t in range(planes - 1):
        for g in range(len(pieces[t])):
            if_sent(t, g, push_piece)
            if t == 0 and g == 0:
                reduce_segments()
        if t == SHARE_AFTER:
            share_swap()
    lay_ids()
    pair_segments()
    hourly_ref[...] = jnp.zeros_like(hourly_ref)
    for g in range(len(pieces[-1])):
        in_arrival(planes - 1, g).wait_recv()
        sums = piece_sums(planes - 1, g)
        for k in range(slots):

            @pl.when(k < span)
            def _():
                hourly_ref[base_hour + k, piece(planes - 1, g)] = sums[k]

    basin_means()
    join_swap()

    for p in range(planes):
        other = p + 1 - 2 * (p % 2)
        n = sum(hour_span(o) for o in range(planes) if o not in (p, other))

        @pl.when(plane == p)
        def _():
            several(zrecv.at[pl.ds(0, n)], sent_sem, z_recv.at[0]).wait_recv()
            several(
                zrecv.at[pl.ds(0, hour_span(other)), pl.ds(0, kept_rows)],
                sent_sem,
                z_recv.at[1],
            ).wait_recv()

    for h in range(hour_count):
        hourly_ref[h] += sum_planes(zrecv, h)

    several(
        all_ids.at[pl.ds(0, planes * members - 1)], id_send, id_recv
    ).wait_send()
    def all_sent(n):
        count = sent_words(dims, scan_block, pair_slots, n) // (8 * LANES)
        several(spare.at[pl.ds(0, count)], sent_sem, swap_recv).wait_send()

    by_span(all_sent)


def write_out(hourly_ref, basin_ref, hourly_out, basin_out, sem):
    pairs = ((hourly_ref, hourly_out), (basin_ref, basin_out))
    copies = [pltpu.make_async_copy(s, d, sem.at[n]) for n, (s, d) in enumerate(pairs)]
    for copy in copies:
        copy.start()
    for copy in copies:
        copy.wait()


def body(reflectivity, scan_hour, basin_ids):
    row_devices = lax.axis_size("row")
    col_devices = lax.axis_size("col")
    scan_block, grid_height, grid_width = reflectivity.shape
    tile_rows = grid_height // row_devices
    tile_cols = grid_width // col_devices
    scan_count = scan_hour.shape[0]
    hour_count = (scan_count + 10) // HOUR_SCANS + 1
    devices = row_devices * col_devices
    owned = grid_height * grid_width // (SEG * BASIN_ROWS) // devices
    planes = row_devices // CORES
    members = CORES * col_devices
    plane_scans = members * scan_block

    def span_of(first, last):
        rest = scan_count - plane_scans * (last + 1)
        return hour_count - rest // HOUR_SCANS - (first * plane_scans) // HOUR_SCANS

    slots = max(span_of(p, p) for p in range(planes))
    pair_slots = max(span_of(2 * j, 2 * j + 1) for j in range(planes // 2))
    seg_shape = (grid_width // SEG, grid_height // CORES)
    dims = (row_devices, col_devices, hour_count, slots, tile_rows, tile_cols, owned)
    piece_count = len(FIRST) + len(LATER) * (planes - 2) + len(OWN)
    spare_count = sent_words(dims, scan_block, pair_slots, slots) // (8 * LANES)
    dma = pltpu.SemaphoreType.DMA
    f32 = jnp.float32
    id_shape = basin_ids.shape[::-1]
    anywhere = pl.BlockSpec(memory_space=pltpu.HBM)
    inside = pl.BlockSpec(memory_space=pltpu.VMEM)
    hourly, basin = pl.pallas_call(
        functools.partial(kernel, dims),
        out_shape=(
            jax.ShapeDtypeStruct((hour_count, tile_rows, tile_cols), f32),
            jax.ShapeDtypeStruct((hour_count, owned), f32),
        ),
        in_specs=[anywhere] * 3,
        out_specs=(inside, inside),
        scratch_shapes=[
            pltpu.VMEM(reflectivity.shape, f32),
            pltpu.SMEM(scan_hour.shape, jnp.int32),
            pltpu.VMEM(id_shape, jnp.int32),
            pltpu.VMEM((planes, members, scan_block, tile_rows, tile_cols), f32),
            pltpu.VMEM((planes, slots, tile_rows, tile_cols), f32),
            pltpu.VMEM((planes * slots, tile_rows, tile_cols), f32),
            pltpu.VMEM((members,) + id_shape, jnp.int32),
            pltpu.VMEM((planes * members,) + id_shape, jnp.int32),
            pltpu.VMEM((CORES,) + seg_shape, jnp.int32),
            pltpu.VMEM((CORES, scan_block) + seg_shape, f32),
            pltpu.VMEM((members, scan_block) + seg_shape, f32),
            pltpu.VMEM((slots,) + seg_shape, f32),
            pltpu.VMEM((planes * slots,) + seg_shape, f32),
            pltpu.VMEM((CORES, hour_count) + seg_shape, f32),
            pltpu.VMEM((CORES + 1, scan_block, SWAP_ROWS, grid_width), f32),
            pltpu.VMEM((col_devices, pair_slots, SWAP_ROWS, tile_cols), f32),
            pltpu.VMEM((col_devices, pair_slots, SWAP_ROWS, tile_cols), f32),
            pltpu.VMEM((spare_count, 8, LANES), f32),
            pltpu.SemaphoreType.REGULAR((3,)),
            dma((2,)),
            dma((2,)),
            dma,
            dma((piece_count,)),
            dma((2,)),
            dma,
            dma,
            dma,
            dma,
            dma,
            dma,
            dma,
            dma,
        ],
        compiler_params=pltpu.CompilerParams(
            collective_id=0, has_side_effects=True, vmem_limit_bytes=40 * 2**20
        ),
    )(*(pltpu.with_memory_space_constraint(v, pltpu.HBM) for v in (reflectivity, scan_hour, basin_ids.T)))
    hourly, basin = pl.pallas_call(
        write_out,
        out_shape=(
            jax.ShapeDtypeStruct(hourly.shape, f32),
            jax.ShapeDtypeStruct(basin.shape, f32),
        ),
        in_specs=[inside] * 2,
        out_specs=(anywhere, anywhere),
        scratch_shapes=[dma((2,))],
        compiler_params=pltpu.CompilerParams(vmem_limit_bytes=8 * 2**20),
    )(hourly, basin)
    return hourly, basin.T


def solution(mesh):
    placed = (P(("row", "col"), None, None), P(), P("row", "col"))
    return jax.shard_map(
        body,
        mesh=mesh,
        in_specs=placed,
        out_specs=(P(None, "row", "col"), P(("row", "col"), None)),
        check_vma=False,
    )
```

```python
import functools
import math

import jax
import jax.numpy as jnp
from jax import lax
from jax.experimental import pallas as pl
from jax.experimental.pallas import tpu as pltpu
from jax.sharding import PartitionSpec as P

SEG = 128
BASIN_ROWS = 8
HOUR_SCANS = 12
CORES = 2
LANES = 128
FIRST = (8, 16, 32)
LATER = (16, 32)
OWN = (16,)
SWAP_ROWS = 16
SHARE_AFTER = 1
MESH = pl.DeviceIdType.MESH

slope_db = math.log(10.0) / 16.0
offset_zr = math.log(200.0) / 1.6 + math.log(12.0)


def sent_words(dims, scan_block, pair_slots, span):
    row_devices, col_devices, hour_count, slots, tile_rows, tile_cols, owned = dims
    planes = row_devices // CORES
    members = CORES * col_devices
    kept_rows = tile_rows - SWAP_ROWS
    seg_words = row_devices * tile_rows // CORES * col_devices * tile_cols // SEG
    chunk_rows = (planes - 2) * tile_rows + kept_rows
    pixels = (members - 1) * (chunk_rows + kept_rows) * tile_cols * scan_block
    segments = ((members - 1) * scan_block + hour_count) * seg_words
    swapped = (CORES + 1) * SWAP_ROWS * col_devices * tile_cols * scan_block
    shared = (col_devices - 1) * pair_slots * SWAP_ROWS * tile_cols
    sums = span * (chunk_rows * tile_cols + (planes - 1) * seg_words)
    return pixels + segments + swapped + shared + sums


def kernel(
    dims,
    refl_ref,
    hour_ref,
    ids_ref,
    hourly_ref,
    basin_ref,
    frame,
    hours,
    ids,
    gather,
    part,
    zrecv,
    plane_ids,
    all_ids,
    flat_ids,
    seg_own,
    seg_in,
    seg_part,
    zseg,
    seg_hour,
    swap_in,
    gsum,
    grecv,
    spare,
    wave_sem,
    local_sem,
    load_sem,
    sent_sem,
    in_recv,
    z_recv,
    id_send,
    id_recv,
    idz_recv,
    seg_recv,
    zseg_recv,
    pair_recv,
    swap_recv,
    g_recv,
):
    row_devices, col_devices, hour_count, slots, tile_rows, tile_cols, owned = dims
    planes = row_devices // CORES
    members = CORES * col_devices
    devices = row_devices * col_devices
    scan_block = gather.shape[2]
    scan_count = hour_ref.shape[0]
    plane_scans = members * scan_block
    cuts = [FIRST] + [LATER] * (planes - 2) + [OWN]
    pieces = [list(zip((0,) + ends[:-1], ends)) for ends in cuts]
    piece_sem = [sum(map(len, cuts[:t])) for t in range(planes)]
    all_segs, half_rows = seg_own.shape[2:]
    kept_rows = tile_rows - SWAP_ROWS
    pair_slots = gsum.shape[1]

    row = lax.axis_index("row")
    col = lax.axis_index("col")
    plane = row // CORES
    core = row % CORES
    mine = core * col_devices + col
    me = row * col_devices + col
    pair = plane // 2
    twin = plane + 1 - 2 * (plane % 2)

    def first_hour(p):
        return (p * plane_scans) // HOUR_SCANS

    def hour_span(p):
        rest = scan_count - plane_scans - p * plane_scans
        return hour_count - rest // HOUR_SCANS - first_hour(p)

    def pair_span(j):
        return first_hour(2 * j + 1) + hour_span(2 * j + 1) - first_hour(2 * j)

    def by_plane(table):
        value = table[0]
        for p in range(1, planes):
            value = jnp.where(plane == p, table[p], value)
        return value

    def chunk_order(p):
        others = sorted((d for d in range(planes) if d != p), key=lambda d: -abs(d - p))
        if 0 in others:
            others.remove(0)
            others.insert(0, 0)
        return others + [p]

    orders = [chunk_order(p) for p in range(planes)]
    order = [by_plane([o[t] for o in orders]) for t in range(planes)]
    whole = [order[t] != twin for t in range(planes)]

    def member_at(k):
        dc = k // col_devices
        dq = k % col_devices
        half = col_devices // 2
        qq = ((col // 2 + dq // 2) % half) * 2 + (col + dq) % 2
        other = ((core + dc) % CORES) * col_devices + qq
        return other, plane * CORES + other // col_devices, other % col_devices

    def several(ref, send_sem, recv_sem):
        return pltpu.make_async_remote_copy(
            src_ref=ref,
            dst_ref=ref,
            send_sem=send_sem,
            recv_sem=recv_sem,
            device_id=((row + 1) % row_devices, col),
            device_id_type=MESH,
        )

    def signal(sem, r, q):
        pl.semaphore_signal(sem, inc=1, device_id=(r, q), device_id_type=MESH)

    def row_at(p):
        return p * CORES + core

    barrier = pltpu.get_barrier_semaphore()
    far_first = sorted(range(1, members), key=lambda k: (-(k % col_devices), k))
    for k in far_first:
        _, r, q = member_at(k)
        signal(barrier, r, q)

    greeter = core == CORES - 1
    below = greeter & (plane > 0)
    above = greeter & (plane < planes - 1)

    @pl.when(below)
    def _():
        signal(barrier, row_at(plane - 1), col)

    @pl.when(above)
    def _():
        signal(barrier, row_at(plane + 1), col)

    def tile_at(d, c):
        return pl.multiple_of((d * CORES + c) * tile_rows, 8)

    def lanes_of(q):
        return pl.ds(pl.multiple_of(q * tile_cols, 128), tile_cols)

    def plane_rows(d):
        rows = CORES * tile_rows
        return pl.ds(pl.multiple_of(d * rows, 8), rows)

    load_ids = pltpu.make_async_copy(ids_ref, ids, local_sem.at[0])
    load_ids.start()
    for t, d in enumerate(order):
        pltpu.make_async_copy(
            refl_ref.at[:, plane_rows(d), :],
            frame.at[:, plane_rows(d), :],
            load_sem.at[min(t, 1)],
        ).start()

    def frame_loaded(late):
        count = (planes - 1 if late else 1) * CORES * tile_rows
        rows = frame.at[:, pl.ds(0, count), :]
        pltpu.make_async_copy(rows, rows, load_sem.at[late]).wait()

    load_hours = pltpu.make_async_copy(hour_ref, hours, local_sem.at[1])
    load_hours.start()
    for k in range(slots):
        zrecv[plane * slots + k] = jnp.zeros((tile_rows, tile_cols), jnp.float32)
        zrecv[twin * slots + k, kept_rows:] = jnp.zeros(
            (SWAP_ROWS, tile_cols), jnp.float32
        )

    load_ids.wait()
    plane_ids[mine] = ids[...]
    beside = jnp.where(below, 1, 0) + jnp.where(above, 1, 0)
    pl.semaphore_wait(barrier, members - 1 + beside)

    def id_copy(k):
        other, r, q = member_at(k)
        return pltpu.make_async_remote_copy(
            src_ref=ids,
            dst_ref=plane_ids.at[mine],
            send_sem=id_send,
            recv_sem=id_recv,
            device_id=(r, q),
            device_id_type=MESH,
        )

    for k in range(1, members):
        id_copy(k).start()

    @pl.when(greeter)
    def _():
        signal(wave_sem.at[2], row_at(twin), col)

    @pl.when(greeter & (plane == 0))
    def _():
        signal(wave_sem.at[0], row_at(plane + 1), col)

    @pl.when(greeter & (plane == planes - 1))
    def _():
        signal(wave_sem.at[1], row_at(plane - 1), col)

    def piece(t, g):
        first, end = pieces[t][g]
        return pl.ds(first, end - first)

    def in_copy(t, g, k):
        other, r, q = member_at(k)
        d = order[t]
        first, end = pieces[t][g]
        top = pl.multiple_of(tile_at(d, other // col_devices) + first, 8)
        return pltpu.make_async_remote_copy(
            src_ref=frame.at[:, pl.ds(top, end - first), lanes_of(q)],
            dst_ref=gather.at[d, mine, :, piece(t, g)],
            send_sem=sent_sem,
            recv_sem=in_recv.at[piece_sem[t] + g],
            device_id=(r, q),
            device_id_type=MESH,
        )

    def in_arrival(t, g):
        ref = gather.at[order[t], pl.ds(0, members - 1), :, piece(t, g)]
        return several(ref, sent_sem, in_recv.at[piece_sem[t] + g])

    def if_sent(t, g, action):
        if pieces[t][g][0] < kept_rows:
            action(t, g)
        else:

            @pl.when(whole[t])
            def _():
                action(t, g)

    def send_piece(t, g):
        for k in sorted(range(1, members), key=lambda k: (-(k % col_devices), -k)):
            in_copy(t, g, k).start()

    def seg_copy(k):
        other, r, q = member_at(k)
        return pltpu.make_async_remote_copy(
            src_ref=seg_own.at[other // col_devices],
            dst_ref=seg_in.at[mine],
            send_sem=sent_sem,
            recv_sem=seg_recv,
            device_id=(r, q),
            device_id_type=MESH,
        )

    def depth_of(raw):
        return jnp.exp(raw * slope_db - offset_zr)

    def sum_segments():
        near_lane = lax.broadcasted_iota(jnp.int32, (SEG, LANES), 1)
        for b in range(scan_block):
            for c in range(CORES):
                rows = pl.ds(c * half_rows, half_rows)
                total = jnp.zeros((half_rows, LANES), jnp.float32)
                for g in range(all_segs):
                    rest = depth_of(frame[b, rows, g * SEG : (g + 1) * SEG])
                    ones = jnp.where(near_lane == g, 1.0, 0.0).astype(jnp.bfloat16)
                    for _ in range(3):
                        head = rest.astype(jnp.bfloat16)
                        rest = rest - head.astype(jnp.float32)
                        total = total + jnp.dot(
                            head, ones, preferred_element_type=jnp.float32
                        )
                seg_own[c, b] = jnp.transpose(total)[:all_segs]

    frame_loaded(0)
    send_piece(0, 0)
    frame_loaded(1)
    sum_segments()
    for k in range(1, members):
        seg_copy(k).start()
    seg_in[mine] = seg_own[core]
    for t in range(planes):
        for g in range(len(pieces[t])):
            if t or g:
                if_sent(t, g, send_piece)

    for d in range(planes):
        rows = pl.ds(tile_at(d, core), tile_rows)
        gather[d, mine] = frame[:, rows, lanes_of(col)]

    def tell_core(sem):
        @pl.when(greeter)
        def _():
            for c in range(CORES - 1):
                signal(sem, plane * CORES + c, col)

        @pl.when(jnp.logical_not(greeter))
        def _():
            pl.semaphore_wait(sem, 1)


    @pl.when(greeter)
    def _():
        pl.semaphore_wait(wave_sem.at[2], 1)

    tell_core(wave_sem.at[0])

    def swap_rows(d, c):
        return pl.ds(pl.multiple_of(tile_at(d, c) + kept_rows, 8), SWAP_ROWS)

    def swap_copy(d, c, slot):
        return pltpu.make_async_remote_copy(
            src_ref=frame.at[:, swap_rows(d, c), :],
            dst_ref=swap_in.at[slot],
            send_sem=sent_sem,
            recv_sem=swap_recv,
            device_id=(d * CORES + c, col),
            device_id_type=MESH,
        )

    for c in range(CORES):
        swap_copy(twin, c, 1 + core).start()
    swap_copy(plane, 1 - core, 0).start()


    @pl.when(below)
    def _():
        pl.semaphore_wait(wave_sem.at[0], 1)

        @pl.when(above)
        def _():
            signal(wave_sem.at[0], row_at(plane + 1), col)

    @pl.when(above)
    def _():
        pl.semaphore_wait(wave_sem.at[1], 1)

        @pl.when(below)
        def _():
            signal(wave_sem.at[1], row_at(plane - 1), col)

    tell_core(wave_sem.at[1])

    several(plane_ids.at[pl.ds(0, members - 1)], id_send, id_recv).wait_recv()

    plane_block = pl.ds(plane * members, members)
    for k in range(1, planes):
        pltpu.make_async_remote_copy(
            src_ref=plane_ids,
            dst_ref=all_ids.at[plane_block],
            send_sem=id_send,
            recv_sem=idz_recv,
            device_id=(row_at((plane + k) % planes), col),
            device_id_type=MESH,
        ).start()
    all_ids[plane_block] = plane_ids[...]
    load_hours.wait()

    base_hour = first_hour(plane)
    span = hour_span(plane)
    pair_base = first_hour(2 * pair)
    spans = sorted({hour_span(p) for p in range(planes)})

    def by_span(action):
        for n in spans:

            @pl.when(span == n)
            def _():
                action(n)

    def z_copy(t, g, k):
        return pltpu.make_async_remote_copy(
            src_ref=part.at[order[t], k, piece(t, g)],
            dst_ref=zrecv.at[plane * slots + k, piece(t, g)],
            send_sem=sent_sem,
            recv_sem=z_recv,
            device_id=(row_at(order[t]), col),
            device_id_type=MESH,
        )

    def zseg_copy(k, n):
        return pltpu.make_async_remote_copy(
            src_ref=seg_part.at[pl.ds(0, n)],
            dst_ref=zseg.at[pl.ds(plane * slots, n)],
            send_sem=sent_sem,
            recv_sem=zseg_recv,
            device_id=(row_at((plane + k) % planes), col),
            device_id_type=MESH,
        )

    def pair_copy():
        return pltpu.make_async_remote_copy(
            src_ref=seg_hour.at[core],
            dst_ref=seg_hour.at[core],
            send_sem=sent_sem,
            recv_sem=pair_recv,
            device_id=(plane * CORES + 1 - core, col),
            device_id_type=MESH,
        )

    def wait_slots(ref, send_sem, recv_sem):
        for p in range(planes):
            n = sum(hour_span(o) for o in range(planes) if o != p)

            @pl.when(plane == p)
            def _():
                several(ref.at[pl.ds(0, n)], send_sem, recv_sem).wait_recv()

    def sum_planes(ref, h):
        total = None
        for p in range(planes):
            if first_hour(p) <= h < first_hour(p) + hour_span(p):
                term = ref[p * slots + h - first_hour(p)]
                total = term if total is None else total + term
        return total

    def add_by_hour(sums, raw, p, member, b, base):
        hour = hours[p * plane_scans + member * scan_block + b] - base
        return [
            total + jnp.where(hour == k, raw, 0.0) for k, total in enumerate(sums)
        ]

    def reduce_segments():
        several(seg_in.at[pl.ds(0, members - 1)], sent_sem, seg_recv).wait_recv()
        sums = [jnp.zeros((all_segs, half_rows), jnp.float32)] * slots
        for i in range(members):
            for b in range(scan_block):
                sums = add_by_hour(sums, seg_in[i, b], plane, i, b, base_hour)
        for k in range(slots):
            seg_part[k] = sums[k]
            zseg[plane * slots + k] = sums[k]

        def send(n):
            for k in range(1, planes):
                zseg_copy(k, n).start()

        by_span(send)

    def pair_segments():
        wait_slots(zseg, sent_sem, zseg_recv)
        for h in range(hour_count):
            seg_hour[core, h] = sum_planes(zseg, h)
        pair_copy().start()

    def lay_ids():
        several(
            all_ids.at[pl.ds(0, (planes - 1) * members)], id_send, idz_recv
        ).wait_recv()
        blocks = row_devices // CORES
        for c in range(CORES):
            lanes = []
            for r in range(c * blocks, (c + 1) * blocks):
                first = r * col_devices
                tiles = [all_ids[first + q] for q in range(col_devices)]
                lanes.append(jnp.concatenate(tiles, axis=0))
            flat_ids[c] = jnp.concatenate(lanes, axis=1)

    def basin_means():
        pair_copy().wait_recv()
        halves = [flat_ids[c] for c in range(CORES)]
        place = lax.broadcasted_iota(jnp.int32, (owned, half_rows), 0)
        zero = jnp.zeros((owned, half_rows), jnp.float32)
        totals = [zero] * hour_count
        count = zero
        for n in range(owned):
            hits = [half == me * owned + n for half in halves]
            for h in range(hour_count):
                kept = [jnp.where(hits[c], seg_hour[c, h], 0.0) for c in range(CORES)]
                kept = jnp.sum(sum(kept), axis=0, keepdims=True)
                totals[h] = jnp.where(place == n, kept, totals[h])
            found = sum(jnp.where(hit, float(SEG), 0.0) for hit in hits)
            count = jnp.where(place == n, jnp.sum(found, axis=0, keepdims=True), count)
        pixels = jnp.sum(count, axis=1, keepdims=True)
        lane = lax.broadcasted_iota(jnp.int32, (owned, LANES), 1)
        means = jnp.zeros((owned, LANES), jnp.float32)
        for h in range(hour_count):
            mean = jnp.sum(totals[h], axis=1, keepdims=True) / pixels
            means = jnp.where(lane == h, mean, means)
        basin_ref[...] = jnp.transpose(means)[:hour_count, :]

    def piece_sums(t, g):
        first, end = pieces[t][g]
        sums = [jnp.zeros((end - first, tile_cols), jnp.float32)] * slots
        for i in range(members):
            for b in range(scan_block):
                depth = depth_of(gather[order[t], i, b, piece(t, g)])
                sums = add_by_hour(sums, depth, plane, i, b, base_hour)
        return sums

    def push_piece(t, g):
        in_arrival(t, g).wait_recv()
        sums = piece_sums(t, g)
        for k in range(slots):
            part[order[t], k, piece(t, g)] = sums[k]
        for k in range(slots):

            @pl.when(k < span)
            def _():
                z_copy(t, g, k).start()

    def share_swap():
        several(swap_in, sent_sem, swap_recv).wait_recv()
        for k in range(col_devices - 1, -1, -1):
            _, r, q = member_at(k)
            lanes = lanes_of(q)
            sums = [jnp.zeros((SWAP_ROWS, tile_cols), jnp.float32)] * pair_slots
            for b in range(scan_block):
                sources = (
                    (frame[b, swap_rows(plane, core), lanes], plane, core),
                    (swap_in[0, b, :, lanes], plane, 1 - core),
                    (swap_in[1, b, :, lanes], twin, 0),
                    (swap_in[2, b, :, lanes], twin, 1),
                )
                for raw, p, c in sources:
                    member = c * col_devices + col
                    sums = add_by_hour(sums, depth_of(raw), p, member, b, pair_base)
            for n in range(pair_slots):
                gsum[k, n] = sums[n]
            if k > 0:
                pltpu.make_async_remote_copy(
                    src_ref=gsum.at[k],
                    dst_ref=grecv.at[col],
                    send_sem=sent_sem,
                    recv_sem=g_recv,
                    device_id=(r, q),
                    device_id_type=MESH,
                ).start()

    def join_swap():
        several(grecv.at[pl.ds(0, col_devices - 1)], sent_sem, g_recv).wait_recv()
        for n in range(pair_slots):
            total = gsum[0, n]
            for k in range(1, col_devices):
                _, _, q = member_at(k)
                total = total + grecv[q, n]

            @pl.when(n < pair_span(pair))
            def _():
                hourly_ref[pair_base + n, kept_rows:] = total

    for t in range(planes - 1):
        for g in range(len(pieces[t])):
            if_sent(t, g, push_piece)
            if t == 0 and g == 0:
                reduce_segments()
        if t == SHARE_AFTER:
            share_swap()
    lay_ids()
    pair_segments()
    hourly_ref[...] = jnp.zeros_like(hourly_ref)
    for g in range(len(pieces[-1])):
        in_arrival(planes - 1, g).wait_recv()
        sums = piece_sums(planes - 1, g)
        for k in range(slots):

            @pl.when(k < span)
            def _():
                hourly_ref[base_hour + k, piece(planes - 1, g)] = sums[k]

    basin_means()
    join_swap()

    for p in range(planes):
        other = p + 1 - 2 * (p % 2)
        n = sum(hour_span(o) for o in range(planes) if o not in (p, other))

        @pl.when(plane == p)
        def _():
            rows = n * tile_rows + hour_span(other) * kept_rows
            count = rows * tile_cols // (8 * LANES)
            several(spare.at[pl.ds(0, count)], sent_sem, z_recv).wait_recv()

    for h in range(hour_count):
        hourly_ref[h] += sum_planes(zrecv, h)

    several(
        all_ids.at[pl.ds(0, planes * members - 1)], id_send, id_recv
    ).wait_send()
    def all_sent(n):
        count = sent_words(dims, scan_block, pair_slots, n) // (8 * LANES)
        several(spare.at[pl.ds(0, count)], sent_sem, swap_recv).wait_send()

    by_span(all_sent)


def write_out(hourly_ref, basin_ref, hourly_out, basin_out, sem):
    pairs = ((hourly_ref, hourly_out), (basin_ref, basin_out))
    copies = [pltpu.make_async_copy(s, d, sem.at[n]) for n, (s, d) in enumerate(pairs)]
    for copy in copies:
        copy.start()
    for copy in copies:
        copy.wait()


def body(reflectivity, scan_hour, basin_ids):
    row_devices = lax.axis_size("row")
    col_devices = lax.axis_size("col")
    scan_block, grid_height, grid_width = reflectivity.shape
    tile_rows = grid_height // row_devices
    tile_cols = grid_width // col_devices
    scan_count = scan_hour.shape[0]
    hour_count = (scan_count + 10) // HOUR_SCANS + 1
    devices = row_devices * col_devices
    owned = grid_height * grid_width // (SEG * BASIN_ROWS) // devices
    planes = row_devices // CORES
    members = CORES * col_devices
    plane_scans = members * scan_block

    def span_of(first, last):
        rest = scan_count - plane_scans * (last + 1)
        return hour_count - rest // HOUR_SCANS - (first * plane_scans) // HOUR_SCANS

    slots = max(span_of(p, p) for p in range(planes))
    pair_slots = max(span_of(2 * j, 2 * j + 1) for j in range(planes // 2))
    seg_shape = (grid_width // SEG, grid_height // CORES)
    dims = (row_devices, col_devices, hour_count, slots, tile_rows, tile_cols, owned)
    piece_count = len(FIRST) + len(LATER) * (planes - 2) + len(OWN)
    spare_count = sent_words(dims, scan_block, pair_slots, slots) // (8 * LANES)
    dma = pltpu.SemaphoreType.DMA
    f32 = jnp.float32
    id_shape = basin_ids.shape[::-1]
    anywhere = pl.BlockSpec(memory_space=pltpu.HBM)
    inside = pl.BlockSpec(memory_space=pltpu.VMEM)
    hourly, basin = pl.pallas_call(
        functools.partial(kernel, dims),
        out_shape=(
            jax.ShapeDtypeStruct((hour_count, tile_rows, tile_cols), f32),
            jax.ShapeDtypeStruct((hour_count, owned), f32),
        ),
        in_specs=[anywhere] * 3,
        out_specs=(inside, inside),
        scratch_shapes=[
            pltpu.VMEM(reflectivity.shape, f32),
            pltpu.SMEM(scan_hour.shape, jnp.int32),
            pltpu.VMEM(id_shape, jnp.int32),
            pltpu.VMEM((planes, members, scan_block, tile_rows, tile_cols), f32),
            pltpu.VMEM((planes, slots, tile_rows, tile_cols), f32),
            pltpu.VMEM((planes * slots, tile_rows, tile_cols), f32),
            pltpu.VMEM((members,) + id_shape, jnp.int32),
            pltpu.VMEM((planes * members,) + id_shape, jnp.int32),
            pltpu.VMEM((CORES,) + seg_shape, jnp.int32),
            pltpu.VMEM((CORES, scan_block) + seg_shape, f32),
            pltpu.VMEM((members, scan_block) + seg_shape, f32),
            pltpu.VMEM((slots,) + seg_shape, f32),
            pltpu.VMEM((planes * slots,) + seg_shape, f32),
            pltpu.VMEM((CORES, hour_count) + seg_shape, f32),
            pltpu.VMEM((CORES + 1, scan_block, SWAP_ROWS, grid_width), f32),
            pltpu.VMEM((col_devices, pair_slots, SWAP_ROWS, tile_cols), f32),
            pltpu.VMEM((col_devices, pair_slots, SWAP_ROWS, tile_cols), f32),
            pltpu.VMEM((spare_count, 8, LANES), f32),
            pltpu.SemaphoreType.REGULAR((3,)),
            dma((2,)),
            dma((2,)),
            dma,
            dma((piece_count,)),
            dma,
            dma,
            dma,
            dma,
            dma,
            dma,
            dma,
            dma,
            dma,
        ],
        compiler_params=pltpu.CompilerParams(
            collective_id=0, has_side_effects=True, vmem_limit_bytes=40 * 2**20
        ),
    )(*(pltpu.with_memory_space_constraint(v, pltpu.HBM) for v in (reflectivity, scan_hour, basin_ids.T)))
    hourly, basin = pl.pallas_call(
        write_out,
        out_shape=(
            jax.ShapeDtypeStruct(hourly.shape, f32),
            jax.ShapeDtypeStruct(basin.shape, f32),
        ),
        in_specs=[inside] * 2,
        out_specs=(anywhere, anywhere),
        scratch_shapes=[dma((2,))],
        compiler_params=pltpu.CompilerParams(vmem_limit_bytes=8 * 2**20),
    )(hourly, basin)
    return hourly, basin.T


def solution(mesh):
    placed = (P(("row", "col"), None, None), P(), P("row", "col"))
    return jax.shard_map(
        body,
        mesh=mesh,
        in_specs=placed,
        out_specs=(P(None, "row", "col"), P(("row", "col"), None)),
        check_vma=False,
    )
```

```python
import functools
import math

import jax
import jax.numpy as jnp
from jax import lax
from jax.experimental import pallas as pl
from jax.experimental.pallas import tpu as pltpu
from jax.sharding import PartitionSpec as P

SEG = 128
BASIN_ROWS = 8
HOUR_SCANS = 12
CORES = 2
LANES = 128
FIRST = (8, 16, 32)
LATER = (16, 32)
OWN = (16,)
SWAP_ROWS = 16
SHARE_AFTER = 1
MESH = pl.DeviceIdType.MESH

slope_db = math.log(10.0) / 16.0
offset_zr = math.log(200.0) / 1.6 + math.log(12.0)


def sent_words(dims, scan_block, pair_slots, span):
    row_devices, col_devices, hour_count, slots, tile_rows, tile_cols, owned = dims
    planes = row_devices // CORES
    members = CORES * col_devices
    kept_rows = tile_rows - SWAP_ROWS
    seg_words = row_devices * tile_rows // CORES * col_devices * tile_cols // SEG
    chunk_rows = (planes - 2) * tile_rows + kept_rows
    pixels = (members - 1) * (chunk_rows + kept_rows) * tile_cols * scan_block
    segments = ((members - 1) * scan_block + hour_count) * seg_words
    swapped = (CORES + 1) * SWAP_ROWS * col_devices * tile_cols * scan_block
    shared = (col_devices - 1) * pair_slots * SWAP_ROWS * tile_cols
    sums = span * (chunk_rows * tile_cols + (planes - 1) * seg_words)
    return pixels + segments + swapped + shared + sums


def kernel(
    dims,
    refl_ref,
    hour_ref,
    ids_ref,
    hourly_ref,
    basin_ref,
    frame,
    hours,
    ids,
    gather,
    part,
    zrecv,
    plane_ids,
    all_ids,
    flat_ids,
    seg_own,
    seg_in,
    seg_part,
    zseg,
    seg_hour,
    swap_in,
    gsum,
    grecv,
    spare,
    wave_sem,
    local_sem,
    load_sem,
    sent_sem,
    in_recv,
    z_recv,
    id_send,
    id_recv,
    idz_recv,
    seg_recv,
    zseg_recv,
    pair_recv,
    swap_recv,
    g_recv,
):
    row_devices, col_devices, hour_count, slots, tile_rows, tile_cols, owned = dims
    planes = row_devices // CORES
    members = CORES * col_devices
    devices = row_devices * col_devices
    scan_block = gather.shape[2]
    scan_count = hour_ref.shape[0]
    plane_scans = members * scan_block
    cuts = [FIRST] + [LATER] * (planes - 2) + [OWN]
    pieces = [list(zip((0,) + ends[:-1], ends)) for ends in cuts]
    piece_sem = [sum(map(len, cuts[:t])) for t in range(planes)]
    all_segs, half_rows = seg_own.shape[2:]
    kept_rows = tile_rows - SWAP_ROWS
    pair_slots = gsum.shape[1]

    row = lax.axis_index("row")
    col = lax.axis_index("col")
    plane = row // CORES
    core = row % CORES
    mine = core * col_devices + col
    me = row * col_devices + col
    pair = plane // 2
    twin = plane + 1 - 2 * (plane % 2)

    def first_hour(p):
        return (p * plane_scans) // HOUR_SCANS

    def hour_span(p):
        rest = scan_count - plane_scans - p * plane_scans
        return hour_count - rest // HOUR_SCANS - first_hour(p)

    def pair_span(j):
        return first_hour(2 * j + 1) + hour_span(2 * j + 1) - first_hour(2 * j)

    def by_plane(table):
        value = table[0]
        for p in range(1, planes):
            value = jnp.where(plane == p, table[p], value)
        return value

    def chunk_order(p):
        others = sorted(
            (d for d in range(planes) if d != p),
            key=lambda d: (d == p + 1 - 2 * (p % 2), abs(d - p)),
        )
        if 0 in others:
            others.remove(0)
            others.insert(0, 0)
        return others + [p]

    orders = [chunk_order(p) for p in range(planes)]
    order = [by_plane([o[t] for o in orders]) for t in range(planes)]
    whole = [order[t] != twin for t in range(planes)]

    def member_at(k):
        dc = k // col_devices
        dq = k % col_devices
        half = col_devices // 2
        qq = ((col // 2 + dq // 2) % half) * 2 + (col + dq) % 2
        other = ((core + dc) % CORES) * col_devices + qq
        return other, plane * CORES + other // col_devices, other % col_devices

    def several(ref, send_sem, recv_sem):
        return pltpu.make_async_remote_copy(
            src_ref=ref,
            dst_ref=ref,
            send_sem=send_sem,
            recv_sem=recv_sem,
            device_id=((row + 1) % row_devices, col),
            device_id_type=MESH,
        )

    def signal(sem, r, q):
        pl.semaphore_signal(sem, inc=1, device_id=(r, q), device_id_type=MESH)

    def row_at(p):
        return p * CORES + core

    barrier = pltpu.get_barrier_semaphore()
    far_first = sorted(range(1, members), key=lambda k: (-(k % col_devices), k))
    for k in far_first:
        _, r, q = member_at(k)
        signal(barrier, r, q)

    greeter = core == CORES - 1
    below = greeter & (plane > 0)
    above = greeter & (plane < planes - 1)

    @pl.when(below)
    def _():
        signal(barrier, row_at(plane - 1), col)

    @pl.when(above)
    def _():
        signal(barrier, row_at(plane + 1), col)

    def tile_at(d, c):
        return pl.multiple_of((d * CORES + c) * tile_rows, 8)

    def lanes_of(q):
        return pl.ds(pl.multiple_of(q * tile_cols, 128), tile_cols)

    def plane_rows(d):
        rows = CORES * tile_rows
        return pl.ds(pl.multiple_of(d * rows, 8), rows)

    load_ids = pltpu.make_async_copy(ids_ref, ids, local_sem.at[0])
    load_ids.start()
    for t, d in enumerate(order):
        pltpu.make_async_copy(
            refl_ref.at[:, plane_rows(d), :],
            frame.at[:, plane_rows(d), :],
            load_sem.at[min(t, 1)],
        ).start()

    def frame_loaded(late):
        count = (planes - 1 if late else 1) * CORES * tile_rows
        rows = frame.at[:, pl.ds(0, count), :]
        pltpu.make_async_copy(rows, rows, load_sem.at[late]).wait()

    load_hours = pltpu.make_async_copy(hour_ref, hours, local_sem.at[1])
    load_hours.start()
    for k in range(slots):
        zrecv[plane * slots + k] = jnp.zeros((tile_rows, tile_cols), jnp.float32)
        zrecv[twin * slots + k, kept_rows:] = jnp.zeros(
            (SWAP_ROWS, tile_cols), jnp.float32
        )

    load_ids.wait()
    plane_ids[mine] = ids[...]
    beside = jnp.where(below, 1, 0) + jnp.where(above, 1, 0)
    pl.semaphore_wait(barrier, members - 1 + beside)

    def id_copy(k):
        other, r, q = member_at(k)
        return pltpu.make_async_remote_copy(
            src_ref=ids,
            dst_ref=plane_ids.at[mine],
            send_sem=id_send,
            recv_sem=id_recv,
            device_id=(r, q),
            device_id_type=MESH,
        )

    for k in range(1, members):
        id_copy(k).start()

    @pl.when(greeter)
    def _():
        signal(wave_sem.at[2], row_at(twin), col)

    @pl.when(greeter & (plane == 0))
    def _():
        signal(wave_sem.at[0], row_at(plane + 1), col)

    @pl.when(greeter & (plane == planes - 1))
    def _():
        signal(wave_sem.at[1], row_at(plane - 1), col)

    def piece(t, g):
        first, end = pieces[t][g]
        return pl.ds(first, end - first)

    def in_copy(t, g, k):
        other, r, q = member_at(k)
        d = order[t]
        first, end = pieces[t][g]
        top = pl.multiple_of(tile_at(d, other // col_devices) + first, 8)
        return pltpu.make_async_remote_copy(
            src_ref=frame.at[:, pl.ds(top, end - first), lanes_of(q)],
            dst_ref=gather.at[d, mine, :, piece(t, g)],
            send_sem=sent_sem,
            recv_sem=in_recv.at[piece_sem[t] + g],
            device_id=(r, q),
            device_id_type=MESH,
        )

    def in_arrival(t, g):
        ref = gather.at[order[t], pl.ds(0, members - 1), :, piece(t, g)]
        return several(ref, sent_sem, in_recv.at[piece_sem[t] + g])

    def if_sent(t, g, action):
        if pieces[t][g][0] < kept_rows:
            action(t, g)
        else:

            @pl.when(whole[t])
            def _():
                action(t, g)

    def send_piece(t, g):
        for k in sorted(range(1, members), key=lambda k: (-(k % col_devices), -k)):
            in_copy(t, g, k).start()

    def seg_copy(k):
        other, r, q = member_at(k)
        return pltpu.make_async_remote_copy(
            src_ref=seg_own.at[other // col_devices],
            dst_ref=seg_in.at[mine],
            send_sem=sent_sem,
            recv_sem=seg_recv,
            device_id=(r, q),
            device_id_type=MESH,
        )

    def depth_of(raw):
        return jnp.exp(raw * slope_db - offset_zr)

    def sum_segments():
        near_lane = lax.broadcasted_iota(jnp.int32, (SEG, LANES), 1)
        for b in range(scan_block):
            for c in range(CORES):
                rows = pl.ds(c * half_rows, half_rows)
                total = jnp.zeros((half_rows, LANES), jnp.float32)
                for g in range(all_segs):
                    rest = depth_of(frame[b, rows, g * SEG : (g + 1) * SEG])
                    ones = jnp.where(near_lane == g, 1.0, 0.0).astype(jnp.bfloat16)
                    for _ in range(3):
                        head = rest.astype(jnp.bfloat16)
                        rest = rest - head.astype(jnp.float32)
                        total = total + jnp.dot(
                            head, ones, preferred_element_type=jnp.float32
                        )
                seg_own[c, b] = jnp.transpose(total)[:all_segs]

    frame_loaded(0)
    send_piece(0, 0)
    frame_loaded(1)
    sum_segments()
    for k in range(1, members):
        seg_copy(k).start()
    seg_in[mine] = seg_own[core]
    for t in range(planes):
        for g in range(len(pieces[t])):
            if t or g:
                if_sent(t, g, send_piece)

    for d in range(planes):
        rows = pl.ds(tile_at(d, core), tile_rows)
        gather[d, mine] = frame[:, rows, lanes_of(col)]

    def tell_core(sem):
        @pl.when(greeter)
        def _():
            for c in range(CORES - 1):
                signal(sem, plane * CORES + c, col)

        @pl.when(jnp.logical_not(greeter))
        def _():
            pl.semaphore_wait(sem, 1)


    @pl.when(greeter)
    def _():
        pl.semaphore_wait(wave_sem.at[2], 1)

    tell_core(wave_sem.at[0])

    def swap_rows(d, c):
        return pl.ds(pl.multiple_of(tile_at(d, c) + kept_rows, 8), SWAP_ROWS)

    def swap_copy(d, c, slot):
        return pltpu.make_async_remote_copy(
            src_ref=frame.at[:, swap_rows(d, c), :],
            dst_ref=swap_in.at[slot],
            send_sem=sent_sem,
            recv_sem=swap_recv,
            device_id=(d * CORES + c, col),
            device_id_type=MESH,
        )

    for c in range(CORES):
        swap_copy(twin, c, 1 + core).start()
    swap_copy(plane, 1 - core, 0).start()


    @pl.when(below)
    def _():
        pl.semaphore_wait(wave_sem.at[0], 1)

        @pl.when(above)
        def _():
            signal(wave_sem.at[0], row_at(plane + 1), col)

    @pl.when(above)
    def _():
        pl.semaphore_wait(wave_sem.at[1], 1)

        @pl.when(below)
        def _():
            signal(wave_sem.at[1], row_at(plane - 1), col)

    tell_core(wave_sem.at[1])

    several(plane_ids.at[pl.ds(0, members - 1)], id_send, id_recv).wait_recv()

    plane_block = pl.ds(plane * members, members)
    for k in range(1, planes):
        pltpu.make_async_remote_copy(
            src_ref=plane_ids,
            dst_ref=all_ids.at[plane_block],
            send_sem=id_send,
            recv_sem=idz_recv,
            device_id=(row_at((plane + k) % planes), col),
            device_id_type=MESH,
        ).start()
    all_ids[plane_block] = plane_ids[...]
    load_hours.wait()

    base_hour = first_hour(plane)
    span = hour_span(plane)
    pair_base = first_hour(2 * pair)
    spans = sorted({hour_span(p) for p in range(planes)})

    def by_span(action):
        for n in spans:

            @pl.when(span == n)
            def _():
                action(n)

    def z_copy(t, g, k):
        return pltpu.make_async_remote_copy(
            src_ref=part.at[order[t], k, piece(t, g)],
            dst_ref=zrecv.at[plane * slots + k, piece(t, g)],
            send_sem=sent_sem,
            recv_sem=z_recv,
            device_id=(row_at(order[t]), col),
            device_id_type=MESH,
        )

    def zseg_copy(k, n):
        return pltpu.make_async_remote_copy(
            src_ref=seg_part.at[pl.ds(0, n)],
            dst_ref=zseg.at[pl.ds(plane * slots, n)],
            send_sem=sent_sem,
            recv_sem=zseg_recv,
            device_id=(row_at((plane + k) % planes), col),
            device_id_type=MESH,
        )

    def pair_copy():
        return pltpu.make_async_remote_copy(
            src_ref=seg_hour.at[core],
            dst_ref=seg_hour.at[core],
            send_sem=sent_sem,
            recv_sem=pair_recv,
            device_id=(plane * CORES + 1 - core, col),
            device_id_type=MESH,
        )

    def wait_slots(ref, send_sem, recv_sem):
        for p in range(planes):
            n = sum(hour_span(o) for o in range(planes) if o != p)

            @pl.when(plane == p)
            def _():
                several(ref.at[pl.ds(0, n)], send_sem, recv_sem).wait_recv()

    def sum_planes(ref, h):
        total = None
        for p in range(planes):
            if first_hour(p) <= h < first_hour(p) + hour_span(p):
                term = ref[p * slots + h - first_hour(p)]
                total = term if total is None else total + term
        return total

    def add_by_hour(sums, raw, p, member, b, base):
        hour = hours[p * plane_scans + member * scan_block + b] - base
        return [
            total + jnp.where(hour == k, raw, 0.0) for k, total in enumerate(sums)
        ]

    def reduce_segments():
        several(seg_in.at[pl.ds(0, members - 1)], sent_sem, seg_recv).wait_recv()
        sums = [jnp.zeros((all_segs, half_rows), jnp.float32)] * slots
        for i in range(members):
            for b in range(scan_block):
                sums = add_by_hour(sums, seg_in[i, b], plane, i, b, base_hour)
        for k in range(slots):
            seg_part[k] = sums[k]
            zseg[plane * slots + k] = sums[k]

        def send(n):
            for k in range(1, planes):
                zseg_copy(k, n).start()

        by_span(send)

    def pair_segments():
        wait_slots(zseg, sent_sem, zseg_recv)
        for h in range(hour_count):
            seg_hour[core, h] = sum_planes(zseg, h)
        pair_copy().start()

    def lay_ids():
        several(
            all_ids.at[pl.ds(0, (planes - 1) * members)], id_send, idz_recv
        ).wait_recv()
        blocks = row_devices // CORES
        for c in range(CORES):
            lanes = []
            for r in range(c * blocks, (c + 1) * blocks):
                first = r * col_devices
                tiles = [all_ids[first + q] for q in range(col_devices)]
                lanes.append(jnp.concatenate(tiles, axis=0))
            flat_ids[c] = jnp.concatenate(lanes, axis=1)

    def basin_means():
        pair_copy().wait_recv()
        halves = [flat_ids[c] for c in range(CORES)]
        place = lax.broadcasted_iota(jnp.int32, (owned, half_rows), 0)
        zero = jnp.zeros((owned, half_rows), jnp.float32)
        totals = [zero] * hour_count
        count = zero
        for n in range(owned):
            hits = [half == me * owned + n for half in halves]
            for h in range(hour_count):
                kept = [jnp.where(hits[c], seg_hour[c, h], 0.0) for c in range(CORES)]
                kept = jnp.sum(sum(kept), axis=0, keepdims=True)
                totals[h] = jnp.where(place == n, kept, totals[h])
            found = sum(jnp.where(hit, float(SEG), 0.0) for hit in hits)
            count = jnp.where(place == n, jnp.sum(found, axis=0, keepdims=True), count)
        pixels = jnp.sum(count, axis=1, keepdims=True)
        lane = lax.broadcasted_iota(jnp.int32, (owned, LANES), 1)
        means = jnp.zeros((owned, LANES), jnp.float32)
        for h in range(hour_count):
            mean = jnp.sum(totals[h], axis=1, keepdims=True) / pixels
            means = jnp.where(lane == h, mean, means)
        basin_ref[...] = jnp.transpose(means)[:hour_count, :]

    def piece_sums(t, g):
        first, end = pieces[t][g]
        sums = [jnp.zeros((end - first, tile_cols), jnp.float32)] * slots
        for i in range(members):
            for b in range(scan_block):
                depth = depth_of(gather[order[t], i, b, piece(t, g)])
                sums = add_by_hour(sums, depth, plane, i, b, base_hour)
        return sums

    def push_piece(t, g):
        in_arrival(t, g).wait_recv()
        sums = piece_sums(t, g)
        for k in range(slots):
            part[order[t], k, piece(t, g)] = sums[k]
        for k in range(slots):

            @pl.when(k < span)
            def _():
                z_copy(t, g, k).start()

    def share_swap():
        several(swap_in, sent_sem, swap_recv).wait_recv()
        for k in range(col_devices - 1, -1, -1):
            _, r, q = member_at(k)
            lanes = lanes_of(q)
            sums = [jnp.zeros((SWAP_ROWS, tile_cols), jnp.float32)] * pair_slots
            for b in range(scan_block):
                sources = (
                    (frame[b, swap_rows(plane, core), lanes], plane, core),
                    (swap_in[0, b, :, lanes], plane, 1 - core),
                    (swap_in[1, b, :, lanes], twin, 0),
                    (swap_in[2, b, :, lanes], twin, 1),
                )
                for raw, p, c in sources:
                    member = c * col_devices + col
                    sums = add_by_hour(sums, depth_of(raw), p, member, b, pair_base)
            for n in range(pair_slots):
                gsum[k, n] = sums[n]
            if k > 0:
                pltpu.make_async_remote_copy(
                    src_ref=gsum.at[k],
                    dst_ref=grecv.at[col],
                    send_sem=sent_sem,
                    recv_sem=g_recv,
                    device_id=(r, q),
                    device_id_type=MESH,
                ).start()

    def join_swap():
        several(grecv.at[pl.ds(0, col_devices - 1)], sent_sem, g_recv).wait_recv()
        for n in range(pair_slots):
            total = gsum[0, n]
            for k in range(1, col_devices):
                _, _, q = member_at(k)
                total = total + grecv[q, n]

            @pl.when(n < pair_span(pair))
            def _():
                hourly_ref[pair_base + n, kept_rows:] = total

    for t in range(planes - 1):
        for g in range(len(pieces[t])):
            if_sent(t, g, push_piece)
            if t == 0 and g == 0:
                reduce_segments()
        if t == SHARE_AFTER:
            share_swap()
    lay_ids()
    pair_segments()
    hourly_ref[...] = jnp.zeros_like(hourly_ref)
    for g in range(len(pieces[-1])):
        in_arrival(planes - 1, g).wait_recv()
        sums = piece_sums(planes - 1, g)
        for k in range(slots):

            @pl.when(k < span)
            def _():
                hourly_ref[base_hour + k, piece(planes - 1, g)] = sums[k]

    basin_means()
    join_swap()

    for p in range(planes):
        other = p + 1 - 2 * (p % 2)
        n = sum(hour_span(o) for o in range(planes) if o not in (p, other))

        @pl.when(plane == p)
        def _():
            rows = n * tile_rows + hour_span(other) * kept_rows
            count = rows * tile_cols // (8 * LANES)
            several(spare.at[pl.ds(0, count)], sent_sem, z_recv).wait_recv()

    for h in range(hour_count):
        hourly_ref[h] += sum_planes(zrecv, h)

    several(
        all_ids.at[pl.ds(0, planes * members - 1)], id_send, id_recv
    ).wait_send()
    def all_sent(n):
        count = sent_words(dims, scan_block, pair_slots, n) // (8 * LANES)
        several(spare.at[pl.ds(0, count)], sent_sem, swap_recv).wait_send()

    by_span(all_sent)


def write_out(hourly_ref, basin_ref, hourly_out, basin_out, sem):
    pairs = ((hourly_ref, hourly_out), (basin_ref, basin_out))
    copies = [pltpu.make_async_copy(s, d, sem.at[n]) for n, (s, d) in enumerate(pairs)]
    for copy in copies:
        copy.start()
    for copy in copies:
        copy.wait()


def body(reflectivity, scan_hour, basin_ids):
    row_devices = lax.axis_size("row")
    col_devices = lax.axis_size("col")
    scan_block, grid_height, grid_width = reflectivity.shape
    tile_rows = grid_height // row_devices
    tile_cols = grid_width // col_devices
    scan_count = scan_hour.shape[0]
    hour_count = (scan_count + 10) // HOUR_SCANS + 1
    devices = row_devices * col_devices
    owned = grid_height * grid_width // (SEG * BASIN_ROWS) // devices
    planes = row_devices // CORES
    members = CORES * col_devices
    plane_scans = members * scan_block

    def span_of(first, last):
        rest = scan_count - plane_scans * (last + 1)
        return hour_count - rest // HOUR_SCANS - (first * plane_scans) // HOUR_SCANS

    slots = max(span_of(p, p) for p in range(planes))
    pair_slots = max(span_of(2 * j, 2 * j + 1) for j in range(planes // 2))
    seg_shape = (grid_width // SEG, grid_height // CORES)
    dims = (row_devices, col_devices, hour_count, slots, tile_rows, tile_cols, owned)
    piece_count = len(FIRST) + len(LATER) * (planes - 2) + len(OWN)
    spare_count = sent_words(dims, scan_block, pair_slots, slots) // (8 * LANES)
    dma = pltpu.SemaphoreType.DMA
    f32 = jnp.float32
    id_shape = basin_ids.shape[::-1]
    anywhere = pl.BlockSpec(memory_space=pltpu.HBM)
    inside = pl.BlockSpec(memory_space=pltpu.VMEM)
    hourly, basin = pl.pallas_call(
        functools.partial(kernel, dims),
        out_shape=(
            jax.ShapeDtypeStruct((hour_count, tile_rows, tile_cols), f32),
            jax.ShapeDtypeStruct((hour_count, owned), f32),
        ),
        in_specs=[anywhere] * 3,
        out_specs=(inside, inside),
        scratch_shapes=[
            pltpu.VMEM(reflectivity.shape, f32),
            pltpu.SMEM(scan_hour.shape, jnp.int32),
            pltpu.VMEM(id_shape, jnp.int32),
            pltpu.VMEM((planes, members, scan_block, tile_rows, tile_cols), f32),
            pltpu.VMEM((planes, slots, tile_rows, tile_cols), f32),
            pltpu.VMEM((planes * slots, tile_rows, tile_cols), f32),
            pltpu.VMEM((members,) + id_shape, jnp.int32),
            pltpu.VMEM((planes * members,) + id_shape, jnp.int32),
            pltpu.VMEM((CORES,) + seg_shape, jnp.int32),
            pltpu.VMEM((CORES, scan_block) + seg_shape, f32),
            pltpu.VMEM((members, scan_block) + seg_shape, f32),
            pltpu.VMEM((slots,) + seg_shape, f32),
            pltpu.VMEM((planes * slots,) + seg_shape, f32),
            pltpu.VMEM((CORES, hour_count) + seg_shape, f32),
            pltpu.VMEM((CORES + 1, scan_block, SWAP_ROWS, grid_width), f32),
            pltpu.VMEM((col_devices, pair_slots, SWAP_ROWS, tile_cols), f32),
            pltpu.VMEM((col_devices, pair_slots, SWAP_ROWS, tile_cols), f32),
            pltpu.VMEM((spare_count, 8, LANES), f32),
            pltpu.SemaphoreType.REGULAR((3,)),
            dma((2,)),
            dma((2,)),
            dma,
            dma((piece_count,)),
            dma,
            dma,
            dma,
            dma,
            dma,
            dma,
            dma,
            dma,
            dma,
        ],
        compiler_params=pltpu.CompilerParams(
            collective_id=0, has_side_effects=True, vmem_limit_bytes=40 * 2**20
        ),
    )(*(pltpu.with_memory_space_constraint(v, pltpu.HBM) for v in (reflectivity, scan_hour, basin_ids.T)))
    hourly, basin = pl.pallas_call(
        write_out,
        out_shape=(
            jax.ShapeDtypeStruct(hourly.shape, f32),
            jax.ShapeDtypeStruct(basin.shape, f32),
        ),
        in_specs=[inside] * 2,
        out_specs=(anywhere, anywhere),
        scratch_shapes=[dma((2,))],
        compiler_params=pltpu.CompilerParams(vmem_limit_bytes=8 * 2**20),
    )(hourly, basin)
    return hourly, basin.T


def solution(mesh):
    placed = (P(("row", "col"), None, None), P(), P("row", "col"))
    return jax.shard_map(
        body,
        mesh=mesh,
        in_specs=placed,
        out_specs=(P(None, "row", "col"), P(("row", "col"), None)),
        check_vma=False,
    )
```
